8 devices in a mesh: model: 4 (over z, y, x), data: 2 (over core).
Axes of the slice: x: 2, y: 2, z: 1, core: 2. Of those that a mesh axis runs over, the one named last changes fastest.
Arguments:
- local_grads: bfloat16 [2, 192, 262144], P('data', None, 'model')
- master: float32 [192, 262144], P(None, ('model', 'data'))
- moment_one: float32 [192, 262144], P(None, ('model', 'data'))
- moment_two: float32 [192, 262144], P(None, ('model', 'data'))
Outputs:
- output 1: bfloat16 [192, 262144], P(None, 'model')
- output 2: float32 [192, 262144], P(None, ('model', 'data'))
- output 3: float32 [192, 262144], P(None, ('model', 'data'))
- output 4: float32 [192, 262144], P(None, ('model', 'data'))
All inputs are finite; a program needn't handle non-finite values.
Results may differ from the reference program's by a relative error of at most 0.001.
Values are sent between devices in bfloat16 or wider.
A program may use at most 1 GiB of HBM per device.

```python
import jax
import jax.numpy as jnp
from jax import lax

D = 512
LAYERS = 16
DATA = 2
STEP = 4
BLOCKS = 12 * LAYERS
BLOCK_SIZE = D * D
LEARN_RATE = 0.08
BETA_ONE = 0.9
BETA_TWO = 0.999
EPSILON = 1e-6
WEIGHT_DECAY = 0.01
MAX_NORM = 1.0
CORR_ONE = 1.0 - BETA_ONE ** STEP
CORR_TWO = 1.0 - BETA_TWO ** STEP


def tensor_sums(block_values):
    return jnp.stack([block_values[..., 0:3].sum(axis=-1), block_values[..., 3], block_values[..., 4:8].sum(axis=-1), block_values[..., 8:12].sum(axis=-1)], axis=-1)


def spread_tensors(tensor_values):
    lead_shape = tensor_values.shape[:-1]
    pieces = [jnp.broadcast_to(tensor_values[..., tensor_pos:tensor_pos + 1], lead_shape + (block_count,)) for tensor_pos, block_count in enumerate((3, 1, 4, 4))]
    return jnp.concatenate(pieces, axis=-1)


def setup_inputs(seed: int = 0) -> dict:
    key_list = jax.random.split(jax.random.key(seed), 8)
    fan_scale = jnp.concatenate([jnp.full((8,), D ** -0.5, jnp.float32), jnp.full((4,), (4 * D) ** -0.5, jnp.float32)])
    weight_factor = jnp.exp(jax.random.uniform(key_list[0], (LAYERS, 4), jnp.float32, minval=-0.8, maxval=0.8))
    weight_scale = (spread_tensors(weight_factor) * fan_scale).reshape(BLOCKS, 1)
    weight_slope = spread_tensors(jax.random.uniform(key_list[1], (LAYERS, 4), jnp.float32, minval=1.5, maxval=2.5)).reshape(BLOCKS, 1)
    position = jnp.arange(BLOCK_SIZE, dtype=jnp.float32) / BLOCK_SIZE - 0.5
    grad_factor = spread_tensors(jnp.exp(jax.random.uniform(key_list[2], (LAYERS, 4), jnp.float32, minval=-1.0, maxval=1.0))).reshape(BLOCKS, 1)
    grad_sigma = grad_factor * (3.0 * MAX_NORM) / jnp.sqrt(BLOCK_SIZE * jnp.sum(grad_factor * grad_factor))
    unit_scale = grad_sigma / jnp.sqrt(2.0)
    shared = jax.random.normal(key_list[3], (BLOCKS, BLOCK_SIZE), jnp.float32)

    def one_replica(replica):
        replica_noise = jax.random.normal(jax.random.fold_in(key_list[4], replica), (BLOCKS, BLOCK_SIZE), jnp.float32)
        return (unit_scale * (shared + DATA ** 0.5 * replica_noise)).astype(jnp.bfloat16)

    local_grads = lax.map(one_replica, jnp.arange(DATA))
    step_sigma = grad_sigma / 3.0
    master = weight_scale * jnp.exp(weight_slope * position) * jax.random.normal(key_list[5], (BLOCKS, BLOCK_SIZE), jnp.float32)
    moment_one = 0.1 * step_sigma * jax.random.normal(key_list[6], (BLOCKS, BLOCK_SIZE), jnp.float32)
    moment_two = 0.003 * step_sigma * step_sigma * jax.random.uniform(key_list[7], (BLOCKS, BLOCK_SIZE), jnp.float32, minval=0.5, maxval=1.5)
    return {'local_grads': local_grads, 'master': master, 'moment_one': moment_one, 'moment_two': moment_two}


def reference(local_grads, master, moment_one, moment_two):
    grad_mean = jnp.sum(local_grads, axis=0, dtype=jnp.float32) / DATA
    clip_scale = jnp.minimum(1.0, MAX_NORM / jnp.sqrt(jnp.sum(grad_mean * grad_mean)))
    scaled = clip_scale * grad_mean
    new_one = BETA_ONE * moment_one + (1.0 - BETA_ONE) * scaled
    new_two = BETA_TWO * moment_two + (1.0 - BETA_TWO) * scaled * scaled
    direction = (new_one / CORR_ONE) / (jnp.sqrt(new_two / CORR_TWO) + EPSILON) + WEIGHT_DECAY * master
    norm_sq = jnp.stack([jnp.sum(master * master, axis=1), jnp.sum(direction * direction, axis=1)])
    tensor_norms = jnp.sqrt(tensor_sums(norm_sq.reshape(2, LAYERS, 12)))
    block_ratio = spread_tensors(tensor_norms[0] / tensor_norms[1]).reshape(BLOCKS, 1)
    new_master = master - LEARN_RATE * block_ratio * direction
    return new_master.astype(jnp.bfloat16), new_master, new_one, new_two
```

```python
import functools

import jax
import jax.numpy as jnp
from jax import lax
from jax.experimental import pallas as pl
from jax.experimental.pallas import tpu as pltpu
from jax.sharding import PartitionSpec as P

STEP = 4
LEARN_RATE = 0.08
BETA_ONE = 0.9
BETA_TWO = 0.999
EPSILON = 1e-6
WEIGHT_DECAY = 0.01
MAX_NORM = 1.0
CORR_ONE = 1.0 - BETA_ONE ** STEP
CORR_TWO = 1.0 - BETA_TWO ** STEP
TINY = 1.2e-38

MESH = pl.DeviceIdType.MESH
F32 = jnp.float32
BF16 = jnp.bfloat16
SCOPE = 4000 << 10
LANES = 128
GROUP = 8

PART = 16384
LAND_SLOTS = 8
OWN_SLOTS = 6
RING = 24
LAG = 6
CHUNK = 8192
SEND_SLOTS = 4
WRITE_SLOTS = 6
WRITE_CHUNK = 8192


def rows(group):
    return pl.ds(pl.multiple_of(group * GROUP, GROUP), GROUP)


def lanes_of():
    return lax.broadcasted_iota(jnp.int32, (GROUP, LANES), 1)


def put_lane(tile, lane_ids, lane, partial):
    row_sum = jnp.sum(partial, axis=1, keepdims=True)
    return tile + jnp.where(lane_ids == lane, row_sum, 0.0)


def tree_sum(values):
    while len(values) > 1:
        values = [a + b for a, b in zip(values[::2], values[1::2])] + ([values[-1]] if len(values) % 2 else [])
    return values[0]


def peers(model_size, data_size):
    model, data = lax.axis_index('model'), lax.axis_index('data')
    out = []
    for step in range(1, model_size * data_size):
        peer_model = lax.rem(model + step // data_size, model_size)
        peer_data = lax.rem(data + step % data_size, data_size)
        out.append(((peer_model, peer_data), peer_model * data_size + peer_data))
    return model * data_size + data, out


def enter(others):
    barrier = pltpu.get_barrier_semaphore()
    for device, _ in others:
        pl.semaphore_signal(barrier, inc=1, device_id=device, device_id_type=MESH)
    pl.semaphore_wait(barrier, len(others))


def share(me, others, source, slots, send_sem, recv_sem):
    copies = []
    for device, index in others:
        copy = pltpu.make_async_remote_copy(src_ref=source, dst_ref=slots.at[me], send_sem=send_sem.at[index], recv_sem=recv_sem.at[me], device_id=device, device_id_type=MESH)
        copy.start()
        copies.append(copy)
    for device, index in others:
        pltpu.make_async_remote_copy(src_ref=source, dst_ref=slots.at[index], send_sem=send_sem.at[index], recv_sem=recv_sem.at[index], device_id=device, device_id_type=MESH).wait_recv()
    for copy in copies:
        copy.wait_send()


def exchange_kernel(sizes, groups, cols, grads, master, one_in, two_in, mean_ref, weight_ref, ring, clip_ref, stat_ref, land, own, part, slots,
                    send_sem, recv_sem, free_sem, own_sem, weight_sem, ring_sem, small_send, small_recv):
    model_size, data_size = sizes
    data = lax.axis_index('data')
    me, others = peers(model_size, data_size)
    peer = lax.rem(data + 1, data_size)
    peer_device = (lax.axis_index('model'), peer)
    per_group = cols // PART
    parts = groups * per_group

    def columns(index, base):
        return pl.ds(pl.multiple_of(base + lax.rem(index, per_group) * PART, PART), PART)

    def own_copy(index):
        slot = lax.rem(index, OWN_SLOTS)
        return pltpu.make_async_copy(grads.at[0, rows(index // per_group), columns(index, data * cols)], own.at[slot], own_sem.at[slot])

    def weight_copy(index):
        at = (rows(index // per_group), columns(index, 0))
        return pltpu.make_async_copy(master.at[at], weight_ref.at[at], weight_sem.at[index])

    def send_copy(index):
        slot = lax.rem(index, LAND_SLOTS)
        return pltpu.make_async_remote_copy(src_ref=grads.at[0, rows(index // per_group), columns(index, peer * cols)], dst_ref=land.at[slot],
                                            send_sem=send_sem.at[slot], recv_sem=recv_sem.at[slot], device_id=peer_device, device_id_type=MESH)

    def ring_copies(chunk):
        at = (rows(chunk // (cols // CHUNK)), pl.ds(pl.multiple_of(lax.rem(chunk, cols // CHUNK) * CHUNK, CHUNK), CHUNK))
        return (pltpu.make_async_copy(one_in.at[at], ring.at[0, chunk], ring_sem.at[0, chunk]), pltpu.make_async_copy(two_in.at[at], ring.at[1, chunk], ring_sem.at[1, chunk]))

    for index in range(OWN_SLOTS):
        own_copy(index).start()
        weight_copy(index).start()
    enter(others)
    for index in range(LAND_SLOTS):
        send_copy(index).start()
    lane_ids = lanes_of()
    width = 1024
    zero = jnp.zeros((GROUP, LANES), F32)

    def one_part(index, carry):
        total, stat = carry
        own_slot, land_slot = lax.rem(index, OWN_SLOTS), lax.rem(index, LAND_SLOTS)
        row_at = rows(index // per_group)
        col_at = lax.rem(index, per_group) * PART

        @pl.when(lax.rem(index, parts // RING) == 0)
        def _():
            for copy in ring_copies(index // (parts // RING)):
                copy.start()

        own_copy(index).wait()
        weight_copy(index).wait()
        send_copy(index).wait_recv()

        def piece(step, sums):
            grad_sum, weight_sum = sums
            near = pl.ds(pl.multiple_of(step * width, width), width)
            far = pl.ds(pl.multiple_of(col_at + step * width, width), width)
            mean = (own[own_slot, :, near].astype(F32) + land[land_slot, :, near].astype(F32)) * 0.5
            mean_ref[row_at, far] = mean
            weight = weight_ref[row_at, far]
            cuts = range(0, width, LANES)
            grad_sum += tree_sum([mean[:, at:at + LANES] * mean[:, at:at + LANES] for at in cuts])
            weight_sum += tree_sum([weight[:, at:at + LANES] * weight[:, at:at + LANES] for at in cuts])
            return grad_sum, weight_sum

        grad_sum, weight_sum = lax.fori_loop(0, PART // width, piece, (zero, zero), unroll=2)

        @pl.when(index + LAND_SLOTS < parts)
        def _():
            pl.semaphore_signal(free_sem, inc=1, device_id=peer_device, device_id_type=MESH)

        @pl.when(index + OWN_SLOTS < parts)
        def _():
            own_copy(index + OWN_SLOTS).start()
            weight_copy(index + OWN_SLOTS).start()

        send_copy(index).wait_send()

        @pl.when(index + LAND_SLOTS < parts)
        def _():
            pl.semaphore_wait(free_sem, 1)
            send_copy(index + LAND_SLOTS).start()

        return total + grad_sum, put_lane(stat, lane_ids, index // per_group, weight_sum)

    total, stat = lax.fori_loop(0, parts, one_part, (zero, zero))
    stat_ref[...] = stat
    part[...] = total
    slots[me] = part[...]
    share(me, others, part, slots, small_send, small_recv)
    whole = tree_sum([slots[index] for index in range(model_size * data_size)])
    whole = jnp.sum(jnp.sum(whole, axis=1, keepdims=True), axis=0, keepdims=True)
    whole = jnp.broadcast_to(whole, (GROUP, LANES))
    clip_ref[...] = jnp.minimum(1.0, MAX_NORM / jnp.sqrt(whole))

    def finish(chunk, carry):
        for copy in ring_copies(chunk):
            copy.wait()
        return carry

    lax.fori_loop(0, RING, finish, 0)


def moment_kernel(groups, cols, mean_in, weight_in, ring_in, clip, weight_stat, one_in, two_in, dir_ref, weight_ref, ring, one_out, two_out, stat_ref,
                  one_get, two_get, one_put, two_put):
    per_group = cols // CHUNK
    chunks = groups * per_group
    width = 1024
    lane_ids = lanes_of()

    def place(chunk):
        return rows(chunk // per_group), pl.ds(pl.multiple_of(lax.rem(chunk, per_group) * CHUNK, CHUNK), CHUNK)

    def gets(chunk):
        slot = lax.rem(chunk, RING)
        at = place(chunk)
        return (pltpu.make_async_copy(one_in.at[at], ring.at[0, slot], one_get.at[slot]), pltpu.make_async_copy(two_in.at[at], ring.at[1, slot], two_get.at[slot]))

    def puts(chunk):
        slot = lax.rem(chunk, RING)
        at = place(chunk)
        return (pltpu.make_async_copy(ring.at[0, slot], one_out.at[at], one_put.at[slot]), pltpu.make_async_copy(ring.at[1, slot], two_out.at[at], two_put.at[slot]))

    def start(copies):
        for copy in copies:
            copy.start()

    def wait(copies):
        for copy in copies:
            copy.wait()

    scale = clip[...]
    one_scale = (1.0 - BETA_ONE) * scale
    two_scale = (1.0 - BETA_TWO) * scale * scale
    ratio = CORR_TWO ** 0.5 / CORR_ONE
    floor = EPSILON * CORR_TWO ** 0.5

    def one_chunk(chunk, stat):
        slot = lax.rem(chunk, RING)
        row_at = rows(chunk // per_group)
        col_at = lax.rem(chunk, per_group) * CHUNK

        @pl.when(chunk >= RING)
        def _():
            wait(gets(chunk))

        def piece(index, total):
            squares = []
            for at in range(0, width, LANES):
                near = pl.ds(pl.multiple_of(index * width + at, LANES), LANES)
                far = pl.ds(pl.multiple_of(col_at + index * width + at, LANES), LANES)
                mean = dir_ref[row_at, far]
                new_one = BETA_ONE * ring[0, slot, :, near] + one_scale * mean
                new_two = BETA_TWO * ring[1, slot, :, near] + two_scale * mean * mean
                ring[0, slot, :, near] = new_one
                ring[1, slot, :, near] = new_two
                root = new_two * lax.rsqrt(jnp.maximum(new_two, TINY))
                direction = (new_one * ratio) / (root + floor) + WEIGHT_DECAY * weight_ref[row_at, far]
                dir_ref[row_at, far] = direction
                squares.append(direction * direction)
            return total + tree_sum(squares)

        total = lax.fori_loop(0, CHUNK // width, piece, jnp.zeros((GROUP, LANES), F32))
        start(puts(chunk))
        ahead = chunk + RING - LAG

        @pl.when(jnp.logical_and(ahead >= RING, ahead < chunks))
        def _():
            wait(puts(ahead - RING))
            start(gets(ahead))

        return put_lane(stat, lane_ids, chunk // per_group, total)

    stat_ref[0] = lax.fori_loop(0, chunks, one_chunk, jnp.zeros((GROUP, LANES), F32))
    stat_ref[1] = weight_stat[...]

    def finish(chunk, carry):
        wait(puts(chunk))
        return carry

    lax.fori_loop(chunks - RING, chunks, finish, 0)


def segment_sums(values):
    lane_ids = lanes_of()
    row_ids = lax.broadcasted_iota(jnp.int32, (GROUP, LANES), 0)
    kind = lax.rem(lane_ids, 3)
    first = jnp.where(kind == 0, 3, 4)
    second = jnp.where(kind == 0, 4, jnp.where(kind == 1, 7, 8))
    segment = jnp.where(row_ids < first, 0, jnp.where(row_ids < second, 1, 2))
    out = jnp.zeros((GROUP, LANES), F32)
    for index in range(3):
        inside = segment == index
        out = jnp.where(inside, jnp.sum(jnp.where(inside, values, 0.0), axis=0, keepdims=True), out)
    return out


def weight_kernel(sizes, groups, cols, direction, weight, stats, land, rate, slots, packed, send_sem, recv_sem, small_send, small_recv):
    model_size, data_size = sizes
    data = lax.axis_index('data')
    me, others = peers(model_size, data_size)
    peer_device = (lax.axis_index('model'), lax.rem(data + 1, data_size))
    enter(others)
    slots[me] = stats[...]
    share(me, others, stats, slots, small_send, small_recv)
    lane_ids = lanes_of()
    dir_sq = segment_sums(tree_sum([slots[index, 0] for index in range(model_size * data_size)]))
    weight_sq = segment_sums(tree_sum([slots[index, 1] for index in range(model_size * data_size)]))
    rate[...] = LEARN_RATE * (jnp.sqrt(weight_sq) / jnp.sqrt(dir_sq))
    width = 1024

    def send_copy(group):
        slot = lax.rem(group, SEND_SLOTS)
        return pltpu.make_async_remote_copy(src_ref=packed.at[slot], dst_ref=land.at[group], send_sem=send_sem.at[slot], recv_sem=recv_sem.at[group],
                                            device_id=peer_device, device_id_type=MESH)

    def one_group(group, carry):
        slot = lax.rem(group, SEND_SLOTS)

        @pl.when(group >= SEND_SLOTS)
        def _():
            send_copy(group - SEND_SLOTS).wait_send()

        group_rate = jnp.sum(jnp.where(lane_ids == group, rate[...], 0.0), axis=1, keepdims=True)

        def piece(index, inner):
            at = pl.ds(pl.multiple_of(index * width, width), width)
            packed[slot, :, at] = (weight[rows(group), at] - group_rate * direction[rows(group), at]).astype(BF16)
            return inner

        lax.fori_loop(0, cols // width, piece, 0, unroll=2)
        send_copy(group).start()
        return carry

    lax.fori_loop(0, groups, one_group, 0)

    def finish(group, carry):
        send_copy(group).wait_recv()
        return carry

    lax.fori_loop(0, groups, finish, 0)
    for group in range(groups - SEND_SLOTS, groups):
        send_copy(group).wait_send()


def write_kernel(sizes, groups, cols, direction, weight, land, rate, params, master, fresh, packed, master_sem, land_sem, own_sem):
    data_size = sizes[1]
    data = lax.axis_index('data')
    peer = lax.rem(data + 1, data_size)
    width = 1024
    lane_ids = lanes_of()
    per_group = cols // WRITE_CHUNK
    chunks = groups * per_group

    def columns(chunk, base):
        return pl.ds(pl.multiple_of(base + lax.rem(chunk, per_group) * WRITE_CHUNK, WRITE_CHUNK), WRITE_CHUNK)

    def puts(chunk):
        slot = lax.rem(chunk, WRITE_SLOTS)
        at = rows(chunk // per_group)
        return (pltpu.make_async_copy(fresh.at[slot], master.at[at, columns(chunk, 0)], master_sem.at[slot]),
                pltpu.make_async_copy(packed.at[slot], params.at[at, columns(chunk, data * cols)], own_sem.at[slot]))

    def land_copy(group):
        return pltpu.make_async_copy(land.at[group], params.at[rows(group), pl.ds(pl.multiple_of(peer * cols, LANES), cols)], land_sem.at[group])

    def one_chunk(chunk, carry):
        slot = lax.rem(chunk, WRITE_SLOTS)
        group = chunk // per_group

        @pl.when(lax.rem(chunk, per_group) == 0)
        def _():
            land_copy(group).start()

        @pl.when(chunk >= WRITE_SLOTS)
        def _():
            for copy in puts(chunk - WRITE_SLOTS):
                copy.wait()

        group_rate = jnp.sum(jnp.where(lane_ids == group, rate[...], 0.0), axis=1, keepdims=True)

        def piece(index, inner):
            near = pl.ds(pl.multiple_of(index * width, width), width)
            far = pl.ds(pl.multiple_of(lax.rem(chunk, per_group) * WRITE_CHUNK + index * width, width), width)
            new = weight[rows(group), far] - group_rate * direction[rows(group), far]
            fresh[slot, :, near] = new
            packed[slot, :, near] = new.astype(BF16)
            return inner

        lax.fori_loop(0, WRITE_CHUNK // width, piece, 0, unroll=2)
        for copy in puts(chunk):
            copy.start()
        return carry

    lax.fori_loop(0, chunks, one_chunk, 0)

    def finish(group, carry):
        land_copy(group).wait()
        return carry

    lax.fori_loop(0, groups, finish, 0)
    for chunk in range(chunks - WRITE_SLOTS, chunks):
        for copy in puts(chunk):
            copy.wait()


def solution(mesh):
    sizes = (mesh.shape['model'], mesh.shape['data'])
    devices = sizes[0] * sizes[1]
    both_axes = ('model', 'data')
    state_spec = P(None, both_axes)
    hbm = pl.BlockSpec(memory_space=pl.ANY)
    vmem = pl.BlockSpec(memory_space=pltpu.VMEM)
    dma = pltpu.SemaphoreType.DMA

    def device_step(local_grads, master, moment_one, moment_two):
        blocks, cols = master.shape
        groups = blocks // GROUP
        kept = pltpu.VMEM((blocks, cols), F32)
        keep = functools.partial(pltpu.with_memory_space_constraint, memory_space=pltpu.VMEM)
        tile = jax.ShapeDtypeStruct((GROUP, LANES), F32)
        state = jax.ShapeDtypeStruct((blocks, cols), F32)

        landed = pltpu.VMEM((groups, GROUP, cols), BF16)
        ring_shape = pltpu.VMEM((2, RING, GROUP, CHUNK), F32)
        landed = pltpu.VMEM((groups, GROUP, cols), BF16)
        parts = groups * (cols // PART)

        mean, weight, ring, clip, weight_stat = pl.pallas_call(
            functools.partial(exchange_kernel, sizes, groups, cols),
            out_shape=(kept, kept, ring_shape, tile, tile),
            in_specs=[hbm] * 4,
            out_specs=[vmem] * 5,
            scratch_shapes=[pltpu.VMEM((LAND_SLOTS, GROUP, PART), BF16), pltpu.VMEM((OWN_SLOTS, GROUP, PART), BF16), pltpu.VMEM((GROUP, LANES), F32), pltpu.VMEM((devices, GROUP, LANES), F32),
                            dma((LAND_SLOTS,)), dma((LAND_SLOTS,)), pltpu.SemaphoreType.REGULAR, dma((OWN_SLOTS,)), dma((parts,)), dma((2, RING)), dma((devices,)), dma((devices,))],
            compiler_params=pltpu.CompilerParams(collective_id=0, has_side_effects=True, vmem_limit_bytes=SCOPE),
            name='exchange',
        )(local_grads, master, moment_one, moment_two)

        direction, weight, _, new_one, new_two, stats = pl.pallas_call(
            functools.partial(moment_kernel, groups, cols),
            out_shape=(kept, kept, ring_shape, state, state, jax.ShapeDtypeStruct((2, GROUP, LANES), F32)),
            in_specs=[vmem] * 5 + [hbm] * 2,
            out_specs=[vmem, vmem, vmem, hbm, hbm, vmem],
            input_output_aliases={0: 0, 1: 1, 2: 2},
            scratch_shapes=[dma((RING,))] * 4,
            compiler_params=pltpu.CompilerParams(vmem_limit_bytes=SCOPE),
            name='moments',
        )(mean, weight, ring, clip, weight_stat, moment_one, moment_two)

        land, rate = pl.pallas_call(
            functools.partial(weight_kernel, sizes, groups, cols),
            out_shape=(landed, tile),
            in_specs=[vmem] * 3,
            out_specs=[vmem] * 2,
            scratch_shapes=[pltpu.VMEM((devices, 2, GROUP, LANES), F32), pltpu.VMEM((SEND_SLOTS, GROUP, cols), BF16),
                            dma((SEND_SLOTS,)), dma((groups,)), dma((devices,)), dma((devices,))],
            compiler_params=pltpu.CompilerParams(collective_id=1, has_side_effects=True, vmem_limit_bytes=SCOPE),
            name='weights',
        )(keep(direction), keep(weight), stats)

        params, new_master = pl.pallas_call(
            functools.partial(write_kernel, sizes, groups, cols),
            out_shape=(jax.ShapeDtypeStruct((blocks, sizes[1] * cols), BF16), state),
            in_specs=[vmem] * 4,
            out_specs=[hbm, hbm],
            scratch_shapes=[pltpu.VMEM((WRITE_SLOTS, GROUP, WRITE_CHUNK), F32), pltpu.VMEM((WRITE_SLOTS, GROUP, WRITE_CHUNK), BF16),
                            dma((WRITE_SLOTS,)), dma((groups,)), dma((WRITE_SLOTS,))],
            compiler_params=pltpu.CompilerParams(vmem_limit_bytes=SCOPE),
            name='write',
        )(keep(direction), keep(weight), keep(land), rate)
        return params, new_master, new_one, new_two

    return jax.shard_map(device_step, mesh=mesh, in_specs=(P('data', None, 'model'), state_spec, state_spec, state_spec),
                         out_specs=(P(None, 'model'), state_spec, state_spec, state_spec), check_vma=False)
```

```python
import functools

import jax
import jax.numpy as jnp
from jax import lax
from jax.experimental import pallas as pl
from jax.experimental.pallas import tpu as pltpu
from jax.sharding import PartitionSpec as P

STEP = 4
LEARN_RATE = 0.08
BETA_ONE = 0.9
BETA_TWO = 0.999
EPSILON = 1e-6
WEIGHT_DECAY = 0.01
MAX_NORM = 1.0
CORR_ONE = 1.0 - BETA_ONE ** STEP
CORR_TWO = 1.0 - BETA_TWO ** STEP
TINY = 1.2e-38

MESH = pl.DeviceIdType.MESH
F32 = jnp.float32
BF16 = jnp.bfloat16
SCOPE = 4000 << 10
LANES = 128
GROUP = 8

PART = 16384
LAND_SLOTS = 8
OWN_SLOTS = 6
RING = 24
LAG = 6
MOMENT_WIDTH = 2048
MEAN_WIDTH = 2048
CHUNK = 8192
SEND_SLOTS = 4
WRITE_SLOTS = 6
WRITE_CHUNK = 8192


def rows(group):
    return pl.ds(pl.multiple_of(group * GROUP, GROUP), GROUP)


def lanes_of():
    return lax.broadcasted_iota(jnp.int32, (GROUP, LANES), 1)


def put_lane(tile, lane_ids, lane, partial):
    row_sum = jnp.sum(partial, axis=1, keepdims=True)
    return tile + jnp.where(lane_ids == lane, row_sum, 0.0)


def tree_sum(values):
    while len(values) > 1:
        values = [a + b for a, b in zip(values[::2], values[1::2])] + ([values[-1]] if len(values) % 2 else [])
    return values[0]


def peers(model_size, data_size):
    model, data = lax.axis_index('model'), lax.axis_index('data')
    out = []
    for step in range(1, model_size * data_size):
        peer_model = lax.rem(model + step // data_size, model_size)
        peer_data = lax.rem(data + step % data_size, data_size)
        out.append(((peer_model, peer_data), peer_model * data_size + peer_data))
    return model * data_size + data, out


def enter(others):
    barrier = pltpu.get_barrier_semaphore()
    for device, _ in others:
        pl.semaphore_signal(barrier, inc=1, device_id=device, device_id_type=MESH)
    pl.semaphore_wait(barrier, len(others))


def share(me, others, source, slots, send_sem, recv_sem):
    copies = []
    for device, index in others:
        copy = pltpu.make_async_remote_copy(src_ref=source, dst_ref=slots.at[me], send_sem=send_sem.at[index], recv_sem=recv_sem.at[me], device_id=device, device_id_type=MESH)
        copy.start()
        copies.append(copy)
    for device, index in others:
        pltpu.make_async_remote_copy(src_ref=source, dst_ref=slots.at[index], send_sem=send_sem.at[index], recv_sem=recv_sem.at[index], device_id=device, device_id_type=MESH).wait_recv()
    for copy in copies:
        copy.wait_send()


def exchange_kernel(sizes, groups, cols, grads, master, one_in, two_in, mean_ref, weight_ref, ring, clip_ref, stat_ref, land, own, part, slots,
                    send_sem, recv_sem, free_sem, own_sem, weight_sem, ring_sem, small_send, small_recv):
    model_size, data_size = sizes
    data = lax.axis_index('data')
    me, others = peers(model_size, data_size)
    peer = lax.rem(data + 1, data_size)
    peer_device = (lax.axis_index('model'), peer)
    per_group = cols // PART
    parts = groups * per_group

    def columns(index, base):
        return pl.ds(pl.multiple_of(base + lax.rem(index, per_group) * PART, PART), PART)

    def own_copy(index):
        slot = lax.rem(index, OWN_SLOTS)
        return pltpu.make_async_copy(grads.at[0, rows(index // per_group), columns(index, data * cols)], own.at[slot], own_sem.at[slot])

    def weight_copy(index):
        at = (rows(index // per_group), columns(index, 0))
        return pltpu.make_async_copy(master.at[at], weight_ref.at[at], weight_sem.at[index])

    def send_copy(index):
        slot = lax.rem(index, LAND_SLOTS)
        return pltpu.make_async_remote_copy(src_ref=grads.at[0, rows(index // per_group), columns(index, peer * cols)], dst_ref=land.at[slot],
                                            send_sem=send_sem.at[slot], recv_sem=recv_sem.at[slot], device_id=peer_device, device_id_type=MESH)

    def ring_copies(chunk):
        at = (rows(chunk // (cols // CHUNK)), pl.ds(pl.multiple_of(lax.rem(chunk, cols // CHUNK) * CHUNK, CHUNK), CHUNK))
        return (pltpu.make_async_copy(one_in.at[at], ring.at[0, chunk], ring_sem.at[0, chunk]), pltpu.make_async_copy(two_in.at[at], ring.at[1, chunk], ring_sem.at[1, chunk]))

    for index in range(OWN_SLOTS):
        own_copy(index).start()
        weight_copy(index).start()
    enter(others)
    for index in range(LAND_SLOTS):
        send_copy(index).start()
    lane_ids = lanes_of()
    width = MEAN_WIDTH
    zero = jnp.zeros((GROUP, LANES), F32)

    def one_part(index, carry):
        total, stat = carry
        own_slot, land_slot = lax.rem(index, OWN_SLOTS), lax.rem(index, LAND_SLOTS)
        row_at = rows(index // per_group)
        col_at = lax.rem(index, per_group) * PART

        @pl.when(lax.rem(index, parts // RING) == 0)
        def _():
            for copy in ring_copies(index // (parts // RING)):
                copy.start()

        own_copy(index).wait()
        weight_copy(index).wait()
        send_copy(index).wait_recv()

        def piece(step, sums):
            grad_sum, weight_sum = sums
            near = pl.ds(pl.multiple_of(step * width, width), width)
            far = pl.ds(pl.multiple_of(col_at + step * width, width), width)
            weight = weight_ref[row_at, far]
            mean = (own[own_slot, :, near].astype(F32) + land[land_slot, :, near].astype(F32)) * 0.5
            mean_ref[row_at, far] = mean
            cuts = range(0, width, LANES)
            grad_sum += tree_sum([mean[:, at:at + LANES] * mean[:, at:at + LANES] for at in cuts])
            weight_sum += tree_sum([weight[:, at:at + LANES] * weight[:, at:at + LANES] for at in cuts])
            return grad_sum, weight_sum

        grad_sum, weight_sum = lax.fori_loop(0, PART // width, piece, (zero, zero))

        @pl.when(index + LAND_SLOTS < parts)
        def _():
            pl.semaphore_signal(free_sem, inc=1, device_id=peer_device, device_id_type=MESH)

        @pl.when(index + OWN_SLOTS < parts)
        def _():
            own_copy(index + OWN_SLOTS).start()
            weight_copy(index + OWN_SLOTS).start()

        send_copy(index).wait_send()

        @pl.when(index + LAND_SLOTS < parts)
        def _():
            pl.semaphore_wait(free_sem, 1)
            send_copy(index + LAND_SLOTS).start()

        return total + grad_sum, put_lane(stat, lane_ids, index // per_group, weight_sum)

    total, stat = lax.fori_loop(0, parts, one_part, (zero, zero))
    stat_ref[...] = stat
    part[...] = total
    slots[me] = part[...]
    share(me, others, part, slots, small_send, small_recv)
    whole = tree_sum([slots[index] for index in range(model_size * data_size)])
    whole = jnp.sum(jnp.sum(whole, axis=1, keepdims=True), axis=0, keepdims=True)
    whole = jnp.broadcast_to(whole, (GROUP, LANES))
    clip_ref[...] = jnp.minimum(1.0, MAX_NORM / jnp.sqrt(whole))

    def finish(chunk, carry):
        for copy in ring_copies(chunk):
            copy.wait()
        return carry

    lax.fori_loop(0, RING, finish, 0)


def moment_kernel(groups, cols, mean_in, weight_in, ring_in, clip, weight_stat, one_in, two_in, dir_ref, weight_ref, ring, one_out, two_out, stat_ref,
                  one_get, two_get, one_put, two_put):
    per_group = cols // CHUNK
    chunks = groups * per_group
    width = MOMENT_WIDTH
    lane_ids = lanes_of()

    def place(chunk):
        return rows(chunk // per_group), pl.ds(pl.multiple_of(lax.rem(chunk, per_group) * CHUNK, CHUNK), CHUNK)

    def gets(chunk):
        slot = lax.rem(chunk, RING)
        at = place(chunk)
        return (pltpu.make_async_copy(one_in.at[at], ring.at[0, slot], one_get.at[slot]), pltpu.make_async_copy(two_in.at[at], ring.at[1, slot], two_get.at[slot]))

    def puts(chunk):
        slot = lax.rem(chunk, RING)
        at = place(chunk)
        return (pltpu.make_async_copy(ring.at[0, slot], one_out.at[at], one_put.at[slot]), pltpu.make_async_copy(ring.at[1, slot], two_out.at[at], two_put.at[slot]))

    def start(copies):
        for copy in copies:
            copy.start()

    def wait(copies):
        for copy in copies:
            copy.wait()

    scale = jnp.concatenate([clip[...]] * (width // LANES), axis=1)
    one_scale = (1.0 - BETA_ONE) * scale
    two_scale = (1.0 - BETA_TWO) * scale * scale
    ratio = CORR_TWO ** 0.5 / CORR_ONE
    floor = EPSILON * CORR_TWO ** 0.5

    def one_chunk(chunk, stat):
        slot = lax.rem(chunk, RING)
        row_at = rows(chunk // per_group)
        col_at = lax.rem(chunk, per_group) * CHUNK

        @pl.when(chunk >= RING)
        def _():
            wait(gets(chunk))

        def piece(index, total):
            near = pl.ds(pl.multiple_of(index * width, width), width)
            far = pl.ds(pl.multiple_of(col_at + index * width, width), width)
            mean, weight = dir_ref[row_at, far], weight_ref[row_at, far]
            old_one, old_two = ring[0, slot, :, near], ring[1, slot, :, near]
            new_one = BETA_ONE * old_one + one_scale * mean
            new_two = BETA_TWO * old_two + two_scale * mean * mean
            root = new_two * lax.rsqrt(jnp.maximum(new_two, TINY))
            direction = (new_one * ratio) / (root + floor) + WEIGHT_DECAY * weight
            ring[0, slot, :, near] = new_one
            ring[1, slot, :, near] = new_two
            dir_ref[row_at, far] = direction
            return total + tree_sum([direction[:, at:at + LANES] * direction[:, at:at + LANES] for at in range(0, width, LANES)])

        total = lax.fori_loop(0, CHUNK // width, piece, jnp.zeros((GROUP, LANES), F32))
        start(puts(chunk))
        ahead = chunk + RING - LAG

        @pl.when(jnp.logical_and(ahead >= RING, ahead < chunks))
        def _():
            wait(puts(ahead - RING))
            start(gets(ahead))

        return put_lane(stat, lane_ids, chunk // per_group, total)

    stat_ref[0] = lax.fori_loop(0, chunks, one_chunk, jnp.zeros((GROUP, LANES), F32))
    stat_ref[1] = weight_stat[...]

    def finish(chunk, carry):
        wait(puts(chunk))
        return carry

    lax.fori_loop(chunks - RING, chunks, finish, 0)


def segment_sums(values):
    lane_ids = lanes_of()
    row_ids = lax.broadcasted_iota(jnp.int32, (GROUP, LANES), 0)
    kind = lax.rem(lane_ids, 3)
    first = jnp.where(kind == 0, 3, 4)
    second = jnp.where(kind == 0, 4, jnp.where(kind == 1, 7, 8))
    segment = jnp.where(row_ids < first, 0, jnp.where(row_ids < second, 1, 2))
    out = jnp.zeros((GROUP, LANES), F32)
    for index in range(3):
        inside = segment == index
        out = jnp.where(inside, jnp.sum(jnp.where(inside, values, 0.0), axis=0, keepdims=True), out)
    return out


def weight_kernel(sizes, groups, cols, direction, weight, stats, land, rate, slots, packed, send_sem, recv_sem, small_send, small_recv):
    model_size, data_size = sizes
    data = lax.axis_index('data')
    me, others = peers(model_size, data_size)
    peer_device = (lax.axis_index('model'), lax.rem(data + 1, data_size))
    enter(others)
    slots[me] = stats[...]
    share(me, others, stats, slots, small_send, small_recv)
    lane_ids = lanes_of()
    dir_sq = segment_sums(tree_sum([slots[index, 0] for index in range(model_size * data_size)]))
    weight_sq = segment_sums(tree_sum([slots[index, 1] for index in range(model_size * data_size)]))
    rate[...] = LEARN_RATE * (jnp.sqrt(weight_sq) / jnp.sqrt(dir_sq))
    width = 1024

    def send_copy(group):
        slot = lax.rem(group, SEND_SLOTS)
        return pltpu.make_async_remote_copy(src_ref=packed.at[slot], dst_ref=land.at[group], send_sem=send_sem.at[slot], recv_sem=recv_sem.at[group],
                                            device_id=peer_device, device_id_type=MESH)

    def one_group(group, carry):
        slot = lax.rem(group, SEND_SLOTS)

        @pl.when(group >= SEND_SLOTS)
        def _():
            send_copy(group - SEND_SLOTS).wait_send()

        group_rate = jnp.sum(jnp.where(lane_ids == group, rate[...], 0.0), axis=1, keepdims=True)

        def piece(index, inner):
            at = pl.ds(pl.multiple_of(index * width, width), width)
            packed[slot, :, at] = (weight[rows(group), at] - group_rate * direction[rows(group), at]).astype(BF16)
            return inner

        lax.fori_loop(0, cols // width, piece, 0, unroll=2)
        send_copy(group).start()
        return carry

    lax.fori_loop(0, groups, one_group, 0)

    def finish(group, carry):
        send_copy(group).wait_recv()
        return carry

    lax.fori_loop(0, groups, finish, 0)
    for group in range(groups - SEND_SLOTS, groups):
        send_copy(group).wait_send()


def write_kernel(sizes, groups, cols, direction, weight, land, rate, params, master, fresh, packed, master_sem, land_sem, own_sem):
    data_size = sizes[1]
    data = lax.axis_index('data')
    peer = lax.rem(data + 1, data_size)
    width = 1024
    lane_ids = lanes_of()
    per_group = cols // WRITE_CHUNK
    chunks = groups * per_group

    def columns(chunk, base):
        return pl.ds(pl.multiple_of(base + lax.rem(chunk, per_group) * WRITE_CHUNK, WRITE_CHUNK), WRITE_CHUNK)

    def puts(chunk):
        slot = lax.rem(chunk, WRITE_SLOTS)
        at = rows(chunk // per_group)
        return (pltpu.make_async_copy(fresh.at[slot], master.at[at, columns(chunk, 0)], master_sem.at[slot]),
                pltpu.make_async_copy(packed.at[slot], params.at[at, columns(chunk, data * cols)], own_sem.at[slot]))

    def land_copy(group):
        return pltpu.make_async_copy(land.at[group], params.at[rows(group), pl.ds(pl.multiple_of(peer * cols, LANES), cols)], land_sem.at[group])

    def one_chunk(chunk, carry):
        slot = lax.rem(chunk, WRITE_SLOTS)
        group = chunk // per_group

        @pl.when(lax.rem(chunk, per_group) == 0)
        def _():
            land_copy(group).start()

        @pl.when(chunk >= WRITE_SLOTS)
        def _():
            for copy in puts(chunk - WRITE_SLOTS):
                copy.wait()

        group_rate = jnp.sum(jnp.where(lane_ids == group, rate[...], 0.0), axis=1, keepdims=True)

        def piece(index, inner):
            near = pl.ds(pl.multiple_of(index * width, width), width)
            far = pl.ds(pl.multiple_of(lax.rem(chunk, per_group) * WRITE_CHUNK + index * width, width), width)
            new = weight[rows(group), far] - group_rate * direction[rows(group), far]
            fresh[slot, :, near] = new
            packed[slot, :, near] = new.astype(BF16)
            return inner

        lax.fori_loop(0, WRITE_CHUNK // width, piece, 0, unroll=2)
        for copy in puts(chunk):
            copy.start()
        return carry

    lax.fori_loop(0, chunks, one_chunk, 0)

    def finish(group, carry):
        land_copy(group).wait()
        return carry

    lax.fori_loop(0, groups, finish, 0)
    for chunk in range(chunks - WRITE_SLOTS, chunks):
        for copy in puts(chunk):
            copy.wait()


def solution(mesh):
    sizes = (mesh.shape['model'], mesh.shape['data'])
    devices = sizes[0] * sizes[1]
    both_axes = ('model', 'data')
    state_spec = P(None, both_axes)
    hbm = pl.BlockSpec(memory_space=pl.ANY)
    vmem = pl.BlockSpec(memory_space=pltpu.VMEM)
    dma = pltpu.SemaphoreType.DMA

    def device_step(local_grads, master, moment_one, moment_two):
        blocks, cols = master.shape
        groups = blocks // GROUP
        kept = pltpu.VMEM((blocks, cols), F32)
        keep = functools.partial(pltpu.with_memory_space_constraint, memory_space=pltpu.VMEM)
        tile = jax.ShapeDtypeStruct((GROUP, LANES), F32)
        state = jax.ShapeDtypeStruct((blocks, cols), F32)

        landed = pltpu.VMEM((groups, GROUP, cols), BF16)
        ring_shape = pltpu.VMEM((2, RING, GROUP, CHUNK), F32)
        landed = pltpu.VMEM((groups, GROUP, cols), BF16)
        parts = groups * (cols // PART)

        mean, weight, ring, clip, weight_stat = pl.pallas_call(
            functools.partial(exchange_kernel, sizes, groups, cols),
            out_shape=(kept, kept, ring_shape, tile, tile),
            in_specs=[hbm] * 4,
            out_specs=[vmem] * 5,
            scratch_shapes=[pltpu.VMEM((LAND_SLOTS, GROUP, PART), BF16), pltpu.VMEM((OWN_SLOTS, GROUP, PART), BF16), pltpu.VMEM((GROUP, LANES), F32), pltpu.VMEM((devices, GROUP, LANES), F32),
                            dma((LAND_SLOTS,)), dma((LAND_SLOTS,)), pltpu.SemaphoreType.REGULAR, dma((OWN_SLOTS,)), dma((parts,)), dma((2, RING)), dma((devices,)), dma((devices,))],
            compiler_params=pltpu.CompilerParams(collective_id=0, has_side_effects=True, vmem_limit_bytes=SCOPE),
            name='exchange',
        )(local_grads, master, moment_one, moment_two)

        direction, weight, _, new_one, new_two, stats = pl.pallas_call(
            functools.partial(moment_kernel, groups, cols),
            out_shape=(kept, kept, ring_shape, state, state, jax.ShapeDtypeStruct((2, GROUP, LANES), F32)),
            in_specs=[vmem] * 5 + [hbm] * 2,
            out_specs=[vmem, vmem, vmem, hbm, hbm, vmem],
            input_output_aliases={0: 0, 1: 1, 2: 2},
            scratch_shapes=[dma((RING,))] * 4,
            compiler_params=pltpu.CompilerParams(vmem_limit_bytes=SCOPE),
            name='moments',
        )(mean, weight, ring, clip, weight_stat, moment_one, moment_two)

        land, rate = pl.pallas_call(
            functools.partial(weight_kernel, sizes, groups, cols),
            out_shape=(landed, tile),
            in_specs=[vmem] * 3,
            out_specs=[vmem] * 2,
            scratch_shapes=[pltpu.VMEM((devices, 2, GROUP, LANES), F32), pltpu.VMEM((SEND_SLOTS, GROUP, cols), BF16),
                            dma((SEND_SLOTS,)), dma((groups,)), dma((devices,)), dma((devices,))],
            compiler_params=pltpu.CompilerParams(collective_id=1, has_side_effects=True, vmem_limit_bytes=SCOPE),
            name='weights',
        )(keep(direction), keep(weight), stats)

        params, new_master = pl.pallas_call(
            functools.partial(write_kernel, sizes, groups, cols),
            out_shape=(jax.ShapeDtypeStruct((blocks, sizes[1] * cols), BF16), state),
            in_specs=[vmem] * 4,
            out_specs=[hbm, hbm],
            scratch_shapes=[pltpu.VMEM((WRITE_SLOTS, GROUP, WRITE_CHUNK), F32), pltpu.VMEM((WRITE_SLOTS, GROUP, WRITE_CHUNK), BF16),
                            dma((WRITE_SLOTS,)), dma((groups,)), dma((WRITE_SLOTS,))],
            compiler_params=pltpu.CompilerParams(vmem_limit_bytes=SCOPE),
            name='write',
        )(keep(direction), keep(weight), keep(land), rate)
        return params, new_master, new_one, new_two

    return jax.shard_map(device_step, mesh=mesh, in_specs=(P('data', None, 'model'), state_spec, state_spec, state_spec),
                         out_specs=(P(None, 'model'), state_spec, state_spec, state_spec), check_vma=False)
```

```python
import functools

import jax
import jax.numpy as jnp
from jax import lax
from jax.experimental import pallas as pl
from jax.experimental.pallas import tpu as pltpu
from jax.sharding import PartitionSpec as P

STEP = 4
LEARN_RATE = 0.08
BETA_ONE = 0.9
BETA_TWO = 0.999
EPSILON = 1e-6
WEIGHT_DECAY = 0.01
MAX_NORM = 1.0
CORR_ONE = 1.0 - BETA_ONE ** STEP
CORR_TWO = 1.0 - BETA_TWO ** STEP
TINY = 1.2e-38

MESH = pl.DeviceIdType.MESH
F32 = jnp.float32
BF16 = jnp.bfloat16
SCOPE = 4000 << 10
LANES = 128
GROUP = 8

PART = 16384
LAND_SLOTS = 11
OWN_SLOTS = 4
EARLY = 16
RING = 24
LAG = 8
MOMENT_WIDTH = 2048
MEAN_WIDTH = 2048
CHUNK = 8192
SEND_SLOTS = 4
WRITE_SLOTS = 10
WRITE_CHUNK = 8192


def rows(group):
    return pl.ds(pl.multiple_of(group * GROUP, GROUP), GROUP)


def lanes_of():
    return lax.broadcasted_iota(jnp.int32, (GROUP, LANES), 1)


def put_lane(tile, lane_ids, lane, partial):
    row_sum = jnp.sum(partial, axis=1, keepdims=True)
    return tile + jnp.where(lane_ids == lane, row_sum, 0.0)


def tree_sum(values):
    while len(values) > 1:
        values = [a + b for a, b in zip(values[::2], values[1::2])] + ([values[-1]] if len(values) % 2 else [])
    return values[0]


def peers(model_size, data_size):
    model, data = lax.axis_index('model'), lax.axis_index('data')
    out = []
    for step in range(1, model_size * data_size):
        peer_model = lax.rem(model + step // data_size, model_size)
        peer_data = lax.rem(data + step % data_size, data_size)
        out.append(((peer_model, peer_data), peer_model * data_size + peer_data))
    return model * data_size + data, out


def enter(others):
    barrier = pltpu.get_barrier_semaphore()
    for device, _ in others:
        pl.semaphore_signal(barrier, inc=1, device_id=device, device_id_type=MESH)
    pl.semaphore_wait(barrier, len(others))


def share(me, others, source, slots, send_sem, recv_sem):
    copies = []
    for device, index in others:
        copy = pltpu.make_async_remote_copy(src_ref=source, dst_ref=slots.at[me], send_sem=send_sem.at[index], recv_sem=recv_sem.at[me], device_id=device, device_id_type=MESH)
        copy.start()
        copies.append(copy)
    for device, index in others:
        pltpu.make_async_remote_copy(src_ref=source, dst_ref=slots.at[index], send_sem=send_sem.at[index], recv_sem=recv_sem.at[index], device_id=device, device_id_type=MESH).wait_recv()
    for copy in copies:
        copy.wait_send()


def exchange_kernel(sizes, groups, cols, grads, master, one_in, two_in, mean_ref, weight_ref, ring, clip_ref, stat_ref, land, own, part, slots,
                    send_sem, recv_sem, free_sem, own_sem, weight_sem, ring_sem, small_send, small_recv):
    model_size, data_size = sizes
    data = lax.axis_index('data')
    me, others = peers(model_size, data_size)
    peer = lax.rem(data + 1, data_size)
    peer_device = (lax.axis_index('model'), peer)
    per_group = cols // PART
    parts = groups * per_group

    def columns(index, base):
        return pl.ds(pl.multiple_of(base + lax.rem(index, per_group) * PART, PART), PART)

    def own_copy(index):
        slot = lax.rem(index, OWN_SLOTS)
        return pltpu.make_async_copy(grads.at[0, rows(index // per_group), columns(index, data * cols)], own.at[slot], own_sem.at[slot])

    def weight_copy(index):
        at = (rows(index // per_group), columns(index, 0))
        return pltpu.make_async_copy(master.at[at], weight_ref.at[at], weight_sem.at[index])

    def send_copy(index):
        slot = lax.rem(index, LAND_SLOTS)
        return pltpu.make_async_remote_copy(src_ref=grads.at[0, rows(index // per_group), columns(index, peer * cols)], dst_ref=land.at[slot],
                                            send_sem=send_sem.at[slot], recv_sem=recv_sem.at[slot], device_id=peer_device, device_id_type=MESH)

    def ring_copies(chunk):
        at = (rows(chunk // (cols // CHUNK)), pl.ds(pl.multiple_of(lax.rem(chunk, cols // CHUNK) * CHUNK, CHUNK), CHUNK))
        return (pltpu.make_async_copy(one_in.at[at], ring.at[0, chunk], ring_sem.at[0, chunk]), pltpu.make_async_copy(two_in.at[at], ring.at[1, chunk], ring_sem.at[1, chunk]))

    for index in range(OWN_SLOTS):
        own_copy(index).start()
    enter(others)
    for index in range(LAND_SLOTS):
        send_copy(index).start()
    for index in range(OWN_SLOTS):
        weight_copy(index).start()
    lane_ids = lanes_of()
    width = MEAN_WIDTH
    zero = jnp.zeros((GROUP, LANES), F32)

    def one_part(index, carry):
        total, stat = carry
        own_slot, land_slot = lax.rem(index, OWN_SLOTS), lax.rem(index, LAND_SLOTS)
        row_at = rows(index // per_group)
        col_at = lax.rem(index, per_group) * PART

        @pl.when(lax.rem(index, parts // EARLY) == 0)
        def _():
            for copy in ring_copies(index // (parts // EARLY)):
                copy.start()

        own_copy(index).wait()
        weight_copy(index).wait()
        send_copy(index).wait_recv()

        def piece(step, sums):
            grad_sum, weight_sum = sums
            near = pl.ds(pl.multiple_of(step * width, width), width)
            far = pl.ds(pl.multiple_of(col_at + step * width, width), width)
            weight = weight_ref[row_at, far]
            mean = (own[own_slot, :, near].astype(F32) + land[land_slot, :, near].astype(F32)) * 0.5
            mean_ref[row_at, far] = mean
            cuts = range(0, width, LANES)
            grad_sum += tree_sum([mean[:, at:at + LANES] * mean[:, at:at + LANES] for at in cuts])
            weight_sum += tree_sum([weight[:, at:at + LANES] * weight[:, at:at + LANES] for at in cuts])
            return grad_sum, weight_sum

        grad_sum, weight_sum = lax.fori_loop(0, PART // width, piece, (zero, zero))

        @pl.when(index + LAND_SLOTS < parts)
        def _():
            pl.semaphore_signal(free_sem, inc=1, device_id=peer_device, device_id_type=MESH)

        @pl.when(index + OWN_SLOTS < parts)
        def _():
            own_copy(index + OWN_SLOTS).start()
            weight_copy(index + OWN_SLOTS).start()

        send_copy(index).wait_send()

        @pl.when(index + LAND_SLOTS < parts)
        def _():
            pl.semaphore_wait(free_sem, 1)
            send_copy(index + LAND_SLOTS).start()

        return total + grad_sum, put_lane(stat, lane_ids, index // per_group, weight_sum)

    total, stat = lax.fori_loop(0, parts, one_part, (zero, zero))
    stat_ref[...] = stat
    part[...] = total
    slots[me] = part[...]
    share(me, others, part, slots, small_send, small_recv)
    whole = tree_sum([slots[index] for index in range(model_size * data_size)])
    whole = jnp.sum(jnp.sum(whole, axis=1, keepdims=True), axis=0, keepdims=True)
    whole = jnp.broadcast_to(whole, (GROUP, LANES))
    clip_ref[...] = jnp.minimum(1.0, MAX_NORM / jnp.sqrt(whole))

    def finish(chunk, carry):
        for copy in ring_copies(chunk):
            copy.wait()
        return carry

    lax.fori_loop(0, EARLY, finish, 0)


def moment_kernel(groups, cols, mean_in, weight_in, ring_in, clip, weight_stat, one_in, two_in, dir_ref, weight_ref, ring, one_out, two_out, stat_ref,
                  one_get, two_get, one_put, two_put):
    per_group = cols // CHUNK
    chunks = groups * per_group
    width = MOMENT_WIDTH
    lane_ids = lanes_of()

    def place(chunk):
        return rows(chunk // per_group), pl.ds(pl.multiple_of(lax.rem(chunk, per_group) * CHUNK, CHUNK), CHUNK)

    def gets(chunk):
        slot = lax.rem(chunk, RING)
        at = place(chunk)
        return (pltpu.make_async_copy(one_in.at[at], ring.at[0, slot], one_get.at[slot]), pltpu.make_async_copy(two_in.at[at], ring.at[1, slot], two_get.at[slot]))

    def puts(chunk):
        slot = lax.rem(chunk, RING)
        at = place(chunk)
        return (pltpu.make_async_copy(ring.at[0, slot], one_out.at[at], one_put.at[slot]), pltpu.make_async_copy(ring.at[1, slot], two_out.at[at], two_put.at[slot]))

    def start(copies, priority=0):
        for copy in copies:
            copy.start(priority=priority)

    def wait(copies):
        for copy in copies:
            copy.wait()

    scale = jnp.concatenate([clip[...]] * (width // LANES), axis=1)
    one_scale = (1.0 - BETA_ONE) * scale
    two_scale = (1.0 - BETA_TWO) * scale * scale
    ratio = CORR_TWO ** 0.5 / CORR_ONE
    floor = EPSILON * CORR_TWO ** 0.5

    def begin(chunk, carry):
        start(gets(chunk))
        return carry

    lax.fori_loop(EARLY, RING - LAG, begin, 0)

    def one_chunk(chunk, stat):
        slot = lax.rem(chunk, RING)
        row_at = rows(chunk // per_group)
        col_at = lax.rem(chunk, per_group) * CHUNK

        @pl.when(chunk >= EARLY)
        def _():
            wait(gets(chunk))

        def piece(index, total):
            near = pl.ds(pl.multiple_of(index * width, width), width)
            far = pl.ds(pl.multiple_of(col_at + index * width, width), width)
            mean, weight = dir_ref[row_at, far], weight_ref[row_at, far]
            old_one, old_two = ring[0, slot, :, near], ring[1, slot, :, near]
            new_one = BETA_ONE * old_one + one_scale * mean
            new_two = BETA_TWO * old_two + two_scale * mean * mean
            root = new_two * lax.rsqrt(jnp.maximum(new_two, TINY))
            direction = (new_one * ratio) / (root + floor) + WEIGHT_DECAY * weight
            ring[0, slot, :, near] = new_one
            ring[1, slot, :, near] = new_two
            dir_ref[row_at, far] = direction
            return total + tree_sum([direction[:, at:at + LANES] * direction[:, at:at + LANES] for at in range(0, width, LANES)])

        total = lax.fori_loop(0, CHUNK // width, piece, jnp.zeros((GROUP, LANES), F32))
        start(puts(chunk), priority=1)
        ahead = chunk + RING - LAG

        @pl.when(jnp.logical_and(ahead >= RING, ahead < chunks))
        def _():
            wait(puts(ahead - RING))

        @pl.when(ahead < chunks)
        def _():
            start(gets(ahead))

        return put_lane(stat, lane_ids, chunk // per_group, total)

    stat_ref[0] = lax.fori_loop(0, chunks, one_chunk, jnp.zeros((GROUP, LANES), F32))
    stat_ref[1] = weight_stat[...]

    def finish(chunk, carry):
        wait(puts(chunk))
        return carry

    lax.fori_loop(chunks - RING, chunks, finish, 0)


def segment_sums(values):
    lane_ids = lanes_of()
    row_ids = lax.broadcasted_iota(jnp.int32, (GROUP, LANES), 0)
    kind = lax.rem(lane_ids, 3)
    first = jnp.where(kind == 0, 3, 4)
    second = jnp.where(kind == 0, 4, jnp.where(kind == 1, 7, 8))
    segment = jnp.where(row_ids < first, 0, jnp.where(row_ids < second, 1, 2))
    out = jnp.zeros((GROUP, LANES), F32)
    for index in range(3):
        inside = segment == index
        out = jnp.where(inside, jnp.sum(jnp.where(inside, values, 0.0), axis=0, keepdims=True), out)
    return out


def weight_kernel(sizes, groups, cols, direction, weight, stats, land, rate, slots, packed, send_sem, recv_sem, small_send, small_recv):
    model_size, data_size = sizes
    data = lax.axis_index('data')
    me, others = peers(model_size, data_size)
    peer_device = (lax.axis_index('model'), lax.rem(data + 1, data_size))
    enter(others)
    slots[me] = stats[...]
    share(me, others, stats, slots, small_send, small_recv)
    lane_ids = lanes_of()
    dir_sq = segment_sums(tree_sum([slots[index, 0] for index in range(model_size * data_size)]))
    weight_sq = segment_sums(tree_sum([slots[index, 1] for index in range(model_size * data_size)]))
    rate[...] = LEARN_RATE * (jnp.sqrt(weight_sq) / jnp.sqrt(dir_sq))
    width = 1024

    def send_copy(group):
        slot = lax.rem(group, SEND_SLOTS)
        return pltpu.make_async_remote_copy(src_ref=packed.at[slot], dst_ref=land.at[group], send_sem=send_sem.at[slot], recv_sem=recv_sem.at[group],
                                            device_id=peer_device, device_id_type=MESH)

    def one_group(group, carry):
        slot = lax.rem(group, SEND_SLOTS)

        @pl.when(group >= SEND_SLOTS)
        def _():
            send_copy(group - SEND_SLOTS).wait_send()

        group_rate = jnp.sum(jnp.where(lane_ids == group, rate[...], 0.0), axis=1, keepdims=True)

        def piece(index, inner):
            at = pl.ds(pl.multiple_of(index * width, width), width)
            packed[slot, :, at] = (weight[rows(group), at] - group_rate * direction[rows(group), at]).astype(BF16)
            return inner

        lax.fori_loop(0, cols // width, piece, 0, unroll=2)
        send_copy(group).start()
        return carry

    lax.fori_loop(0, groups, one_group, 0)

    def finish(group, carry):
        send_copy(group).wait_recv()
        return carry

    lax.fori_loop(0, groups, finish, 0)
    for group in range(groups - SEND_SLOTS, groups):
        send_copy(group).wait_send()


def write_kernel(sizes, groups, cols, direction, weight, land, rate, params, master, fresh, packed, master_sem, land_sem, own_sem):
    data_size = sizes[1]
    data = lax.axis_index('data')
    peer = lax.rem(data + 1, data_size)
    width = 1024
    lane_ids = lanes_of()
    per_group = cols // WRITE_CHUNK
    chunks = groups * per_group

    def columns(chunk, base):
        return pl.ds(pl.multiple_of(base + lax.rem(chunk, per_group) * WRITE_CHUNK, WRITE_CHUNK), WRITE_CHUNK)

    def puts(chunk):
        slot = lax.rem(chunk, WRITE_SLOTS)
        at = rows(chunk // per_group)
        return (pltpu.make_async_copy(fresh.at[slot], master.at[at, columns(chunk, 0)], master_sem.at[slot]),
                pltpu.make_async_copy(packed.at[slot], params.at[at, columns(chunk, data * cols)], own_sem.at[slot]))

    def land_copy(group):
        return pltpu.make_async_copy(land.at[group], params.at[rows(group), pl.ds(pl.multiple_of(peer * cols, LANES), cols)], land_sem.at[group])

    def one_chunk(chunk, carry):
        slot = lax.rem(chunk, WRITE_SLOTS)
        group = chunk // per_group

        @pl.when(chunk >= WRITE_SLOTS)
        def _():
            for copy in puts(chunk - WRITE_SLOTS):
                copy.wait()

        group_rate = jnp.sum(jnp.where(lane_ids == group, rate[...], 0.0), axis=1, keepdims=True)

        def piece(index, inner):
            near = pl.ds(pl.multiple_of(index * width, width), width)
            far = pl.ds(pl.multiple_of(lax.rem(chunk, per_group) * WRITE_CHUNK + index * width, width), width)
            new = weight[rows(group), far] - group_rate * direction[rows(group), far]
            fresh[slot, :, near] = new
            packed[slot, :, near] = new.astype(BF16)
            return inner

        lax.fori_loop(0, WRITE_CHUNK // width, piece, 0, unroll=2)
        for copy in puts(chunk):
            copy.start()
        return carry

    def begin(group, carry):
        land_copy(group).start(priority=1)
        return carry

    lax.fori_loop(0, groups, begin, 0)
    lax.fori_loop(0, chunks, one_chunk, 0)

    def finish(group, carry):
        land_copy(group).wait()
        return carry

    lax.fori_loop(0, groups, finish, 0)
    for chunk in range(chunks - WRITE_SLOTS, chunks):
        for copy in puts(chunk):
            copy.wait()


def solution(mesh):
    sizes = (mesh.shape['model'], mesh.shape['data'])
    devices = sizes[0] * sizes[1]
    both_axes = ('model', 'data')
    state_spec = P(None, both_axes)
    hbm = pl.BlockSpec(memory_space=pl.ANY)
    vmem = pl.BlockSpec(memory_space=pltpu.VMEM)
    dma = pltpu.SemaphoreType.DMA

    def device_step(local_grads, master, moment_one, moment_two):
        blocks, cols = master.shape
        groups = blocks // GROUP
        kept = pltpu.VMEM((blocks, cols), F32)
        keep = functools.partial(pltpu.with_memory_space_constraint, memory_space=pltpu.VMEM)
        tile = jax.ShapeDtypeStruct((GROUP, LANES), F32)
        state = jax.ShapeDtypeStruct((blocks, cols), F32)

        landed = pltpu.VMEM((groups, GROUP, cols), BF16)
        ring_shape = pltpu.VMEM((2, RING, GROUP, CHUNK), F32)
        landed = pltpu.VMEM((groups, GROUP, cols), BF16)
        parts = groups * (cols // PART)

        mean, weight, ring, clip, weight_stat = pl.pallas_call(
            functools.partial(exchange_kernel, sizes, groups, cols),
            out_shape=(kept, kept, ring_shape, tile, tile),
            in_specs=[hbm] * 4,
            out_specs=[vmem] * 5,
            scratch_shapes=[pltpu.VMEM((LAND_SLOTS, GROUP, PART), BF16), pltpu.VMEM((OWN_SLOTS, GROUP, PART), BF16), pltpu.VMEM((GROUP, LANES), F32), pltpu.VMEM((devices, GROUP, LANES), F32),
                            dma((LAND_SLOTS,)), dma((LAND_SLOTS,)), pltpu.SemaphoreType.REGULAR, dma((OWN_SLOTS,)), dma((parts,)), dma((2, EARLY)), dma((devices,)), dma((devices,))],
            compiler_params=pltpu.CompilerParams(collective_id=0, has_side_effects=True, vmem_limit_bytes=SCOPE),
            name='exchange',
        )(local_grads, master, moment_one, moment_two)

        direction, weight, _, new_one, new_two, stats = pl.pallas_call(
            functools.partial(moment_kernel, groups, cols),
            out_shape=(kept, kept, ring_shape, state, state, jax.ShapeDtypeStruct((2, GROUP, LANES), F32)),
            in_specs=[vmem] * 5 + [hbm] * 2,
            out_specs=[vmem, vmem, vmem, hbm, hbm, vmem],
            input_output_aliases={0: 0, 1: 1, 2: 2},
            scratch_shapes=[dma((RING,))] * 4,
            compiler_params=pltpu.CompilerParams(vmem_limit_bytes=SCOPE),
            name='moments',
        )(mean, weight, ring, clip, weight_stat, moment_one, moment_two)

        land, rate = pl.pallas_call(
            functools.partial(weight_kernel, sizes, groups, cols),
            out_shape=(landed, tile),
            in_specs=[vmem] * 3,
            out_specs=[vmem] * 2,
            scratch_shapes=[pltpu.VMEM((devices, 2, GROUP, LANES), F32), pltpu.VMEM((SEND_SLOTS, GROUP, cols), BF16),
                            dma((SEND_SLOTS,)), dma((groups,)), dma((devices,)), dma((devices,))],
            compiler_params=pltpu.CompilerParams(collective_id=1, has_side_effects=True, vmem_limit_bytes=SCOPE),
            name='weights',
        )(keep(direction), keep(weight), stats)

        params, new_master = pl.pallas_call(
            functools.partial(write_kernel, sizes, groups, cols),
            out_shape=(jax.ShapeDtypeStruct((blocks, sizes[1] * cols), BF16), state),
            in_specs=[vmem] * 4,
            out_specs=[hbm, hbm],
            scratch_shapes=[pltpu.VMEM((WRITE_SLOTS, GROUP, WRITE_CHUNK), F32), pltpu.VMEM((WRITE_SLOTS, GROUP, WRITE_CHUNK), BF16),
                            dma((WRITE_SLOTS,)), dma((groups,)), dma((WRITE_SLOTS,))],
            compiler_params=pltpu.CompilerParams(vmem_limit_bytes=SCOPE),
            name='write',
        )(keep(direction), keep(weight), keep(land), rate)
        return params, new_master, new_one, new_two

    return jax.shard_map(device_step, mesh=mesh, in_specs=(P('data', None, 'model'), state_spec, state_spec, state_spec),
                         out_specs=(P(None, 'model'), state_spec, state_spec, state_spec), check_vma=False)
```

```python
import functools

import jax
import jax.numpy as jnp
from jax import lax
from jax.experimental import pallas as pl
from jax.experimental.pallas import tpu as pltpu
from jax.sharding import PartitionSpec as P

STEP = 4
LEARN_RATE = 0.08
BETA_ONE = 0.9
BETA_TWO = 0.999
EPSILON = 1e-6
WEIGHT_DECAY = 0.01
MAX_NORM = 1.0
CORR_ONE = 1.0 - BETA_ONE ** STEP
CORR_TWO = 1.0 - BETA_TWO ** STEP
TINY = 1.2e-38

MESH = pl.DeviceIdType.MESH
F32 = jnp.float32
BF16 = jnp.bfloat16
SCOPE = 4000 << 10
LANES = 128
GROUP = 8

PART = 16384
AHEAD = 4
LAND_SLOTS = 8
STAGE_SLOTS = 9
OWN_SLOTS = 6
RING = 20
LAG = 7
MOMENT_WIDTH = 2048
MEAN_WIDTH = 2048
CHUNK = 8192
SEND_SLOTS = 4
WRITE_SLOTS = 5
WRITE_CHUNK = 16384


def rows(group):
    return pl.ds(pl.multiple_of(group * GROUP, GROUP), GROUP)


def lanes_of():
    return lax.broadcasted_iota(jnp.int32, (GROUP, LANES), 1)


def put_lane(tile, lane_ids, lane, partial):
    row_sum = jnp.sum(partial, axis=1, keepdims=True)
    return tile + jnp.where(lane_ids == lane, row_sum, 0.0)


def tree_sum(values):
    while len(values) > 1:
        values = [a + b for a, b in zip(values[::2], values[1::2])] + ([values[-1]] if len(values) % 2 else [])
    return values[0]


def peers(model_size, data_size):
    model, data = lax.axis_index('model'), lax.axis_index('data')
    out = []
    for step in range(1, model_size * data_size):
        peer_model = lax.rem(model + step // data_size, model_size)
        peer_data = lax.rem(data + step % data_size, data_size)
        out.append(((peer_model, peer_data), peer_model * data_size + peer_data))
    return model * data_size + data, out


def enter(others):
    barrier = pltpu.get_barrier_semaphore()
    for device, _ in others:
        pl.semaphore_signal(barrier, inc=1, device_id=device, device_id_type=MESH)
    pl.semaphore_wait(barrier, len(others))


def share(me, others, source, slots, send_sem, recv_sem):
    copies = []
    for device, index in others:
        copy = pltpu.make_async_remote_copy(src_ref=source, dst_ref=slots.at[me], send_sem=send_sem.at[index], recv_sem=recv_sem.at[me], device_id=device, device_id_type=MESH)
        copy.start()
        copies.append(copy)
    for device, index in others:
        pltpu.make_async_remote_copy(src_ref=source, dst_ref=slots.at[index], send_sem=send_sem.at[index], recv_sem=recv_sem.at[index], device_id=device, device_id_type=MESH).wait_recv()
    for copy in copies:
        copy.wait_send()


def exchange_kernel(sizes, groups, cols, grads, master, one_in, two_in, mean_ref, weight_ref, ring, land, clip_ref, stat_ref, stage, own, part, slots,
                    stage_sem, send_sem, recv_sem, free_sem, own_sem, weight_sem, ring_sem, small_send, small_recv):
    model_size, data_size = sizes
    data = lax.axis_index('data')
    me, others = peers(model_size, data_size)
    peer = lax.rem(data + 1, data_size)
    peer_device = (lax.axis_index('model'), peer)
    per_group = cols // PART
    parts = groups * per_group

    def columns(index, base):
        return pl.ds(pl.multiple_of(base + lax.rem(index, per_group) * PART, PART), PART)

    def own_copy(index):
        slot = lax.rem(index, OWN_SLOTS)
        return pltpu.make_async_copy(grads.at[0, rows(index // per_group), columns(index, data * cols)], own.at[slot], own_sem.at[slot])

    def weight_copy(index):
        at = (rows(index // per_group), columns(index, 0))
        return pltpu.make_async_copy(master.at[at], weight_ref.at[at], weight_sem.at[index])

    def stage_copy(index):
        slot = lax.rem(index, STAGE_SLOTS)
        return pltpu.make_async_copy(grads.at[0, rows(index // per_group), columns(index, peer * cols)], stage.at[slot], stage_sem.at[slot])

    def send_copy(index):
        from_slot, to_slot = lax.rem(index, STAGE_SLOTS), lax.rem(index, LAND_SLOTS)
        return pltpu.make_async_remote_copy(src_ref=stage.at[from_slot], dst_ref=land.at[to_slot], send_sem=send_sem.at[from_slot], recv_sem=recv_sem.at[to_slot],
                                            device_id=peer_device, device_id_type=MESH)

    def ring_copies(chunk):
        at = (rows(chunk // (cols // CHUNK)), pl.ds(pl.multiple_of(lax.rem(chunk, cols // CHUNK) * CHUNK, CHUNK), CHUNK))
        return (pltpu.make_async_copy(one_in.at[at], ring.at[0, chunk], ring_sem.at[0, chunk]), pltpu.make_async_copy(two_in.at[at], ring.at[1, chunk], ring_sem.at[1, chunk]))

    def begin_stage(index, carry):
        stage_copy(index).start()
        return carry

    def begin_own(index, carry):
        own_copy(index).start()
        weight_copy(index).start()
        return carry

    def begin_send(index, carry):
        stage_copy(index).wait()
        send_copy(index).start()
        return carry

    lax.fori_loop(0, STAGE_SLOTS, begin_stage, 0)
    lax.fori_loop(0, OWN_SLOTS, begin_own, 0)
    enter(others)
    lax.fori_loop(0, AHEAD, begin_send, 0)
    lane_ids = lanes_of()
    width = MEAN_WIDTH
    zero = jnp.zeros((GROUP, LANES), F32)
    first_ring = parts - RING // 2

    def one_part(index, carry):
        total, stat = carry
        own_slot, land_slot = lax.rem(index, OWN_SLOTS), lax.rem(index, LAND_SLOTS)
        row_at = rows(index // per_group)
        col_at = lax.rem(index, per_group) * PART

        @pl.when(jnp.logical_and(index + AHEAD >= LAND_SLOTS, index + AHEAD < parts))
        def _():
            pl.semaphore_wait(free_sem, 1)

        @pl.when(index + AHEAD < parts)
        def _():
            begin_send(index + AHEAD, 0)

        own_copy(index).wait()
        weight_copy(index).wait()
        send_copy(index).wait_recv()

        def piece(step, sums):
            grad_sum, weight_sum = sums
            near = pl.ds(pl.multiple_of(step * width, width), width)
            far = pl.ds(pl.multiple_of(col_at + step * width, width), width)
            weight = weight_ref[row_at, far]
            mean = (own[own_slot, :, near].astype(F32) + land[land_slot, :, near].astype(F32)) * 0.5
            mean_ref[row_at, far] = mean
            cuts = range(0, width, LANES)
            grad_sum += tree_sum([mean[:, at:at + LANES] * mean[:, at:at + LANES] for at in cuts])
            weight_sum += tree_sum([weight[:, at:at + LANES] * weight[:, at:at + LANES] for at in cuts])
            return grad_sum, weight_sum

        grad_sum, weight_sum = lax.fori_loop(0, PART // width, piece, (zero, zero))

        @pl.when(index + LAND_SLOTS < parts)
        def _():
            pl.semaphore_signal(free_sem, inc=1, device_id=peer_device, device_id_type=MESH)

        @pl.when(index + OWN_SLOTS < parts)
        def _():
            begin_own(index + OWN_SLOTS, 0)

        send_copy(index).wait_send()

        @pl.when(index + STAGE_SLOTS < parts)
        def _():
            begin_stage(index + STAGE_SLOTS, 0)

        @pl.when(index >= first_ring)
        def _():
            for late in range(2):
                for copy in ring_copies((index - first_ring) * 2 + late):
                    copy.start()

        return total + grad_sum, put_lane(stat, lane_ids, index // per_group, weight_sum)

    total, stat = lax.fori_loop(0, parts, one_part, (zero, zero))
    stat_ref[...] = stat
    part[...] = total
    slots[me] = part[...]
    share(me, others, part, slots, small_send, small_recv)
    whole = tree_sum([slots[index] for index in range(model_size * data_size)])
    whole = jnp.sum(jnp.sum(whole, axis=1, keepdims=True), axis=0, keepdims=True)
    whole = jnp.broadcast_to(whole, (GROUP, LANES))
    clip_ref[...] = jnp.minimum(1.0, MAX_NORM / jnp.sqrt(whole))

    def finish(chunk, carry):
        for copy in ring_copies(chunk):
            copy.wait()
        return carry

    lax.fori_loop(0, RING, finish, 0)


def moment_kernel(groups, cols, mean_in, weight_in, ring_in, land_in, clip, weight_stat, one_in, two_in, dir_ref, weight_ref, ring, land, one_out, two_out, stat_ref,
                  one_get, two_get, one_put, two_put):
    per_group = cols // CHUNK
    chunks = groups * per_group
    width = MOMENT_WIDTH
    lane_ids = lanes_of()

    def place(chunk):
        return rows(chunk // per_group), pl.ds(pl.multiple_of(lax.rem(chunk, per_group) * CHUNK, CHUNK), CHUNK)

    def gets(chunk):
        slot = lax.rem(chunk, RING)
        at = place(chunk)
        return (pltpu.make_async_copy(one_in.at[at], ring.at[0, slot], one_get.at[slot]), pltpu.make_async_copy(two_in.at[at], ring.at[1, slot], two_get.at[slot]))

    def puts(chunk):
        slot = lax.rem(chunk, RING)
        at = place(chunk)
        return (pltpu.make_async_copy(ring.at[0, slot], one_out.at[at], one_put.at[slot]), pltpu.make_async_copy(ring.at[1, slot], two_out.at[at], two_put.at[slot]))

    def start(copies, priority=0):
        for copy in copies:
            copy.start(priority=priority)

    def wait(copies):
        for copy in copies:
            copy.wait()

    scale = jnp.concatenate([clip[...]] * (width // LANES), axis=1)
    one_scale = (1.0 - BETA_ONE) * scale
    two_scale = (1.0 - BETA_TWO) * scale * scale
    ratio = CORR_TWO ** 0.5 / CORR_ONE
    floor = EPSILON * CORR_TWO ** 0.5

    def one_chunk(chunk, stat):
        slot = lax.rem(chunk, RING)
        row_at = rows(chunk // per_group)
        col_at = lax.rem(chunk, per_group) * CHUNK

        @pl.when(chunk >= RING)
        def _():
            wait(gets(chunk))

        def piece(index, total):
            near = pl.ds(pl.multiple_of(index * width, width), width)
            far = pl.ds(pl.multiple_of(col_at + index * width, width), width)
            mean, weight = dir_ref[row_at, far], weight_ref[row_at, far]
            old_one, old_two = ring[0, slot, :, near], ring[1, slot, :, near]
            new_one = BETA_ONE * old_one + one_scale * mean
            new_two = BETA_TWO * old_two + two_scale * mean * mean
            root = new_two * lax.rsqrt(jnp.maximum(new_two, TINY))
            direction = (new_one * ratio) / (root + floor) + WEIGHT_DECAY * weight
            ring[0, slot, :, near] = new_one
            ring[1, slot, :, near] = new_two
            dir_ref[row_at, far] = direction
            return total + tree_sum([direction[:, at:at + LANES] * direction[:, at:at + LANES] for at in range(0, width, LANES)])

        total = lax.fori_loop(0, CHUNK // width, piece, jnp.zeros((GROUP, LANES), F32))
        start(puts(chunk), priority=1)
        ahead = chunk + RING - LAG

        @pl.when(jnp.logical_and(ahead >= RING, ahead < chunks))
        def _():
            wait(puts(ahead - RING))
            start(gets(ahead))

        return put_lane(stat, lane_ids, chunk // per_group, total)

    stat_ref[0] = lax.fori_loop(0, chunks, one_chunk, jnp.zeros((GROUP, LANES), F32))
    stat_ref[1] = weight_stat[...]

    def finish(chunk, carry):
        wait(puts(chunk))
        return carry

    lax.fori_loop(chunks - RING, chunks, finish, 0)


def segment_sums(values):
    lane_ids = lanes_of()
    row_ids = lax.broadcasted_iota(jnp.int32, (GROUP, LANES), 0)
    kind = lax.rem(lane_ids, 3)
    first = jnp.where(kind == 0, 3, 4)
    second = jnp.where(kind == 0, 4, jnp.where(kind == 1, 7, 8))
    segment = jnp.where(row_ids < first, 0, jnp.where(row_ids < second, 1, 2))
    out = jnp.zeros((GROUP, LANES), F32)
    for index in range(3):
        inside = segment == index
        out = jnp.where(inside, jnp.sum(jnp.where(inside, values, 0.0), axis=0, keepdims=True), out)
    return out


def weight_kernel(sizes, groups, cols, direction, weight, stats, land, rate, slots, packed, send_sem, recv_sem, small_send, small_recv):
    model_size, data_size = sizes
    data = lax.axis_index('data')
    me, others = peers(model_size, data_size)
    peer_device = (lax.axis_index('model'), lax.rem(data + 1, data_size))
    enter(others)
    slots[me] = stats[...]
    share(me, others, stats, slots, small_send, small_recv)
    lane_ids = lanes_of()
    dir_sq = segment_sums(tree_sum([slots[index, 0] for index in range(model_size * data_size)]))
    weight_sq = segment_sums(tree_sum([slots[index, 1] for index in range(model_size * data_size)]))
    rate[...] = LEARN_RATE * (jnp.sqrt(weight_sq) / jnp.sqrt(dir_sq))
    width = 1024

    def send_copy(group):
        slot = lax.rem(group, SEND_SLOTS)
        return pltpu.make_async_remote_copy(src_ref=packed.at[slot], dst_ref=land.at[group], send_sem=send_sem.at[slot], recv_sem=recv_sem.at[group],
                                            device_id=peer_device, device_id_type=MESH)

    def one_group(group, carry):
        slot = lax.rem(group, SEND_SLOTS)

        @pl.when(group >= SEND_SLOTS)
        def _():
            send_copy(group - SEND_SLOTS).wait_send()

        group_rate = jnp.sum(jnp.where(lane_ids == group, rate[...], 0.0), axis=1, keepdims=True)

        def piece(index, inner):
            at = pl.ds(pl.multiple_of(index * width, width), width)
            packed[slot, :, at] = (weight[rows(group), at] - group_rate * direction[rows(group), at]).astype(BF16)
            return inner

        lax.fori_loop(0, cols // width, piece, 0, unroll=2)
        send_copy(group).start()
        return carry

    lax.fori_loop(0, groups, one_group, 0)

    def finish(group, carry):
        send_copy(group).wait_recv()
        return carry

    lax.fori_loop(0, groups, finish, 0)
    for group in range(groups - SEND_SLOTS, groups):
        send_copy(group).wait_send()


def write_kernel(sizes, groups, cols, direction, weight, land, rate, params, master, fresh, packed, master_sem, land_sem, own_sem):
    data_size = sizes[1]
    data = lax.axis_index('data')
    peer = lax.rem(data + 1, data_size)
    width = 1024
    lane_ids = lanes_of()
    per_group = cols // WRITE_CHUNK
    chunks = groups * per_group

    def columns(chunk, base):
        return pl.ds(pl.multiple_of(base + lax.rem(chunk, per_group) * WRITE_CHUNK, WRITE_CHUNK), WRITE_CHUNK)

    def puts(chunk):
        slot = lax.rem(chunk, WRITE_SLOTS)
        at = rows(chunk // per_group)
        return (pltpu.make_async_copy(fresh.at[slot], master.at[at, columns(chunk, 0)], master_sem.at[slot]),
                pltpu.make_async_copy(packed.at[slot], params.at[at, columns(chunk, data * cols)], own_sem.at[slot]))

    def land_copy(group):
        return pltpu.make_async_copy(land.at[group], params.at[rows(group), pl.ds(pl.multiple_of(peer * cols, LANES), cols)], land_sem.at[group])

    def one_chunk(chunk, carry):
        slot = lax.rem(chunk, WRITE_SLOTS)
        group = chunk // per_group

        @pl.when(lax.rem(chunk, per_group) == 0)
        def _():
            land_copy(group).start()

        @pl.when(chunk >= WRITE_SLOTS)
        def _():
            for copy in puts(chunk - WRITE_SLOTS):
                copy.wait()

        group_rate = jnp.sum(jnp.where(lane_ids == group, rate[...], 0.0), axis=1, keepdims=True)

        def piece(index, inner):
            near = pl.ds(pl.multiple_of(index * width, width), width)
            far = pl.ds(pl.multiple_of(lax.rem(chunk, per_group) * WRITE_CHUNK + index * width, width), width)
            new = weight[rows(group), far] - group_rate * direction[rows(group), far]
            fresh[slot, :, near] = new
            packed[slot, :, near] = new.astype(BF16)
            return inner

        lax.fori_loop(0, WRITE_CHUNK // width, piece, 0, unroll=2)
        for copy in puts(chunk):
            copy.start()
        return carry

    lax.fori_loop(0, chunks, one_chunk, 0)

    def finish(group, carry):
        land_copy(group).wait()
        return carry

    lax.fori_loop(0, groups, finish, 0)
    for chunk in range(chunks - WRITE_SLOTS, chunks):
        for copy in puts(chunk):
            copy.wait()


def solution(mesh):
    sizes = (mesh.shape['model'], mesh.shape['data'])
    devices = sizes[0] * sizes[1]
    both_axes = ('model', 'data')
    state_spec = P(None, both_axes)
    hbm = pl.BlockSpec(memory_space=pl.ANY)
    vmem = pl.BlockSpec(memory_space=pltpu.VMEM)
    dma = pltpu.SemaphoreType.DMA

    def device_step(local_grads, master, moment_one, moment_two):
        blocks, cols = master.shape
        groups = blocks // GROUP
        kept = pltpu.VMEM((blocks, cols), F32)
        keep = functools.partial(pltpu.with_memory_space_constraint, memory_space=pltpu.VMEM)
        tile = jax.ShapeDtypeStruct((GROUP, LANES), F32)
        state = jax.ShapeDtypeStruct((blocks, cols), F32)

        landed = pltpu.VMEM((groups, GROUP, cols), BF16)
        ring_shape = pltpu.VMEM((2, RING, GROUP, CHUNK), F32)
        landed = pltpu.VMEM((groups, GROUP, cols), BF16)
        parts = groups * (cols // PART)

        caught = pltpu.VMEM((LAND_SLOTS, GROUP, PART), BF16)

        mean, weight, ring, catch, clip, weight_stat = pl.pallas_call(
            functools.partial(exchange_kernel, sizes, groups, cols),
            out_shape=(kept, kept, ring_shape, caught, tile, tile),
            in_specs=[hbm] * 4,
            out_specs=[vmem] * 6,
            scratch_shapes=[pltpu.VMEM((STAGE_SLOTS, GROUP, PART), BF16), pltpu.VMEM((OWN_SLOTS, GROUP, PART), BF16), pltpu.VMEM((GROUP, LANES), F32), pltpu.VMEM((devices, GROUP, LANES), F32),
                            dma((STAGE_SLOTS,)), dma((STAGE_SLOTS,)), dma((LAND_SLOTS,)), pltpu.SemaphoreType.REGULAR, dma((OWN_SLOTS,)), dma((parts,)), dma((2, RING)), dma((devices,)), dma((devices,))],
            compiler_params=pltpu.CompilerParams(collective_id=0, has_side_effects=True, vmem_limit_bytes=SCOPE),
            name='exchange',
        )(local_grads, master, moment_one, moment_two)

        direction, weight, _, _, new_one, new_two, stats = pl.pallas_call(
            functools.partial(moment_kernel, groups, cols),
            out_shape=(kept, kept, ring_shape, caught, state, state, jax.ShapeDtypeStruct((2, GROUP, LANES), F32)),
            in_specs=[vmem] * 6 + [hbm] * 2,
            out_specs=[vmem, vmem, vmem, vmem, hbm, hbm, vmem],
            input_output_aliases={0: 0, 1: 1, 2: 2, 3: 3},
            scratch_shapes=[dma((RING,))] * 4,
            compiler_params=pltpu.CompilerParams(vmem_limit_bytes=SCOPE),
            name='moments',
        )(mean, weight, ring, catch, clip, weight_stat, moment_one, moment_two)

        land, rate = pl.pallas_call(
            functools.partial(weight_kernel, sizes, groups, cols),
            out_shape=(landed, tile),
            in_specs=[vmem] * 3,
            out_specs=[vmem] * 2,
            scratch_shapes=[pltpu.VMEM((devices, 2, GROUP, LANES), F32), pltpu.VMEM((SEND_SLOTS, GROUP, cols), BF16),
                            dma((SEND_SLOTS,)), dma((groups,)), dma((devices,)), dma((devices,))],
            compiler_params=pltpu.CompilerParams(collective_id=1, has_side_effects=True, vmem_limit_bytes=SCOPE),
            name='weights',
        )(keep(direction), keep(weight), stats)

        params, new_master = pl.pallas_call(
            functools.partial(write_kernel, sizes, groups, cols),
            out_shape=(jax.ShapeDtypeStruct((blocks, sizes[1] * cols), BF16), state),
            in_specs=[vmem] * 4,
            out_specs=[hbm, hbm],
            scratch_shapes=[pltpu.VMEM((WRITE_SLOTS, GROUP, WRITE_CHUNK), F32), pltpu.VMEM((WRITE_SLOTS, GROUP, WRITE_CHUNK), BF16),
                            dma((WRITE_SLOTS,)), dma((groups,)), dma((WRITE_SLOTS,))],
            compiler_params=pltpu.CompilerParams(vmem_limit_bytes=SCOPE),
            name='write',
        )(keep(direction), keep(weight), keep(land), rate)
        return params, new_master, new_one, new_two

    return jax.shard_map(device_step, mesh=mesh, in_specs=(P('data', None, 'model'), state_spec, state_spec, state_spec),
                         out_specs=(P(None, 'model'), state_spec, state_spec, state_spec), check_vma=False)
```

```python
import functools

import jax
import jax.numpy as jnp
from jax import lax
from jax.experimental import pallas as pl
from jax.experimental.pallas import tpu as pltpu
from jax.sharding import PartitionSpec as P

STEP = 4
LEARN_RATE = 0.08
BETA_ONE = 0.9
BETA_TWO = 0.999
EPSILON = 1e-6
WEIGHT_DECAY = 0.01
MAX_NORM = 1.0
CORR_ONE = 1.0 - BETA_ONE ** STEP
CORR_TWO = 1.0 - BETA_TWO ** STEP
TINY = 1.2e-38

MESH = pl.DeviceIdType.MESH
F32 = jnp.float32
BF16 = jnp.bfloat16
SCOPE = 4000 << 10
LANES = 128
GROUP = 8

PART = 16384
AHEAD = 4
LAND_SLOTS = 8
STAGE_SLOTS = 9
OWN_SLOTS = 6
RING = 10
LAG = 4
MOMENT_WIDTH = 2048
MEAN_WIDTH = 2048
CHUNK = 16384
SEND_SLOTS = 4
WRITE_SLOTS = 5
WRITE_CHUNK = 16384


def rows(group):
    return pl.ds(pl.multiple_of(group * GROUP, GROUP), GROUP)


def lanes_of():
    return lax.broadcasted_iota(jnp.int32, (GROUP, LANES), 1)


def put_lane(tile, lane_ids, lane, partial):
    row_sum = jnp.sum(partial, axis=1, keepdims=True)
    return tile + jnp.where(lane_ids == lane, row_sum, 0.0)


def tree_sum(values):
    while len(values) > 1:
        values = [a + b for a, b in zip(values[::2], values[1::2])] + ([values[-1]] if len(values) % 2 else [])
    return values[0]


def peers(model_size, data_size):
    model, data = lax.axis_index('model'), lax.axis_index('data')
    out = []
    for step in range(1, model_size * data_size):
        peer_model = lax.rem(model + step // data_size, model_size)
        peer_data = lax.rem(data + step % data_size, data_size)
        out.append(((peer_model, peer_data), peer_model * data_size + peer_data))
    return model * data_size + data, out


def enter(others):
    barrier = pltpu.get_barrier_semaphore()
    for device, _ in others:
        pl.semaphore_signal(barrier, inc=1, device_id=device, device_id_type=MESH)
    pl.semaphore_wait(barrier, len(others))


def share(me, others, source, slots, send_sem, recv_sem):
    copies = []
    for device, index in others:
        copy = pltpu.make_async_remote_copy(src_ref=source, dst_ref=slots.at[me], send_sem=send_sem.at[index], recv_sem=recv_sem.at[me], device_id=device, device_id_type=MESH)
        copy.start()
        copies.append(copy)
    for device, index in others:
        pltpu.make_async_remote_copy(src_ref=source, dst_ref=slots.at[index], send_sem=send_sem.at[index], recv_sem=recv_sem.at[index], device_id=device, device_id_type=MESH).wait_recv()
    for copy in copies:
        copy.wait_send()


def exchange_kernel(sizes, groups, cols, grads, master, one_in, two_in, mean_ref, weight_ref, ring, land, clip_ref, stat_ref, stage, own, part, slots,
                    stage_sem, send_sem, recv_sem, free_sem, own_sem, weight_sem, ring_sem, small_send, small_recv):
    model_size, data_size = sizes
    data = lax.axis_index('data')
    me, others = peers(model_size, data_size)
    peer = lax.rem(data + 1, data_size)
    peer_device = (lax.axis_index('model'), peer)
    per_group = cols // PART
    parts = groups * per_group

    def columns(index, base):
        return pl.ds(pl.multiple_of(base + lax.rem(index, per_group) * PART, PART), PART)

    def own_copy(index):
        slot = lax.rem(index, OWN_SLOTS)
        return pltpu.make_async_copy(grads.at[0, rows(index // per_group), columns(index, data * cols)], own.at[slot], own_sem.at[slot])

    def weight_copy(index):
        at = (rows(index // per_group), columns(index, 0))
        return pltpu.make_async_copy(master.at[at], weight_ref.at[at], weight_sem.at[index])

    def stage_copy(index):
        slot = lax.rem(index, STAGE_SLOTS)
        return pltpu.make_async_copy(grads.at[0, rows(index // per_group), columns(index, peer * cols)], stage.at[slot], stage_sem.at[slot])

    def send_copy(index):
        from_slot, to_slot = lax.rem(index, STAGE_SLOTS), lax.rem(index, LAND_SLOTS)
        return pltpu.make_async_remote_copy(src_ref=stage.at[from_slot], dst_ref=land.at[to_slot], send_sem=send_sem.at[from_slot], recv_sem=recv_sem.at[to_slot],
                                            device_id=peer_device, device_id_type=MESH)

    def ring_copies(chunk):
        at = (rows(chunk // (cols // CHUNK)), pl.ds(pl.multiple_of(lax.rem(chunk, cols // CHUNK) * CHUNK, CHUNK), CHUNK))
        return (pltpu.make_async_copy(one_in.at[at], ring.at[0, chunk], ring_sem.at[0, chunk]), pltpu.make_async_copy(two_in.at[at], ring.at[1, chunk], ring_sem.at[1, chunk]))

    def begin_stage(index, carry):
        stage_copy(index).start()
        return carry

    def begin_own(index, carry):
        own_copy(index).start()
        weight_copy(index).start()
        return carry

    def begin_send(index, carry):
        stage_copy(index).wait()
        send_copy(index).start()
        return carry

    lax.fori_loop(0, STAGE_SLOTS, begin_stage, 0)
    lax.fori_loop(0, OWN_SLOTS, begin_own, 0)
    enter(others)
    lax.fori_loop(0, AHEAD, begin_send, 0)
    lane_ids = lanes_of()
    width = MEAN_WIDTH
    zero = jnp.zeros((GROUP, LANES), F32)
    first_ring = parts - RING // 2

    def one_part(index, carry):
        total, stat = carry
        own_slot, land_slot = lax.rem(index, OWN_SLOTS), lax.rem(index, LAND_SLOTS)
        row_at = rows(index // per_group)
        col_at = lax.rem(index, per_group) * PART

        @pl.when(jnp.logical_and(index + AHEAD >= LAND_SLOTS, index + AHEAD < parts))
        def _():
            pl.semaphore_wait(free_sem, 1)

        @pl.when(index + AHEAD < parts)
        def _():
            begin_send(index + AHEAD, 0)

        own_copy(index).wait()
        weight_copy(index).wait()
        send_copy(index).wait_recv()

        def piece(step, sums):
            grad_sum, weight_sum = sums
            near = pl.ds(pl.multiple_of(step * width, width), width)
            far = pl.ds(pl.multiple_of(col_at + step * width, width), width)
            weight = weight_ref[row_at, far]
            mean = (own[own_slot, :, near].astype(F32) + land[land_slot, :, near].astype(F32)) * 0.5
            mean_ref[row_at, far] = mean
            cuts = range(0, width, LANES)
            grad_sum += tree_sum([mean[:, at:at + LANES] * mean[:, at:at + LANES] for at in cuts])
            weight_sum += tree_sum([weight[:, at:at + LANES] * weight[:, at:at + LANES] for at in cuts])
            return grad_sum, weight_sum

        grad_sum, weight_sum = lax.fori_loop(0, PART // width, piece, (zero, zero))

        @pl.when(index + LAND_SLOTS < parts)
        def _():
            pl.semaphore_signal(free_sem, inc=1, device_id=peer_device, device_id_type=MESH)

        @pl.when(index + OWN_SLOTS < parts)
        def _():
            begin_own(index + OWN_SLOTS, 0)

        send_copy(index).wait_send()

        @pl.when(index + STAGE_SLOTS < parts)
        def _():
            begin_stage(index + STAGE_SLOTS, 0)

        @pl.when(index >= first_ring)
        def _():
            for late in range(2):
                for copy in ring_copies((index - first_ring) * 2 + late):
                    copy.start()

        return total + grad_sum, put_lane(stat, lane_ids, index // per_group, weight_sum)

    total, stat = lax.fori_loop(0, parts, one_part, (zero, zero))
    stat_ref[...] = stat
    part[...] = total
    slots[me] = part[...]
    share(me, others, part, slots, small_send, small_recv)
    whole = tree_sum([slots[index] for index in range(model_size * data_size)])
    whole = jnp.sum(jnp.sum(whole, axis=1, keepdims=True), axis=0, keepdims=True)
    whole = jnp.broadcast_to(whole, (GROUP, LANES))
    clip_ref[...] = jnp.minimum(1.0, MAX_NORM / jnp.sqrt(whole))

    def finish(chunk, carry):
        for copy in ring_copies(chunk):
            copy.wait()
        return carry

    lax.fori_loop(0, RING, finish, 0)


def moment_kernel(groups, cols, mean_in, weight_in, ring_in, land_in, clip, weight_stat, one_in, two_in, dir_ref, weight_ref, ring, land, one_out, two_out, stat_ref,
                  one_get, two_get, one_put, two_put):
    per_group = cols // CHUNK
    chunks = groups * per_group
    width = MOMENT_WIDTH
    lane_ids = lanes_of()

    def place(chunk):
        return rows(chunk // per_group), pl.ds(pl.multiple_of(lax.rem(chunk, per_group) * CHUNK, CHUNK), CHUNK)

    def gets(chunk):
        slot = lax.rem(chunk, RING)
        at = place(chunk)
        return (pltpu.make_async_copy(one_in.at[at], ring.at[0, slot], one_get.at[slot]), pltpu.make_async_copy(two_in.at[at], ring.at[1, slot], two_get.at[slot]))

    def puts(chunk):
        slot = lax.rem(chunk, RING)
        at = place(chunk)
        return (pltpu.make_async_copy(ring.at[0, slot], one_out.at[at], one_put.at[slot]), pltpu.make_async_copy(ring.at[1, slot], two_out.at[at], two_put.at[slot]))

    def start(copies):
        for priority, copy in enumerate(copies):
            copy.start(priority=priority)

    def wait(copies):
        for copy in copies:
            copy.wait()

    scale = jnp.concatenate([clip[...]] * (width // LANES), axis=1)
    one_scale = (1.0 - BETA_ONE) * scale
    two_scale = (1.0 - BETA_TWO) * scale * scale
    ratio = CORR_TWO ** 0.5 / CORR_ONE
    floor = EPSILON * CORR_TWO ** 0.5

    def one_chunk(chunk, stat):
        slot = lax.rem(chunk, RING)
        row_at = rows(chunk // per_group)
        col_at = lax.rem(chunk, per_group) * CHUNK

        @pl.when(chunk >= RING)
        def _():
            wait(gets(chunk))

        def piece(index, total):
            near = pl.ds(pl.multiple_of(index * width, width), width)
            far = pl.ds(pl.multiple_of(col_at + index * width, width), width)
            mean, weight = dir_ref[row_at, far], weight_ref[row_at, far]
            old_one, old_two = ring[0, slot, :, near], ring[1, slot, :, near]
            new_one = BETA_ONE * old_one + one_scale * mean
            new_two = BETA_TWO * old_two + two_scale * mean * mean
            root = new_two * lax.rsqrt(jnp.maximum(new_two, TINY))
            direction = (new_one * ratio) / (root + floor) + WEIGHT_DECAY * weight
            ring[0, slot, :, near] = new_one
            ring[1, slot, :, near] = new_two
            dir_ref[row_at, far] = direction
            return total + tree_sum([direction[:, at:at + LANES] * direction[:, at:at + LANES] for at in range(0, width, LANES)])

        total = lax.fori_loop(0, CHUNK // width, piece, jnp.zeros((GROUP, LANES), F32))
        start(puts(chunk))
        ahead = chunk + RING - LAG

        @pl.when(jnp.logical_and(ahead >= RING, ahead < chunks))
        def _():
            wait(puts(ahead - RING))
            start(gets(ahead))

        return put_lane(stat, lane_ids, chunk // per_group, total)

    stat_ref[0] = lax.fori_loop(0, chunks, one_chunk, jnp.zeros((GROUP, LANES), F32))
    stat_ref[1] = weight_stat[...]

    def finish(chunk, carry):
        wait(puts(chunk))
        return carry

    lax.fori_loop(chunks - RING, chunks, finish, 0)


def segment_sums(values):
    lane_ids = lanes_of()
    row_ids = lax.broadcasted_iota(jnp.int32, (GROUP, LANES), 0)
    kind = lax.rem(lane_ids, 3)
    first = jnp.where(kind == 0, 3, 4)
    second = jnp.where(kind == 0, 4, jnp.where(kind == 1, 7, 8))
    segment = jnp.where(row_ids < first, 0, jnp.where(row_ids < second, 1, 2))
    out = jnp.zeros((GROUP, LANES), F32)
    for index in range(3):
        inside = segment == index
        out = jnp.where(inside, jnp.sum(jnp.where(inside, values, 0.0), axis=0, keepdims=True), out)
    return out


def weight_kernel(sizes, groups, cols, direction, weight, stats, land, rate, slots, packed, send_sem, recv_sem, small_send, small_recv):
    model_size, data_size = sizes
    data = lax.axis_index('data')
    me, others = peers(model_size, data_size)
    peer_device = (lax.axis_index('model'), lax.rem(data + 1, data_size))
    enter(others)
    slots[me] = stats[...]
    share(me, others, stats, slots, small_send, small_recv)
    lane_ids = lanes_of()
    dir_sq = segment_sums(tree_sum([slots[index, 0] for index in range(model_size * data_size)]))
    weight_sq = segment_sums(tree_sum([slots[index, 1] for index in range(model_size * data_size)]))
    rate[...] = LEARN_RATE * (jnp.sqrt(weight_sq) / jnp.sqrt(dir_sq))
    width = 1024

    def send_copy(group):
        slot = lax.rem(group, SEND_SLOTS)
        return pltpu.make_async_remote_copy(src_ref=packed.at[slot], dst_ref=land.at[group], send_sem=send_sem.at[slot], recv_sem=recv_sem.at[group],
                                            device_id=peer_device, device_id_type=MESH)

    def one_group(group, carry):
        slot = lax.rem(group, SEND_SLOTS)

        @pl.when(group >= SEND_SLOTS)
        def _():
            send_copy(group - SEND_SLOTS).wait_send()

        group_rate = jnp.sum(jnp.where(lane_ids == group, rate[...], 0.0), axis=1, keepdims=True)

        def piece(index, inner):
            at = pl.ds(pl.multiple_of(index * width, width), width)
            packed[slot, :, at] = (weight[rows(group), at] - group_rate * direction[rows(group), at]).astype(BF16)
            return inner

        lax.fori_loop(0, cols // width, piece, 0, unroll=2)
        send_copy(group).start()
        return carry

    lax.fori_loop(0, groups, one_group, 0)

    def finish(group, carry):
        send_copy(group).wait_recv()
        return carry

    lax.fori_loop(0, groups, finish, 0)
    for group in range(groups - SEND_SLOTS, groups):
        send_copy(group).wait_send()


def write_kernel(sizes, groups, cols, direction, weight, land, rate, params, master, fresh, packed, master_sem, land_sem, own_sem):
    data_size = sizes[1]
    data = lax.axis_index('data')
    peer = lax.rem(data + 1, data_size)
    width = 1024
    lane_ids = lanes_of()
    per_group = cols // WRITE_CHUNK
    chunks = groups * per_group

    def columns(chunk, base):
        return pl.ds(pl.multiple_of(base + lax.rem(chunk, per_group) * WRITE_CHUNK, WRITE_CHUNK), WRITE_CHUNK)

    def puts(chunk):
        slot = lax.rem(chunk, WRITE_SLOTS)
        at = rows(chunk // per_group)
        return (pltpu.make_async_copy(fresh.at[slot], master.at[at, columns(chunk, 0)], master_sem.at[slot]),
                pltpu.make_async_copy(packed.at[slot], params.at[at, columns(chunk, data * cols)], own_sem.at[slot]))

    def land_copy(group):
        return pltpu.make_async_copy(land.at[group], params.at[rows(group), pl.ds(pl.multiple_of(peer * cols, LANES), cols)], land_sem.at[group])

    def one_chunk(chunk, carry):
        slot = lax.rem(chunk, WRITE_SLOTS)
        group = chunk // per_group

        @pl.when(lax.rem(chunk, per_group) == 0)
        def _():
            land_copy(group).start()

        @pl.when(chunk >= WRITE_SLOTS)
        def _():
            for copy in puts(chunk - WRITE_SLOTS):
                copy.wait()

        group_rate = jnp.sum(jnp.where(lane_ids == group, rate[...], 0.0), axis=1, keepdims=True)

        def piece(index, inner):
            near = pl.ds(pl.multiple_of(index * width, width), width)
            far = pl.ds(pl.multiple_of(lax.rem(chunk, per_group) * WRITE_CHUNK + index * width, width), width)
            new = weight[rows(group), far] - group_rate * direction[rows(group), far]
            fresh[slot, :, near] = new
            packed[slot, :, near] = new.astype(BF16)
            return inner

        lax.fori_loop(0, WRITE_CHUNK // width, piece, 0, unroll=2)
        for priority, copy in enumerate(puts(chunk)):
            copy.start(priority=priority)
        return carry

    lax.fori_loop(0, chunks, one_chunk, 0)

    def finish(group, carry):
        land_copy(group).wait()
        return carry

    lax.fori_loop(0, groups, finish, 0)
    for chunk in range(chunks - WRITE_SLOTS, chunks):
        for copy in puts(chunk):
            copy.wait()


def solution(mesh):
    sizes = (mesh.shape['model'], mesh.shape['data'])
    devices = sizes[0] * sizes[1]
    both_axes = ('model', 'data')
    state_spec = P(None, both_axes)
    hbm = pl.BlockSpec(memory_space=pl.ANY)
    vmem = pl.BlockSpec(memory_space=pltpu.VMEM)
    dma = pltpu.SemaphoreType.DMA

    def device_step(local_grads, master, moment_one, moment_two):
        blocks, cols = master.shape
        groups = blocks // GROUP
        kept = pltpu.VMEM((blocks, cols), F32)
        keep = functools.partial(pltpu.with_memory_space_constraint, memory_space=pltpu.VMEM)
        tile = jax.ShapeDtypeStruct((GROUP, LANES), F32)
        state = jax.ShapeDtypeStruct((blocks, cols), F32)

        landed = pltpu.VMEM((groups, GROUP, cols), BF16)
        ring_shape = pltpu.VMEM((2, RING, GROUP, CHUNK), F32)
        landed = pltpu.VMEM((groups, GROUP, cols), BF16)
        parts = groups * (cols // PART)

        caught = pltpu.VMEM((LAND_SLOTS, GROUP, PART), BF16)

        mean, weight, ring, catch, clip, weight_stat = pl.pallas_call(
            functools.partial(exchange_kernel, sizes, groups, cols),
            out_shape=(kept, kept, ring_shape, caught, tile, tile),
            in_specs=[hbm] * 4,
            out_specs=[vmem] * 6,
            scratch_shapes=[pltpu.VMEM((STAGE_SLOTS, GROUP, PART), BF16), pltpu.VMEM((OWN_SLOTS, GROUP, PART), BF16), pltpu.VMEM((GROUP, LANES), F32), pltpu.VMEM((devices, GROUP, LANES), F32),
                            dma((STAGE_SLOTS,)), dma((STAGE_SLOTS,)), dma((LAND_SLOTS,)), pltpu.SemaphoreType.REGULAR, dma((OWN_SLOTS,)), dma((parts,)), dma((2, RING)), dma((devices,)), dma((devices,))],
            compiler_params=pltpu.CompilerParams(collective_id=0, has_side_effects=True, vmem_limit_bytes=SCOPE),
            name='exchange',
        )(local_grads, master, moment_one, moment_two)

        direction, weight, _, _, new_one, new_two, stats = pl.pallas_call(
            functools.partial(moment_kernel, groups, cols),
            out_shape=(kept, kept, ring_shape, caught, state, state, jax.ShapeDtypeStruct((2, GROUP, LANES), F32)),
            in_specs=[vmem] * 6 + [hbm] * 2,
            out_specs=[vmem, vmem, vmem, vmem, hbm, hbm, vmem],
            input_output_aliases={0: 0, 1: 1, 2: 2, 3: 3},
            scratch_shapes=[dma((RING,))] * 4,
            compiler_params=pltpu.CompilerParams(vmem_limit_bytes=SCOPE),
            name='moments',
        )(mean, weight, ring, catch, clip, weight_stat, moment_one, moment_two)

        land, rate = pl.pallas_call(
            functools.partial(weight_kernel, sizes, groups, cols),
            out_shape=(landed, tile),
            in_specs=[vmem] * 3,
            out_specs=[vmem] * 2,
            scratch_shapes=[pltpu.VMEM((devices, 2, GROUP, LANES), F32), pltpu.VMEM((SEND_SLOTS, GROUP, cols), BF16),
                            dma((SEND_SLOTS,)), dma((groups,)), dma((devices,)), dma((devices,))],
            compiler_params=pltpu.CompilerParams(collective_id=1, has_side_effects=True, vmem_limit_bytes=SCOPE),
            name='weights',
        )(keep(direction), keep(weight), stats)

        params, new_master = pl.pallas_call(
            functools.partial(write_kernel, sizes, groups, cols),
            out_shape=(jax.ShapeDtypeStruct((blocks, sizes[1] * cols), BF16), state),
            in_specs=[vmem] * 4,
            out_specs=[hbm, hbm],
            scratch_shapes=[pltpu.VMEM((WRITE_SLOTS, GROUP, WRITE_CHUNK), F32), pltpu.VMEM((WRITE_SLOTS, GROUP, WRITE_CHUNK), BF16),
                            dma((WRITE_SLOTS,)), dma((groups,)), dma((WRITE_SLOTS,))],
            compiler_params=pltpu.CompilerParams(vmem_limit_bytes=SCOPE),
            name='write',
        )(keep(direction), keep(weight), keep(land), rate)
        return params, new_master, new_one, new_two

    return jax.shard_map(device_step, mesh=mesh, in_specs=(P('data', None, 'model'), state_spec, state_spec, state_spec),
                         out_specs=(P(None, 'model'), state_spec, state_spec, state_spec), check_vma=False)
```

```python
import functools

import jax
import jax.numpy as jnp
from jax import lax
from jax.experimental import pallas as pl
from jax.experimental.pallas import tpu as pltpu
from jax.sharding import PartitionSpec as P

STEP = 4
LEARN_RATE = 0.08
BETA_ONE = 0.9
BETA_TWO = 0.999
EPSILON = 1e-6
WEIGHT_DECAY = 0.01
MAX_NORM = 1.0
CORR_ONE = 1.0 - BETA_ONE ** STEP
CORR_TWO = 1.0 - BETA_TWO ** STEP
TINY = 1.2e-38

MESH = pl.DeviceIdType.MESH
F32 = jnp.float32
BF16 = jnp.bfloat16
SCOPE = 4000 << 10
LANES = 128
GROUP = 8

PART = 16384
AHEAD = 4
LAND_SLOTS = 8
STAGE_SLOTS = 9
OWN_SLOTS = 6
RING = 20
LAG = 8
MOMENT_WIDTH = 4096
MEAN_WIDTH = 2048
CHUNK = 8192
SEND_SLOTS = 4
WRITE_SLOTS = 5
WRITE_CHUNK = 16384


def rows(group):
    return pl.ds(pl.multiple_of(group * GROUP, GROUP), GROUP)


def lanes_of():
    return lax.broadcasted_iota(jnp.int32, (GROUP, LANES), 1)


def put_lane(tile, lane_ids, lane, partial):
    row_sum = jnp.sum(partial, axis=1, keepdims=True)
    return tile + jnp.where(lane_ids == lane, row_sum, 0.0)


def tree_sum(values):
    while len(values) > 1:
        values = [a + b for a, b in zip(values[::2], values[1::2])] + ([values[-1]] if len(values) % 2 else [])
    return values[0]


def peers(model_size, data_size):
    model, data = lax.axis_index('model'), lax.axis_index('data')
    out = []
    for step in range(1, model_size * data_size):
        peer_model = lax.rem(model + step // data_size, model_size)
        peer_data = lax.rem(data + step % data_size, data_size)
        out.append(((peer_model, peer_data), peer_model * data_size + peer_data))
    return model * data_size + data, out


def enter(others):
    barrier = pltpu.get_barrier_semaphore()
    for device, _ in others:
        pl.semaphore_signal(barrier, inc=1, device_id=device, device_id_type=MESH)
    pl.semaphore_wait(barrier, len(others))


def share(me, others, source, slots, send_sem, recv_sem):
    copies = []
    for device, index in others:
        copy = pltpu.make_async_remote_copy(src_ref=source, dst_ref=slots.at[me], send_sem=send_sem.at[index], recv_sem=recv_sem.at[me], device_id=device, device_id_type=MESH)
        copy.start()
        copies.append(copy)
    for device, index in others:
        pltpu.make_async_remote_copy(src_ref=source, dst_ref=slots.at[index], send_sem=send_sem.at[index], recv_sem=recv_sem.at[index], device_id=device, device_id_type=MESH).wait_recv()
    for copy in copies:
        copy.wait_send()


def exchange_kernel(sizes, groups, cols, grads, master, one_in, two_in, mean_ref, weight_ref, ring, land, clip_ref, stat_ref, stage, own, part, slots,
                    stage_sem, send_sem, recv_sem, free_sem, own_sem, weight_sem, ring_sem, small_send, small_recv):
    model_size, data_size = sizes
    data = lax.axis_index('data')
    me, others = peers(model_size, data_size)
    peer = lax.rem(data + 1, data_size)
    peer_device = (lax.axis_index('model'), peer)
    per_group = cols // PART
    parts = groups * per_group

    def columns(index, base):
        return pl.ds(pl.multiple_of(base + lax.rem(index, per_group) * PART, PART), PART)

    def own_copy(index):
        slot = lax.rem(index, OWN_SLOTS)
        return pltpu.make_async_copy(grads.at[0, rows(index // per_group), columns(index, data * cols)], own.at[slot], own_sem.at[slot])

    def weight_copy(index):
        at = (rows(index // per_group), columns(index, 0))
        return pltpu.make_async_copy(master.at[at], weight_ref.at[at], weight_sem.at[index])

    def stage_copy(index):
        slot = lax.rem(index, STAGE_SLOTS)
        return pltpu.make_async_copy(grads.at[0, rows(index // per_group), columns(index, peer * cols)], stage.at[slot], stage_sem.at[slot])

    def send_copy(index):
        from_slot, to_slot = lax.rem(index, STAGE_SLOTS), lax.rem(index, LAND_SLOTS)
        return pltpu.make_async_remote_copy(src_ref=stage.at[from_slot], dst_ref=land.at[to_slot], send_sem=send_sem.at[from_slot], recv_sem=recv_sem.at[to_slot],
                                            device_id=peer_device, device_id_type=MESH)

    def ring_copies(chunk):
        at = (rows(chunk // (cols // CHUNK)), pl.ds(pl.multiple_of(lax.rem(chunk, cols // CHUNK) * CHUNK, CHUNK), CHUNK))
        return (pltpu.make_async_copy(one_in.at[at], ring.at[0, chunk], ring_sem.at[0, chunk]), pltpu.make_async_copy(two_in.at[at], ring.at[1, chunk], ring_sem.at[1, chunk]))

    def begin_stage(index, carry):
        stage_copy(index).start()
        return carry

    def begin_own(index, carry):
        own_copy(index).start()
        weight_copy(index).start()
        return carry

    def begin_send(index, carry):
        stage_copy(index).wait()
        send_copy(index).start()
        return carry

    lax.fori_loop(0, STAGE_SLOTS, begin_stage, 0)
    lax.fori_loop(0, OWN_SLOTS, begin_own, 0)
    enter(others)
    lax.fori_loop(0, AHEAD, begin_send, 0)
    lane_ids = lanes_of()
    width = MEAN_WIDTH
    zero = jnp.zeros((GROUP, LANES), F32)
    first_ring = parts - RING // 2

    def one_part(index, carry):
        total, stat = carry
        own_slot, land_slot = lax.rem(index, OWN_SLOTS), lax.rem(index, LAND_SLOTS)
        row_at = rows(index // per_group)
        col_at = lax.rem(index, per_group) * PART

        @pl.when(jnp.logical_and(index + AHEAD >= LAND_SLOTS, index + AHEAD < parts))
        def _():
            pl.semaphore_wait(free_sem, 1)

        @pl.when(index + AHEAD < parts)
        def _():
            begin_send(index + AHEAD, 0)

        own_copy(index).wait()
        weight_copy(index).wait()
        send_copy(index).wait_recv()

        def piece(step, sums):
            grad_sum, weight_sum = sums
            near = pl.ds(pl.multiple_of(step * width, width), width)
            far = pl.ds(pl.multiple_of(col_at + step * width, width), width)
            weight = weight_ref[row_at, far]
            mean = (own[own_slot, :, near].astype(F32) + land[land_slot, :, near].astype(F32)) * 0.5
            mean_ref[row_at, far] = mean
            cuts = range(0, width, LANES)
            grad_sum += tree_sum([mean[:, at:at + LANES] * mean[:, at:at + LANES] for at in cuts])
            weight_sum += tree_sum([weight[:, at:at + LANES] * weight[:, at:at + LANES] for at in cuts])
            return grad_sum, weight_sum

        grad_sum, weight_sum = lax.fori_loop(0, PART // width, piece, (zero, zero))

        @pl.when(index + LAND_SLOTS < parts)
        def _():
            pl.semaphore_signal(free_sem, inc=1, device_id=peer_device, device_id_type=MESH)

        @pl.when(index + OWN_SLOTS < parts)
        def _():
            begin_own(index + OWN_SLOTS, 0)

        send_copy(index).wait_send()

        @pl.when(index + STAGE_SLOTS < parts)
        def _():
            begin_stage(index + STAGE_SLOTS, 0)

        @pl.when(index >= first_ring)
        def _():
            for late in range(2):
                for copy in ring_copies((index - first_ring) * 2 + late):
                    copy.start()

        return total + grad_sum, put_lane(stat, lane_ids, index // per_group, weight_sum)

    total, stat = lax.fori_loop(0, parts, one_part, (zero, zero))
    stat_ref[...] = stat
    part[...] = total
    slots[me] = part[...]
    share(me, others, part, slots, small_send, small_recv)
    whole = tree_sum([slots[index] for index in range(model_size * data_size)])
    whole = jnp.sum(jnp.sum(whole, axis=1, keepdims=True), axis=0, keepdims=True)
    whole = jnp.broadcast_to(whole, (GROUP, LANES))
    clip_ref[...] = jnp.minimum(1.0, MAX_NORM / jnp.sqrt(whole))

    def finish(chunk, carry):
        for copy in ring_copies(chunk):
            copy.wait()
        return carry

    lax.fori_loop(0, RING, finish, 0)


def moment_kernel(groups, cols, mean_in, weight_in, ring_in, land_in, clip, weight_stat, one_in, two_in, dir_ref, weight_ref, ring, land, one_out, two_out, stat_ref,
                  one_get, two_get, one_put, two_put):
    per_group = cols // CHUNK
    chunks = groups * per_group
    width = MOMENT_WIDTH
    lane_ids = lanes_of()

    def place(chunk):
        return rows(chunk // per_group), pl.ds(pl.multiple_of(lax.rem(chunk, per_group) * CHUNK, CHUNK), CHUNK)

    def gets(chunk):
        slot = lax.rem(chunk, RING)
        at = place(chunk)
        return (pltpu.make_async_copy(one_in.at[at], ring.at[0, slot], one_get.at[slot]), pltpu.make_async_copy(two_in.at[at], ring.at[1, slot], two_get.at[slot]))

    def puts(chunk):
        slot = lax.rem(chunk, RING)
        at = place(chunk)
        return (pltpu.make_async_copy(ring.at[0, slot], one_out.at[at], one_put.at[slot]), pltpu.make_async_copy(ring.at[1, slot], two_out.at[at], two_put.at[slot]))

    def start(copies, priority=0):
        for copy in copies:
            copy.start(priority=priority)

    def wait(copies):
        for copy in copies:
            copy.wait()

    scale = jnp.concatenate([clip[...]] * (width // LANES), axis=1)
    one_scale = (1.0 - BETA_ONE) * scale
    two_scale = (1.0 - BETA_TWO) * scale * scale
    ratio = CORR_TWO ** 0.5 / CORR_ONE
    floor = EPSILON * CORR_TWO ** 0.5

    def one_chunk(chunk, stat):
        slot = lax.rem(chunk, RING)
        row_at = rows(chunk // per_group)
        col_at = lax.rem(chunk, per_group) * CHUNK

        @pl.when(chunk >= RING)
        def _():
            wait(gets(chunk))

        def piece(index, total):
            near = pl.ds(pl.multiple_of(index * width, width), width)
            far = pl.ds(pl.multiple_of(col_at + index * width, width), width)
            mean, weight = dir_ref[row_at, far], weight_ref[row_at, far]
            old_one, old_two = ring[0, slot, :, near], ring[1, slot, :, near]
            new_one = BETA_ONE * old_one + one_scale * mean
            new_two = BETA_TWO * old_two + two_scale * mean * mean
            root = new_two * lax.rsqrt(jnp.maximum(new_two, TINY))
            direction = (new_one * ratio) / (root + floor) + WEIGHT_DECAY * weight
            ring[0, slot, :, near] = new_one
            ring[1, slot, :, near] = new_two
            dir_ref[row_at, far] = direction
            return total + tree_sum([direction[:, at:at + LANES] * direction[:, at:at + LANES] for at in range(0, width, LANES)])

        total = lax.fori_loop(0, CHUNK // width, piece, jnp.zeros((GROUP, LANES), F32))
        start(puts(chunk), priority=1)
        ahead = chunk + RING - LAG

        @pl.when(jnp.logical_and(ahead >= RING, ahead < chunks))
        def _():
            wait(puts(ahead - RING))
            start(gets(ahead))

        return put_lane(stat, lane_ids, chunk // per_group, total)

    stat_ref[0] = lax.fori_loop(0, chunks, one_chunk, jnp.zeros((GROUP, LANES), F32))
    stat_ref[1] = weight_stat[...]

    def finish(chunk, carry):
        wait(puts(chunk))
        return carry

    lax.fori_loop(chunks - RING, chunks, finish, 0)


def segment_sums(values):
    lane_ids = lanes_of()
    row_ids = lax.broadcasted_iota(jnp.int32, (GROUP, LANES), 0)
    kind = lax.rem(lane_ids, 3)
    first = jnp.where(kind == 0, 3, 4)
    second = jnp.where(kind == 0, 4, jnp.where(kind == 1, 7, 8))
    segment = jnp.where(row_ids < first, 0, jnp.where(row_ids < second, 1, 2))
    out = jnp.zeros((GROUP, LANES), F32)
    for index in range(3):
        inside = segment == index
        out = jnp.where(inside, jnp.sum(jnp.where(inside, values, 0.0), axis=0, keepdims=True), out)
    return out


def weight_kernel(sizes, groups, cols, direction, weight, stats, land, rate, slots, packed, send_sem, recv_sem, small_send, small_recv):
    model_size, data_size = sizes
    data = lax.axis_index('data')
    me, others = peers(model_size, data_size)
    peer_device = (lax.axis_index('model'), lax.rem(data + 1, data_size))
    enter(others)
    slots[me] = stats[...]
    share(me, others, stats, slots, small_send, small_recv)
    lane_ids = lanes_of()
    dir_sq = segment_sums(tree_sum([slots[index, 0] for index in range(model_size * data_size)]))
    weight_sq = segment_sums(tree_sum([slots[index, 1] for index in range(model_size * data_size)]))
    rate[...] = LEARN_RATE * (jnp.sqrt(weight_sq) / jnp.sqrt(dir_sq))
    width = 1024

    def send_copy(group):
        slot = lax.rem(group, SEND_SLOTS)
        return pltpu.make_async_remote_copy(src_ref=packed.at[slot], dst_ref=land.at[group], send_sem=send_sem.at[slot], recv_sem=recv_sem.at[group],
                                            device_id=peer_device, device_id_type=MESH)

    def one_group(group, carry):
        slot = lax.rem(group, SEND_SLOTS)

        @pl.when(group >= SEND_SLOTS)
        def _():
            send_copy(group - SEND_SLOTS).wait_send()

        group_rate = jnp.sum(jnp.where(lane_ids == group, rate[...], 0.0), axis=1, keepdims=True)

        def piece(index, inner):
            at = pl.ds(pl.multiple_of(index * width, width), width)
            packed[slot, :, at] = (weight[rows(group), at] - group_rate * direction[rows(group), at]).astype(BF16)
            return inner

        lax.fori_loop(0, cols // width, piece, 0, unroll=2)
        send_copy(group).start()
        return carry

    lax.fori_loop(0, groups, one_group, 0)

    def finish(group, carry):
        send_copy(group).wait_recv()
        return carry

    lax.fori_loop(0, groups, finish, 0)
    for group in range(groups - SEND_SLOTS, groups):
        send_copy(group).wait_send()


def write_kernel(sizes, groups, cols, direction, weight, land, rate, params, master, fresh, packed, master_sem, land_sem, own_sem):
    data_size = sizes[1]
    data = lax.axis_index('data')
    peer = lax.rem(data + 1, data_size)
    width = 1024
    lane_ids = lanes_of()
    per_group = cols // WRITE_CHUNK
    chunks = groups * per_group

    def columns(chunk, base):
        return pl.ds(pl.multiple_of(base + lax.rem(chunk, per_group) * WRITE_CHUNK, WRITE_CHUNK), WRITE_CHUNK)

    def puts(chunk):
        slot = lax.rem(chunk, WRITE_SLOTS)
        at = rows(chunk // per_group)
        return (pltpu.make_async_copy(fresh.at[slot], master.at[at, columns(chunk, 0)], master_sem.at[slot]),
                pltpu.make_async_copy(packed.at[slot], params.at[at, columns(chunk, data * cols)], own_sem.at[slot]))

    def land_copy(group):
        return pltpu.make_async_copy(land.at[group], params.at[rows(group), pl.ds(pl.multiple_of(peer * cols, LANES), cols)], land_sem.at[group])

    def one_chunk(chunk, carry):
        slot = lax.rem(chunk, WRITE_SLOTS)
        group = chunk // per_group

        @pl.when(lax.rem(chunk, per_group) == 0)
        def _():
            land_copy(group).start()

        @pl.when(chunk >= WRITE_SLOTS)
        def _():
            for copy in puts(chunk - WRITE_SLOTS):
                copy.wait()

        group_rate = jnp.sum(jnp.where(lane_ids == group, rate[...], 0.0), axis=1, keepdims=True)

        def piece(index, inner):
            near = pl.ds(pl.multiple_of(index * width, width), width)
            far = pl.ds(pl.multiple_of(lax.rem(chunk, per_group) * WRITE_CHUNK + index * width, width), width)
            new = weight[rows(group), far] - group_rate * direction[rows(group), far]
            fresh[slot, :, near] = new
            packed[slot, :, near] = new.astype(BF16)
            return inner

        lax.fori_loop(0, WRITE_CHUNK // width, piece, 0, unroll=2)
        for priority, copy in enumerate(puts(chunk)):
            copy.start(priority=priority)
        return carry

    lax.fori_loop(0, chunks, one_chunk, 0)

    def finish(group, carry):
        land_copy(group).wait()
        return carry

    lax.fori_loop(0, groups, finish, 0)
    for chunk in range(chunks - WRITE_SLOTS, chunks):
        for copy in puts(chunk):
            copy.wait()


def solution(mesh):
    sizes = (mesh.shape['model'], mesh.shape['data'])
    devices = sizes[0] * sizes[1]
    both_axes = ('model', 'data')
    state_spec = P(None, both_axes)
    hbm = pl.BlockSpec(memory_space=pl.ANY)
    vmem = pl.BlockSpec(memory_space=pltpu.VMEM)
    dma = pltpu.SemaphoreType.DMA

    def device_step(local_grads, master, moment_one, moment_two):
        blocks, cols = master.shape
        groups = blocks // GROUP
        kept = pltpu.VMEM((blocks, cols), F32)
        keep = functools.partial(pltpu.with_memory_space_constraint, memory_space=pltpu.VMEM)
        tile = pltpu.VMEM((GROUP, LANES), F32)
        state = jax.ShapeDtypeStruct((blocks, cols), F32)

        landed = pltpu.VMEM((groups, GROUP, cols), BF16)
        ring_shape = pltpu.VMEM((2, RING, GROUP, CHUNK), F32)
        landed = pltpu.VMEM((groups, GROUP, cols), BF16)
        parts = groups * (cols // PART)

        caught = pltpu.VMEM((LAND_SLOTS, GROUP, PART), BF16)

        mean, weight, ring, catch, clip, weight_stat = pl.pallas_call(
            functools.partial(exchange_kernel, sizes, groups, cols),
            out_shape=(kept, kept, ring_shape, caught, tile, tile),
            in_specs=[hbm] * 4,
            out_specs=[vmem] * 6,
            scratch_shapes=[pltpu.VMEM((STAGE_SLOTS, GROUP, PART), BF16), pltpu.VMEM((OWN_SLOTS, GROUP, PART), BF16), pltpu.VMEM((GROUP, LANES), F32), pltpu.VMEM((devices, GROUP, LANES), F32),
                            dma((STAGE_SLOTS,)), dma((STAGE_SLOTS,)), dma((LAND_SLOTS,)), pltpu.SemaphoreType.REGULAR, dma((OWN_SLOTS,)), dma((parts,)), dma((2, RING)), dma((devices,)), dma((devices,))],
            compiler_params=pltpu.CompilerParams(collective_id=0, has_side_effects=True, vmem_limit_bytes=SCOPE),
            name='exchange',
        )(local_grads, master, moment_one, moment_two)

        direction, weight, _, _, new_one, new_two, stats = pl.pallas_call(
            functools.partial(moment_kernel, groups, cols),
            out_shape=(kept, kept, ring_shape, caught, state, state, pltpu.VMEM((2, GROUP, LANES), F32)),
            in_specs=[vmem] * 6 + [hbm] * 2,
            out_specs=[vmem, vmem, vmem, vmem, hbm, hbm, vmem],
            input_output_aliases={0: 0, 1: 1, 2: 2, 3: 3},
            scratch_shapes=[dma((RING,))] * 4,
            compiler_params=pltpu.CompilerParams(vmem_limit_bytes=SCOPE),
            name='moments',
        )(mean, weight, ring, catch, keep(clip), keep(weight_stat), moment_one, moment_two)

        land, rate = pl.pallas_call(
            functools.partial(weight_kernel, sizes, groups, cols),
            out_shape=(landed, tile),
            in_specs=[vmem] * 3,
            out_specs=[vmem] * 2,
            scratch_shapes=[pltpu.VMEM((devices, 2, GROUP, LANES), F32), pltpu.VMEM((SEND_SLOTS, GROUP, cols), BF16),
                            dma((SEND_SLOTS,)), dma((groups,)), dma((devices,)), dma((devices,))],
            compiler_params=pltpu.CompilerParams(collective_id=1, has_side_effects=True, vmem_limit_bytes=SCOPE),
            name='weights',
        )(keep(direction), keep(weight), keep(stats))

        params, new_master = pl.pallas_call(
            functools.partial(write_kernel, sizes, groups, cols),
            out_shape=(jax.ShapeDtypeStruct((blocks, sizes[1] * cols), BF16), state),
            in_specs=[vmem] * 4,
            out_specs=[hbm, hbm],
            scratch_shapes=[pltpu.VMEM((WRITE_SLOTS, GROUP, WRITE_CHUNK), F32), pltpu.VMEM((WRITE_SLOTS, GROUP, WRITE_CHUNK), BF16),
                            dma((WRITE_SLOTS,)), dma((groups,)), dma((WRITE_SLOTS,))],
            compiler_params=pltpu.CompilerParams(vmem_limit_bytes=SCOPE),
            name='write',
        )(keep(direction), keep(weight), keep(land), keep(rate))
        return params, new_master, new_one, new_two

    return jax.shard_map(device_step, mesh=mesh, in_specs=(P('data', None, 'model'), state_spec, state_spec, state_spec),
                         out_specs=(P(None, 'model'), state_spec, state_spec, state_spec), check_vma=False)
```

```python
import functools

import jax
import jax.numpy as jnp
from jax import lax
from jax.experimental import pallas as pl
from jax.experimental.pallas import tpu as pltpu
from jax.sharding import PartitionSpec as P

STEP = 4
LEARN_RATE = 0.08
BETA_ONE = 0.9
BETA_TWO = 0.999
EPSILON = 1e-6
WEIGHT_DECAY = 0.01
MAX_NORM = 1.0
CORR_ONE = 1.0 - BETA_ONE ** STEP
CORR_TWO = 1.0 - BETA_TWO ** STEP
TINY = 1.2e-38

MESH = pl.DeviceIdType.MESH
F32 = jnp.float32
BF16 = jnp.bfloat16
SCOPE = 4000 << 10
LANES = 128
GROUP = 8

PART = 16384
AHEAD = 4
LAND_SLOTS = 8
STAGE_SLOTS = 9
OWN_SLOTS = 6
RING = 20
LAG = 8
MOMENT_WIDTH = 4096
MEAN_WIDTH = 2048
CHUNK = 8192
SEND_SLOTS = 4
RIDE = 12
RIDE_SLOTS = 2
WRITE_SLOTS = 5
WRITE_CHUNK = 16384


def rows(group):
    return pl.ds(pl.multiple_of(group * GROUP, GROUP), GROUP)


def lanes_of():
    return lax.broadcasted_iota(jnp.int32, (GROUP, LANES), 1)


def put_lane(tile, lane_ids, lane, partial):
    row_sum = jnp.sum(partial, axis=1, keepdims=True)
    return tile + jnp.where(lane_ids == lane, row_sum, 0.0)


def tree_sum(values):
    while len(values) > 1:
        values = [a + b for a, b in zip(values[::2], values[1::2])] + ([values[-1]] if len(values) % 2 else [])
    return values[0]


def peers(model_size, data_size):
    model, data = lax.axis_index('model'), lax.axis_index('data')
    out = []
    for step in range(1, model_size * data_size):
        peer_model = lax.rem(model + step // data_size, model_size)
        peer_data = lax.rem(data + step % data_size, data_size)
        out.append(((peer_model, peer_data), peer_model * data_size + peer_data))
    return model * data_size + data, out


def enter(others):
    barrier = pltpu.get_barrier_semaphore()
    for device, _ in others:
        pl.semaphore_signal(barrier, inc=1, device_id=device, device_id_type=MESH)
    pl.semaphore_wait(barrier, len(others))


def share(me, others, source, slots, send_sem, recv_sem):
    copies = []
    for device, index in others:
        copy = pltpu.make_async_remote_copy(src_ref=source, dst_ref=slots.at[me], send_sem=send_sem.at[index], recv_sem=recv_sem.at[me], device_id=device, device_id_type=MESH)
        copy.start()
        copies.append(copy)
    for device, index in others:
        pltpu.make_async_remote_copy(src_ref=source, dst_ref=slots.at[index], send_sem=send_sem.at[index], recv_sem=recv_sem.at[index], device_id=device, device_id_type=MESH).wait_recv()
    for copy in copies:
        copy.wait_send()


def exchange_kernel(sizes, groups, cols, grads, master, one_in, two_in, mean_ref, weight_ref, ring, land, clip_ref, stat_ref, stage, own, part, slots,
                    stage_sem, send_sem, recv_sem, free_sem, own_sem, weight_sem, ring_sem, small_send, small_recv):
    model_size, data_size = sizes
    data = lax.axis_index('data')
    me, others = peers(model_size, data_size)
    peer = lax.rem(data + 1, data_size)
    peer_device = (lax.axis_index('model'), peer)
    per_group = cols // PART
    parts = groups * per_group

    def columns(index, base):
        return pl.ds(pl.multiple_of(base + lax.rem(index, per_group) * PART, PART), PART)

    def own_copy(index):
        slot = lax.rem(index, OWN_SLOTS)
        return pltpu.make_async_copy(grads.at[0, rows(index // per_group), columns(index, data * cols)], own.at[slot], own_sem.at[slot])

    def weight_copy(index):
        at = (rows(index // per_group), columns(index, 0))
        return pltpu.make_async_copy(master.at[at], weight_ref.at[at], weight_sem.at[index])

    def stage_copy(index):
        slot = lax.rem(index, STAGE_SLOTS)
        return pltpu.make_async_copy(grads.at[0, rows(index // per_group), columns(index, peer * cols)], stage.at[slot], stage_sem.at[slot])

    def send_copy(index):
        from_slot, to_slot = lax.rem(index, STAGE_SLOTS), lax.rem(index, LAND_SLOTS)
        return pltpu.make_async_remote_copy(src_ref=stage.at[from_slot], dst_ref=land.at[to_slot], send_sem=send_sem.at[from_slot], recv_sem=recv_sem.at[to_slot],
                                            device_id=peer_device, device_id_type=MESH)

    def ring_copies(chunk):
        at = (rows(chunk // (cols // CHUNK)), pl.ds(pl.multiple_of(lax.rem(chunk, cols // CHUNK) * CHUNK, CHUNK), CHUNK))
        return (pltpu.make_async_copy(one_in.at[at], ring.at[0, chunk], ring_sem.at[0, chunk]), pltpu.make_async_copy(two_in.at[at], ring.at[1, chunk], ring_sem.at[1, chunk]))

    def begin_stage(index, carry):
        stage_copy(index).start()
        return carry

    def begin_own(index, carry):
        own_copy(index).start()
        weight_copy(index).start()
        return carry

    def begin_send(index, carry):
        stage_copy(index).wait()
        send_copy(index).start()
        return carry

    lax.fori_loop(0, STAGE_SLOTS, begin_stage, 0)
    lax.fori_loop(0, OWN_SLOTS, begin_own, 0)
    enter(others)
    lax.fori_loop(0, AHEAD, begin_send, 0)
    lane_ids = lanes_of()
    width = MEAN_WIDTH
    zero = jnp.zeros((GROUP, LANES), F32)
    first_ring = parts - RING // 2

    def one_part(index, carry):
        total, stat = carry
        own_slot, land_slot = lax.rem(index, OWN_SLOTS), lax.rem(index, LAND_SLOTS)
        row_at = rows(index // per_group)
        col_at = lax.rem(index, per_group) * PART

        @pl.when(jnp.logical_and(index + AHEAD >= LAND_SLOTS, index + AHEAD < parts))
        def _():
            pl.semaphore_wait(free_sem, 1)

        @pl.when(index + AHEAD < parts)
        def _():
            begin_send(index + AHEAD, 0)

        own_copy(index).wait()
        weight_copy(index).wait()
        send_copy(index).wait_recv()

        def piece(step, sums):
            grad_sum, weight_sum = sums
            near = pl.ds(pl.multiple_of(step * width, width), width)
            far = pl.ds(pl.multiple_of(col_at + step * width, width), width)
            weight = weight_ref[row_at, far]
            mean = (own[own_slot, :, near].astype(F32) + land[land_slot, :, near].astype(F32)) * 0.5
            mean_ref[row_at, far] = mean
            cuts = range(0, width, LANES)
            grad_sum += tree_sum([mean[:, at:at + LANES] * mean[:, at:at + LANES] for at in cuts])
            weight_sum += tree_sum([weight[:, at:at + LANES] * weight[:, at:at + LANES] for at in cuts])
            return grad_sum, weight_sum

        grad_sum, weight_sum = lax.fori_loop(0, PART // width, piece, (zero, zero))

        @pl.when(index + LAND_SLOTS < parts)
        def _():
            pl.semaphore_signal(free_sem, inc=1, device_id=peer_device, device_id_type=MESH)

        @pl.when(index + OWN_SLOTS < parts)
        def _():
            begin_own(index + OWN_SLOTS, 0)

        send_copy(index).wait_send()

        @pl.when(index + STAGE_SLOTS < parts)
        def _():
            begin_stage(index + STAGE_SLOTS, 0)

        @pl.when(index >= first_ring)
        def _():
            for late in range(2):
                for copy in ring_copies((index - first_ring) * 2 + late):
                    copy.start()

        return total + grad_sum, put_lane(stat, lane_ids, index // per_group, weight_sum)

    total, stat = lax.fori_loop(0, parts, one_part, (zero, zero))
    stat_ref[...] = stat
    part[...] = total
    slots[me] = part[...]
    share(me, others, part, slots, small_send, small_recv)
    whole = tree_sum([slots[index] for index in range(model_size * data_size)])
    whole = jnp.sum(jnp.sum(whole, axis=1, keepdims=True), axis=0, keepdims=True)
    whole = jnp.broadcast_to(whole, (GROUP, LANES))
    clip_ref[...] = jnp.minimum(1.0, MAX_NORM / jnp.sqrt(whole))

    def finish(chunk, carry):
        for copy in ring_copies(chunk):
            copy.wait()
        return carry

    lax.fori_loop(0, RING, finish, 0)


def moment_kernel(groups, cols, mean_in, weight_in, ring_in, land_in, clip, weight_stat, one_in, two_in, dir_ref, weight_ref, ring, land, one_out, two_out, stat_ref,
                  one_get, two_get, one_put, two_put):
    per_group = cols // CHUNK
    chunks = groups * per_group
    width = MOMENT_WIDTH
    lane_ids = lanes_of()

    def place(chunk):
        return rows(chunk // per_group), pl.ds(pl.multiple_of(lax.rem(chunk, per_group) * CHUNK, CHUNK), CHUNK)

    def gets(chunk):
        slot = lax.rem(chunk, RING)
        at = place(chunk)
        return (pltpu.make_async_copy(one_in.at[at], ring.at[0, slot], one_get.at[slot]), pltpu.make_async_copy(two_in.at[at], ring.at[1, slot], two_get.at[slot]))

    def puts(chunk):
        slot = lax.rem(chunk, RING)
        at = place(chunk)
        return (pltpu.make_async_copy(ring.at[0, slot], one_out.at[at], one_put.at[slot]), pltpu.make_async_copy(ring.at[1, slot], two_out.at[at], two_put.at[slot]))

    def start(copies, priority=0):
        for copy in copies:
            copy.start(priority=priority)

    def wait(copies):
        for copy in copies:
            copy.wait()

    scale = jnp.concatenate([clip[...]] * (width // LANES), axis=1)
    one_scale = (1.0 - BETA_ONE) * scale
    two_scale = (1.0 - BETA_TWO) * scale * scale
    ratio = CORR_TWO ** 0.5 / CORR_ONE
    floor = EPSILON * CORR_TWO ** 0.5

    def one_chunk(chunk, stat):
        slot = lax.rem(chunk, RING)
        row_at = rows(chunk // per_group)
        col_at = lax.rem(chunk, per_group) * CHUNK

        @pl.when(chunk >= RING)
        def _():
            wait(gets(chunk))

        def piece(index, total):
            near = pl.ds(pl.multiple_of(index * width, width), width)
            far = pl.ds(pl.multiple_of(col_at + index * width, width), width)
            mean, weight = dir_ref[row_at, far], weight_ref[row_at, far]
            old_one, old_two = ring[0, slot, :, near], ring[1, slot, :, near]
            new_one = BETA_ONE * old_one + one_scale * mean
            new_two = BETA_TWO * old_two + two_scale * mean * mean
            root = new_two * lax.rsqrt(jnp.maximum(new_two, TINY))
            direction = (new_one * ratio) / (root + floor) + WEIGHT_DECAY * weight
            ring[0, slot, :, near] = new_one
            ring[1, slot, :, near] = new_two
            dir_ref[row_at, far] = direction
            return total + tree_sum([direction[:, at:at + LANES] * direction[:, at:at + LANES] for at in range(0, width, LANES)])

        total = lax.fori_loop(0, CHUNK // width, piece, jnp.zeros((GROUP, LANES), F32))
        start(puts(chunk), priority=1)
        ahead = chunk + RING - LAG

        @pl.when(jnp.logical_and(ahead >= RING, ahead < chunks))
        def _():
            wait(puts(ahead - RING))
            start(gets(ahead))

        return put_lane(stat, lane_ids, chunk // per_group, total)

    stat_ref[0] = lax.fori_loop(0, chunks, one_chunk, jnp.zeros((GROUP, LANES), F32))
    stat_ref[1] = weight_stat[...]

    def finish(chunk, carry):
        wait(puts(chunk))
        return carry

    lax.fori_loop(chunks - RING, chunks, finish, 0)


def segment_sums(values):
    lane_ids = lanes_of()
    row_ids = lax.broadcasted_iota(jnp.int32, (GROUP, LANES), 0)
    kind = lax.rem(lane_ids, 3)
    first = jnp.where(kind == 0, 3, 4)
    second = jnp.where(kind == 0, 4, jnp.where(kind == 1, 7, 8))
    segment = jnp.where(row_ids < first, 0, jnp.where(row_ids < second, 1, 2))
    out = jnp.zeros((GROUP, LANES), F32)
    for index in range(3):
        inside = segment == index
        out = jnp.where(inside, jnp.sum(jnp.where(inside, values, 0.0), axis=0, keepdims=True), out)
    return out


def weight_kernel(sizes, groups, cols, direction, weight, stats, land, rate, ride, slots, packed, spare, send_sem, recv_sem, ride_sem, small_send, small_recv):
    model_size, data_size = sizes
    data = lax.axis_index('data')
    me, others = peers(model_size, data_size)
    peer_device = (lax.axis_index('model'), lax.rem(data + 1, data_size))
    sent = groups - RIDE
    enter(others)
    slots[me] = stats[...]
    share(me, others, stats, slots, small_send, small_recv)
    lane_ids = lanes_of()
    dir_sq = segment_sums(tree_sum([slots[index, 0] for index in range(model_size * data_size)]))
    weight_sq = segment_sums(tree_sum([slots[index, 1] for index in range(model_size * data_size)]))
    rate[0] = LEARN_RATE * (jnp.sqrt(weight_sq) / jnp.sqrt(dir_sq))
    width = 1024

    def send_copy(group):
        slot = lax.rem(group, SEND_SLOTS)
        return pltpu.make_async_remote_copy(src_ref=packed.at[slot], dst_ref=land.at[group], send_sem=send_sem.at[slot], recv_sem=recv_sem.at[group],
                                            device_id=peer_device, device_id_type=MESH)

    def ride_copy(index):
        slot = lax.rem(index, RIDE_SLOTS)
        return pltpu.make_async_copy(spare.at[slot], ride.at[index], ride_sem.at[slot])

    def pack(group, target, slot):
        group_rate = jnp.sum(jnp.where(lane_ids == group, rate[0], 0.0), axis=1, keepdims=True)

        def piece(index, inner):
            at = pl.ds(pl.multiple_of(index * width, width), width)
            target[slot, :, at] = (weight[rows(group), at] - group_rate * direction[rows(group), at]).astype(BF16)
            return inner

        lax.fori_loop(0, cols // width, piece, 0, unroll=2)

    def one_group(group, carry):
        slot = lax.rem(group, SEND_SLOTS)

        @pl.when(group >= SEND_SLOTS)
        def _():
            send_copy(group - SEND_SLOTS).wait_send()

        pack(group, packed, slot)
        send_copy(group).start()

        @pl.when(group < RIDE)
        def _():
            @pl.when(group >= RIDE_SLOTS)
            def _():
                ride_copy(group - RIDE_SLOTS).wait()

            pack(sent + group, spare, lax.rem(group, RIDE_SLOTS))
            ride_copy(group).start()

        return carry

    lax.fori_loop(0, sent, one_group, 0)

    def finish(group, carry):
        send_copy(group).wait_recv()
        return carry

    lax.fori_loop(0, sent, finish, 0)
    for group in range(sent - SEND_SLOTS, sent):
        send_copy(group).wait_send()
    for index in range(RIDE - RIDE_SLOTS, RIDE):
        ride_copy(index).wait()


def write_kernel(sizes, groups, cols, direction, weight, land, rate, params, master, fresh, packed, master_sem, land_sem, own_sem):
    data_size = sizes[1]
    data = lax.axis_index('data')
    peer = lax.rem(data + 1, data_size)
    width = 1024
    lane_ids = lanes_of()
    per_group = cols // WRITE_CHUNK
    chunks = groups * per_group

    def columns(chunk, base):
        return pl.ds(pl.multiple_of(base + lax.rem(chunk, per_group) * WRITE_CHUNK, WRITE_CHUNK), WRITE_CHUNK)

    def puts(chunk):
        slot = lax.rem(chunk, WRITE_SLOTS)
        at = rows(chunk // per_group)
        return (pltpu.make_async_copy(fresh.at[slot], master.at[at, columns(chunk, 0)], master_sem.at[slot]),
                pltpu.make_async_copy(packed.at[slot], params.at[at, columns(chunk, data * cols)], own_sem.at[slot]))

    def land_copy(group):
        return pltpu.make_async_copy(land.at[group], params.at[rows(group), pl.ds(pl.multiple_of(peer * cols, LANES), cols)], land_sem.at[group])

    def one_chunk(chunk, carry):
        slot = lax.rem(chunk, WRITE_SLOTS)
        group = chunk // per_group

        @pl.when(jnp.logical_and(lax.rem(chunk, per_group) == 0, group < groups - RIDE))
        def _():
            land_copy(group).start()

        @pl.when(chunk >= WRITE_SLOTS)
        def _():
            for copy in puts(chunk - WRITE_SLOTS):
                copy.wait()

        group_rate = jnp.sum(jnp.where(lane_ids == group, rate[0], 0.0), axis=1, keepdims=True)

        def piece(index, inner):
            near = pl.ds(pl.multiple_of(index * width, width), width)
            far = pl.ds(pl.multiple_of(lax.rem(chunk, per_group) * WRITE_CHUNK + index * width, width), width)
            new = weight[rows(group), far] - group_rate * direction[rows(group), far]
            fresh[slot, :, near] = new
            packed[slot, :, near] = new.astype(BF16)
            return inner

        lax.fori_loop(0, WRITE_CHUNK // width, piece, 0, unroll=2)
        for priority, copy in enumerate(puts(chunk)):
            copy.start(priority=priority)
        return carry

    lax.fori_loop(0, chunks, one_chunk, 0)

    def finish(group, carry):
        land_copy(group).wait()
        return carry

    lax.fori_loop(0, groups - RIDE, finish, 0)
    for chunk in range(chunks - WRITE_SLOTS, chunks):
        for copy in puts(chunk):
            copy.wait()


def place_kernel(sizes, groups, cols, given, params_in, params, put_sem):
    data_size = sizes[1]
    peer = lax.rem(lax.axis_index('data') + 1, data_size)

    def put(index):
        return pltpu.make_async_copy(given.at[index], params.at[rows(groups - RIDE + index), pl.ds(pl.multiple_of(peer * cols, LANES), cols)], put_sem.at[index])

    def begin(index, carry):
        put(index).start()
        return carry

    def finish(index, carry):
        put(index).wait()
        return carry

    lax.fori_loop(0, RIDE, begin, 0)
    lax.fori_loop(0, RIDE, finish, 0)


def solution(mesh):
    sizes = (mesh.shape['model'], mesh.shape['data'])
    devices = sizes[0] * sizes[1]
    both_axes = ('model', 'data')
    state_spec = P(None, both_axes)
    hbm = pl.BlockSpec(memory_space=pl.ANY)
    vmem = pl.BlockSpec(memory_space=pltpu.VMEM)
    dma = pltpu.SemaphoreType.DMA

    def device_step(local_grads, master, moment_one, moment_two):
        blocks, cols = master.shape
        groups = blocks // GROUP
        kept = pltpu.VMEM((blocks, cols), F32)
        keep = functools.partial(pltpu.with_memory_space_constraint, memory_space=pltpu.VMEM)
        tile = pltpu.VMEM((GROUP, LANES), F32)
        state = jax.ShapeDtypeStruct((blocks, cols), F32)

        landed = pltpu.VMEM((groups - RIDE, GROUP, cols), BF16)
        riding = jax.ShapeDtypeStruct((RIDE, GROUP, cols), BF16)
        ring_shape = pltpu.VMEM((2, RING, GROUP, CHUNK), F32)
        landed = pltpu.VMEM((groups - RIDE, GROUP, cols), BF16)
        riding = jax.ShapeDtypeStruct((RIDE, GROUP, cols), BF16)
        parts = groups * (cols // PART)

        caught = pltpu.VMEM((LAND_SLOTS, GROUP, PART), BF16)

        mean, weight, ring, catch, clip, weight_stat = pl.pallas_call(
            functools.partial(exchange_kernel, sizes, groups, cols),
            out_shape=(kept, kept, ring_shape, caught, tile, tile),
            in_specs=[hbm] * 4,
            out_specs=[vmem] * 6,
            scratch_shapes=[pltpu.VMEM((STAGE_SLOTS, GROUP, PART), BF16), pltpu.VMEM((OWN_SLOTS, GROUP, PART), BF16), pltpu.VMEM((GROUP, LANES), F32), pltpu.VMEM((devices, GROUP, LANES), F32),
                            dma((STAGE_SLOTS,)), dma((STAGE_SLOTS,)), dma((LAND_SLOTS,)), pltpu.SemaphoreType.REGULAR, dma((OWN_SLOTS,)), dma((parts,)), dma((2, RING)), dma((devices,)), dma((devices,))],
            compiler_params=pltpu.CompilerParams(collective_id=0, has_side_effects=True, vmem_limit_bytes=SCOPE),
            name='exchange',
        )(local_grads, master, moment_one, moment_two)

        direction, weight, _, _, new_one, new_two, stats = pl.pallas_call(
            functools.partial(moment_kernel, groups, cols),
            out_shape=(kept, kept, ring_shape, caught, state, state, pltpu.VMEM((2, GROUP, LANES), F32)),
            in_specs=[vmem] * 6 + [hbm] * 2,
            out_specs=[vmem, vmem, vmem, vmem, hbm, hbm, vmem],
            input_output_aliases={0: 0, 1: 1, 2: 2, 3: 3},
            scratch_shapes=[dma((RING,))] * 4,
            compiler_params=pltpu.CompilerParams(vmem_limit_bytes=SCOPE),
            name='moments',
        )(mean, weight, ring, catch, keep(clip), keep(weight_stat), moment_one, moment_two)

        land, rate, ride = pl.pallas_call(
            functools.partial(weight_kernel, sizes, groups, cols),
            out_shape=(landed, pltpu.VMEM((2, GROUP, LANES), F32), riding),
            in_specs=[vmem] * 3,
            out_specs=[vmem, vmem, hbm],
            input_output_aliases={2: 1},
            scratch_shapes=[pltpu.VMEM((devices, 2, GROUP, LANES), F32), pltpu.VMEM((SEND_SLOTS, GROUP, cols), BF16), pltpu.VMEM((RIDE_SLOTS, GROUP, cols), BF16),
                            dma((SEND_SLOTS,)), dma((groups - RIDE,)), dma((RIDE_SLOTS,)), dma((devices,)), dma((devices,))],
            compiler_params=pltpu.CompilerParams(collective_id=1, has_side_effects=True, vmem_limit_bytes=SCOPE),
            name='weights',
        )(keep(direction), keep(weight), keep(stats))

        given = lax.ppermute(ride, 'data', [(rank, (rank + 1) % sizes[1]) for rank in range(sizes[1])])

        params, new_master = pl.pallas_call(
            functools.partial(write_kernel, sizes, groups, cols),
            out_shape=(jax.ShapeDtypeStruct((blocks, sizes[1] * cols), BF16), state),
            in_specs=[vmem] * 4,
            out_specs=[hbm, hbm],
            scratch_shapes=[pltpu.VMEM((WRITE_SLOTS, GROUP, WRITE_CHUNK), F32), pltpu.VMEM((WRITE_SLOTS, GROUP, WRITE_CHUNK), BF16),
                            dma((WRITE_SLOTS,)), dma((groups,)), dma((WRITE_SLOTS,))],
            compiler_params=pltpu.CompilerParams(vmem_limit_bytes=SCOPE),
            name='write',
        )(keep(direction), keep(weight), keep(land), keep(rate))
        params = pl.pallas_call(
            functools.partial(place_kernel, sizes, groups, cols),
            out_shape=jax.ShapeDtypeStruct((blocks, sizes[1] * cols), BF16),
            in_specs=[vmem, hbm],
            out_specs=hbm,
            input_output_aliases={1: 0},
            scratch_shapes=[dma((RIDE,))],
            compiler_params=pltpu.CompilerParams(vmem_limit_bytes=SCOPE),
            name='place',
        )(keep(given), params)
        return params, new_master, new_one, new_two

    return jax.shard_map(device_step, mesh=mesh, in_specs=(P('data', None, 'model'), state_spec, state_spec, state_spec),
                         out_specs=(P(None, 'model'), state_spec, state_spec, state_spec), check_vma=False)
```

```python
import functools

import jax
import jax.numpy as jnp
from jax import lax
from jax.experimental import pallas as pl
from jax.experimental.pallas import tpu as pltpu
from jax.sharding import PartitionSpec as P

STEP = 4
LEARN_RATE = 0.08
BETA_ONE = 0.9
BETA_TWO = 0.999
EPSILON = 1e-6
WEIGHT_DECAY = 0.01
MAX_NORM = 1.0
CORR_ONE = 1.0 - BETA_ONE ** STEP
CORR_TWO = 1.0 - BETA_TWO ** STEP
TINY = 1.2e-38

MESH = pl.DeviceIdType.MESH
F32 = jnp.float32
BF16 = jnp.bfloat16
SCOPE = 4000 << 10
LANES = 128
GROUP = 8

PART = 32768
AHEAD = 2
LAND_SLOTS = 4
STAGE_SLOTS = 4
OWN_SLOTS = 3
RING = 20
LAG = 8
MOMENT_WIDTH = 4096
MEAN_WIDTH = 2048
CHUNK = 8192
SEND_SLOTS = 4
RIDE = 16
RIDE_SLOTS = 2
WRITE_SLOTS = 5
WRITE_CHUNK = 16384


def rows(group):
    return pl.ds(pl.multiple_of(group * GROUP, GROUP), GROUP)


def lanes_of():
    return lax.broadcasted_iota(jnp.int32, (GROUP, LANES), 1)


def put_lane(tile, lane_ids, lane, partial):
    row_sum = jnp.sum(partial, axis=1, keepdims=True)
    return tile + jnp.where(lane_ids == lane, row_sum, 0.0)


def tree_sum(values):
    while len(values) > 1:
        values = [a + b for a, b in zip(values[::2], values[1::2])] + ([values[-1]] if len(values) % 2 else [])
    return values[0]


def peers(model_size, data_size):
    model, data = lax.axis_index('model'), lax.axis_index('data')
    out = []
    for step in range(1, model_size * data_size):
        peer_model = lax.rem(model + step // data_size, model_size)
        peer_data = lax.rem(data + step % data_size, data_size)
        out.append(((peer_model, peer_data), peer_model * data_size + peer_data))
    return model * data_size + data, out


def enter(others):
    barrier = pltpu.get_barrier_semaphore()
    for device, _ in others:
        pl.semaphore_signal(barrier, inc=1, device_id=device, device_id_type=MESH)
    pl.semaphore_wait(barrier, len(others))


def share(me, others, source, slots, send_sem, recv_sem):
    copies = []
    for device, index in others:
        copy = pltpu.make_async_remote_copy(src_ref=source, dst_ref=slots.at[me], send_sem=send_sem.at[index], recv_sem=recv_sem.at[me], device_id=device, device_id_type=MESH)
        copy.start()
        copies.append(copy)
    for device, index in others:
        pltpu.make_async_remote_copy(src_ref=source, dst_ref=slots.at[index], send_sem=send_sem.at[index], recv_sem=recv_sem.at[index], device_id=device, device_id_type=MESH).wait_recv()
    for copy in copies:
        copy.wait_send()


def exchange_kernel(sizes, groups, cols, grads, master, one_in, two_in, mean_ref, weight_ref, ring, land, clip_ref, stat_ref, stage, own, part, slots,
                    stage_sem, send_sem, recv_sem, free_sem, own_sem, weight_sem, ring_sem, small_send, small_recv):
    model_size, data_size = sizes
    data = lax.axis_index('data')
    me, others = peers(model_size, data_size)
    peer = lax.rem(data + 1, data_size)
    peer_device = (lax.axis_index('model'), peer)
    per_group = cols // PART
    parts = groups * per_group

    def columns(index, base):
        return pl.ds(pl.multiple_of(base + lax.rem(index, per_group) * PART, PART), PART)

    def own_copy(index):
        slot = lax.rem(index, OWN_SLOTS)
        return pltpu.make_async_copy(grads.at[0, rows(index // per_group), columns(index, data * cols)], own.at[slot], own_sem.at[slot])

    def weight_copy(index):
        at = (rows(index // per_group), columns(index, 0))
        return pltpu.make_async_copy(master.at[at], weight_ref.at[at], weight_sem.at[index])

    def stage_copy(index):
        slot = lax.rem(index, STAGE_SLOTS)
        return pltpu.make_async_copy(grads.at[0, rows(index // per_group), columns(index, peer * cols)], stage.at[slot], stage_sem.at[slot])

    def send_copy(index):
        from_slot, to_slot = lax.rem(index, STAGE_SLOTS), lax.rem(index, LAND_SLOTS)
        return pltpu.make_async_remote_copy(src_ref=stage.at[from_slot], dst_ref=land.at[to_slot], send_sem=send_sem.at[from_slot], recv_sem=recv_sem.at[to_slot],
                                            device_id=peer_device, device_id_type=MESH)

    def ring_copies(chunk):
        at = (rows(chunk // (cols // CHUNK)), pl.ds(pl.multiple_of(lax.rem(chunk, cols // CHUNK) * CHUNK, CHUNK), CHUNK))
        return (pltpu.make_async_copy(one_in.at[at], ring.at[0, chunk], ring_sem.at[0, chunk]), pltpu.make_async_copy(two_in.at[at], ring.at[1, chunk], ring_sem.at[1, chunk]))

    def begin_stage(index, carry):
        stage_copy(index).start()
        return carry

    def begin_own(index, carry):
        own_copy(index).start()
        weight_copy(index).start()
        return carry

    def begin_send(index, carry):
        stage_copy(index).wait()
        send_copy(index).start()
        return carry

    lax.fori_loop(0, STAGE_SLOTS, begin_stage, 0)
    lax.fori_loop(0, OWN_SLOTS, begin_own, 0)
    enter(others)
    lax.fori_loop(0, AHEAD, begin_send, 0)
    lane_ids = lanes_of()
    width = MEAN_WIDTH
    zero = jnp.zeros((GROUP, LANES), F32)
    first_ring = parts - RING // 4

    def one_part(index, carry):
        total, stat = carry
        own_slot, land_slot = lax.rem(index, OWN_SLOTS), lax.rem(index, LAND_SLOTS)
        row_at = rows(index // per_group)
        col_at = lax.rem(index, per_group) * PART

        @pl.when(jnp.logical_and(index + AHEAD >= LAND_SLOTS, index + AHEAD < parts))
        def _():
            pl.semaphore_wait(free_sem, 1)

        @pl.when(index + AHEAD < parts)
        def _():
            begin_send(index + AHEAD, 0)

        own_copy(index).wait()
        weight_copy(index).wait()
        send_copy(index).wait_recv()

        def piece(step, sums):
            grad_sum, weight_sum = sums
            near = pl.ds(pl.multiple_of(step * width, width), width)
            far = pl.ds(pl.multiple_of(col_at + step * width, width), width)
            weight = weight_ref[row_at, far]
            mean = (own[own_slot, :, near].astype(F32) + land[land_slot, :, near].astype(F32)) * 0.5
            mean_ref[row_at, far] = mean
            cuts = range(0, width, LANES)
            grad_sum += tree_sum([mean[:, at:at + LANES] * mean[:, at:at + LANES] for at in cuts])
            weight_sum += tree_sum([weight[:, at:at + LANES] * weight[:, at:at + LANES] for at in cuts])
            return grad_sum, weight_sum

        grad_sum, weight_sum = lax.fori_loop(0, PART // width, piece, (zero, zero))

        @pl.when(index + LAND_SLOTS < parts)
        def _():
            pl.semaphore_signal(free_sem, inc=1, device_id=peer_device, device_id_type=MESH)

        @pl.when(index + OWN_SLOTS < parts)
        def _():
            begin_own(index + OWN_SLOTS, 0)

        send_copy(index).wait_send()

        @pl.when(index + STAGE_SLOTS < parts)
        def _():
            begin_stage(index + STAGE_SLOTS, 0)

        @pl.when(index >= first_ring)
        def _():
            for late in range(4):
                for copy in ring_copies((index - first_ring) * 4 + late):
                    copy.start()

        return total + grad_sum, put_lane(stat, lane_ids, index // per_group, weight_sum)

    total, stat = lax.fori_loop(0, parts, one_part, (zero, zero))
    stat_ref[...] = stat
    part[...] = total
    slots[me] = part[...]
    share(me, others, part, slots, small_send, small_recv)
    whole = tree_sum([slots[index] for index in range(model_size * data_size)])
    whole = jnp.sum(jnp.sum(whole, axis=1, keepdims=True), axis=0, keepdims=True)
    whole = jnp.broadcast_to(whole, (GROUP, LANES))
    clip_ref[...] = jnp.minimum(1.0, MAX_NORM / jnp.sqrt(whole))

    def finish(chunk, carry):
        for copy in ring_copies(chunk):
            copy.wait()
        return carry

    lax.fori_loop(0, RING, finish, 0)


def moment_kernel(groups, cols, mean_in, weight_in, ring_in, land_in, clip, weight_stat, one_in, two_in, dir_ref, weight_ref, ring, land, one_out, two_out, stat_ref,
                  one_get, two_get, one_put, two_put):
    per_group = cols // CHUNK
    chunks = groups * per_group
    width = MOMENT_WIDTH
    lane_ids = lanes_of()

    def place(chunk):
        return rows(chunk // per_group), pl.ds(pl.multiple_of(lax.rem(chunk, per_group) * CHUNK, CHUNK), CHUNK)

    def gets(chunk):
        slot = lax.rem(chunk, RING)
        at = place(chunk)
        return (pltpu.make_async_copy(one_in.at[at], ring.at[0, slot], one_get.at[slot]), pltpu.make_async_copy(two_in.at[at], ring.at[1, slot], two_get.at[slot]))

    def puts(chunk):
        slot = lax.rem(chunk, RING)
        at = place(chunk)
        return (pltpu.make_async_copy(ring.at[0, slot], one_out.at[at], one_put.at[slot]), pltpu.make_async_copy(ring.at[1, slot], two_out.at[at], two_put.at[slot]))

    def start(copies, priority=0):
        for copy in copies:
            copy.start(priority=priority)

    def wait(copies):
        for copy in copies:
            copy.wait()

    scale = jnp.concatenate([clip[...]] * (width // LANES), axis=1)
    one_scale = (1.0 - BETA_ONE) * scale
    two_scale = (1.0 - BETA_TWO) * scale * scale
    ratio = CORR_TWO ** 0.5 / CORR_ONE
    floor = EPSILON * CORR_TWO ** 0.5

    def one_chunk(chunk, stat):
        slot = lax.rem(chunk, RING)
        row_at = rows(chunk // per_group)
        col_at = lax.rem(chunk, per_group) * CHUNK

        @pl.when(chunk >= RING)
        def _():
            wait(gets(chunk))

        def piece(index, total):
            near = pl.ds(pl.multiple_of(index * width, width), width)
            far = pl.ds(pl.multiple_of(col_at + index * width, width), width)
            mean, weight = dir_ref[row_at, far], weight_ref[row_at, far]
            old_one, old_two = ring[0, slot, :, near], ring[1, slot, :, near]
            new_one = BETA_ONE * old_one + one_scale * mean
            new_two = BETA_TWO * old_two + two_scale * mean * mean
            root = new_two * lax.rsqrt(jnp.maximum(new_two, TINY))
            direction = (new_one * ratio) / (root + floor) + WEIGHT_DECAY * weight
            ring[0, slot, :, near] = new_one
            ring[1, slot, :, near] = new_two
            dir_ref[row_at, far] = direction
            return total + tree_sum([direction[:, at:at + LANES] * direction[:, at:at + LANES] for at in range(0, width, LANES)])

        total = lax.fori_loop(0, CHUNK // width, piece, jnp.zeros((GROUP, LANES), F32))
        start(puts(chunk), priority=1)
        ahead = chunk + RING - LAG

        @pl.when(jnp.logical_and(ahead >= RING, ahead < chunks))
        def _():
            wait(puts(ahead - RING))
            start(gets(ahead))

        return put_lane(stat, lane_ids, chunk // per_group, total)

    stat_ref[0] = lax.fori_loop(0, chunks, one_chunk, jnp.zeros((GROUP, LANES), F32))
    stat_ref[1] = weight_stat[...]

    def finish(chunk, carry):
        wait(puts(chunk))
        return carry

    lax.fori_loop(chunks - RING, chunks, finish, 0)


def segment_sums(values):
    lane_ids = lanes_of()
    row_ids = lax.broadcasted_iota(jnp.int32, (GROUP, LANES), 0)
    kind = lax.rem(lane_ids, 3)
    first = jnp.where(kind == 0, 3, 4)
    second = jnp.where(kind == 0, 4, jnp.where(kind == 1, 7, 8))
    segment = jnp.where(row_ids < first, 0, jnp.where(row_ids < second, 1, 2))
    out = jnp.zeros((GROUP, LANES), F32)
    for index in range(3):
        inside = segment == index
        out = jnp.where(inside, jnp.sum(jnp.where(inside, values, 0.0), axis=0, keepdims=True), out)
    return out


def weight_kernel(sizes, groups, cols, direction, weight, stats, land, rate, ride, slots, packed, spare, send_sem, recv_sem, ride_sem, small_send, small_recv):
    model_size, data_size = sizes
    data = lax.axis_index('data')
    me, others = peers(model_size, data_size)
    peer_device = (lax.axis_index('model'), lax.rem(data + 1, data_size))
    sent = groups - RIDE
    enter(others)
    slots[me] = stats[...]
    share(me, others, stats, slots, small_send, small_recv)
    lane_ids = lanes_of()
    dir_sq = segment_sums(tree_sum([slots[index, 0] for index in range(model_size * data_size)]))
    weight_sq = segment_sums(tree_sum([slots[index, 1] for index in range(model_size * data_size)]))
    rate[0] = LEARN_RATE * (jnp.sqrt(weight_sq) / jnp.sqrt(dir_sq))
    width = 1024

    def send_copy(group):
        slot = lax.rem(group, SEND_SLOTS)
        return pltpu.make_async_remote_copy(src_ref=packed.at[slot], dst_ref=land.at[group], send_sem=send_sem.at[slot], recv_sem=recv_sem.at[group],
                                            device_id=peer_device, device_id_type=MESH)

    def ride_copy(index):
        slot = lax.rem(index, RIDE_SLOTS)
        return pltpu.make_async_copy(spare.at[slot], ride.at[index], ride_sem.at[slot])

    def pack(group, target, slot):
        group_rate = jnp.sum(jnp.where(lane_ids == group, rate[0], 0.0), axis=1, keepdims=True)

        def piece(index, inner):
            at = pl.ds(pl.multiple_of(index * width, width), width)
            target[slot, :, at] = (weight[rows(group), at] - group_rate * direction[rows(group), at]).astype(BF16)
            return inner

        lax.fori_loop(0, cols // width, piece, 0, unroll=2)

    def one_group(group, carry):
        slot = lax.rem(group, SEND_SLOTS)

        @pl.when(group >= SEND_SLOTS)
        def _():
            send_copy(group - SEND_SLOTS).wait_send()

        pack(group, packed, slot)
        send_copy(group).start()

        def one_ride(index, inner):
            @pl.when(index >= RIDE_SLOTS)
            def _():
                ride_copy(index - RIDE_SLOTS).wait()

            pack(sent + index, spare, lax.rem(index, RIDE_SLOTS))
            ride_copy(index).start()
            return inner

        lax.fori_loop(group * RIDE // sent, (group + 1) * RIDE // sent, one_ride, 0)
        return carry

    lax.fori_loop(0, sent, one_group, 0)

    def finish(group, carry):
        send_copy(group).wait_recv()
        return carry

    lax.fori_loop(0, sent, finish, 0)
    for group in range(sent - SEND_SLOTS, sent):
        send_copy(group).wait_send()
    for index in range(RIDE - RIDE_SLOTS, RIDE):
        ride_copy(index).wait()


def write_kernel(sizes, groups, cols, direction, weight, land, rate, params, master, fresh, packed, master_sem, land_sem, own_sem):
    data_size = sizes[1]
    data = lax.axis_index('data')
    peer = lax.rem(data + 1, data_size)
    width = 1024
    lane_ids = lanes_of()
    per_group = cols // WRITE_CHUNK
    chunks = groups * per_group

    def columns(chunk, base):
        return pl.ds(pl.multiple_of(base + lax.rem(chunk, per_group) * WRITE_CHUNK, WRITE_CHUNK), WRITE_CHUNK)

    def puts(chunk):
        slot = lax.rem(chunk, WRITE_SLOTS)
        at = rows(chunk // per_group)
        return (pltpu.make_async_copy(fresh.at[slot], master.at[at, columns(chunk, 0)], master_sem.at[slot]),
                pltpu.make_async_copy(packed.at[slot], params.at[at, columns(chunk, data * cols)], own_sem.at[slot]))

    def land_copy(group):
        return pltpu.make_async_copy(land.at[group], params.at[rows(group), pl.ds(pl.multiple_of(peer * cols, LANES), cols)], land_sem.at[group])

    def one_chunk(chunk, carry):
        slot = lax.rem(chunk, WRITE_SLOTS)
        group = chunk // per_group

        @pl.when(jnp.logical_and(lax.rem(chunk, per_group) == 0, group < groups - RIDE))
        def _():
            land_copy(group).start()

        @pl.when(chunk >= WRITE_SLOTS)
        def _():
            for copy in puts(chunk - WRITE_SLOTS):
                copy.wait()

        group_rate = jnp.sum(jnp.where(lane_ids == group, rate[0], 0.0), axis=1, keepdims=True)

        def piece(index, inner):
            near = pl.ds(pl.multiple_of(index * width, width), width)
            far = pl.ds(pl.multiple_of(lax.rem(chunk, per_group) * WRITE_CHUNK + index * width, width), width)
            new = weight[rows(group), far] - group_rate * direction[rows(group), far]
            fresh[slot, :, near] = new
            packed[slot, :, near] = new.astype(BF16)
            return inner

        lax.fori_loop(0, WRITE_CHUNK // width, piece, 0, unroll=2)
        for priority, copy in enumerate(puts(chunk)):
            copy.start(priority=priority)
        return carry

    lax.fori_loop(0, chunks, one_chunk, 0)

    def finish(group, carry):
        land_copy(group).wait()
        return carry

    lax.fori_loop(0, groups - RIDE, finish, 0)
    for chunk in range(chunks - WRITE_SLOTS, chunks):
        for copy in puts(chunk):
            copy.wait()


def place_kernel(sizes, groups, cols, given, params_in, params, put_sem):
    data_size = sizes[1]
    peer = lax.rem(lax.axis_index('data') + 1, data_size)

    def put(index):
        return pltpu.make_async_copy(given.at[index], params.at[rows(groups - RIDE + index), pl.ds(pl.multiple_of(peer * cols, LANES), cols)], put_sem.at[index])

    def begin(index, carry):
        put(index).start()
        return carry

    def finish(index, carry):
        put(index).wait()
        return carry

    lax.fori_loop(0, RIDE, begin, 0)
    lax.fori_loop(0, RIDE, finish, 0)


def solution(mesh):
    sizes = (mesh.shape['model'], mesh.shape['data'])
    devices = sizes[0] * sizes[1]
    both_axes = ('model', 'data')
    state_spec = P(None, both_axes)
    hbm = pl.BlockSpec(memory_space=pl.ANY)
    vmem = pl.BlockSpec(memory_space=pltpu.VMEM)
    dma = pltpu.SemaphoreType.DMA

    def device_step(local_grads, master, moment_one, moment_two):
        blocks, cols = master.shape
        groups = blocks // GROUP
        kept = pltpu.VMEM((blocks, cols), F32)
        keep = functools.partial(pltpu.with_memory_space_constraint, memory_space=pltpu.VMEM)
        tile = pltpu.VMEM((GROUP, LANES), F32)
        state = jax.ShapeDtypeStruct((blocks, cols), F32)

        landed = pltpu.VMEM((groups - RIDE, GROUP, cols), BF16)
        riding = jax.ShapeDtypeStruct((RIDE, GROUP, cols), BF16)
        ring_shape = pltpu.VMEM((2, RING, GROUP, CHUNK), F32)
        landed = pltpu.VMEM((groups - RIDE, GROUP, cols), BF16)
        riding = jax.ShapeDtypeStruct((RIDE, GROUP, cols), BF16)
        parts = groups * (cols // PART)

        caught = pltpu.VMEM((LAND_SLOTS, GROUP, PART), BF16)

        mean, weight, ring, catch, clip, weight_stat = pl.pallas_call(
            functools.partial(exchange_kernel, sizes, groups, cols),
            out_shape=(kept, kept, ring_shape, caught, tile, tile),
            in_specs=[hbm] * 4,
            out_specs=[vmem] * 6,
            scratch_shapes=[pltpu.VMEM((STAGE_SLOTS, GROUP, PART), BF16), pltpu.VMEM((OWN_SLOTS, GROUP, PART), BF16), pltpu.VMEM((GROUP, LANES), F32), pltpu.VMEM((devices, GROUP, LANES), F32),
                            dma((STAGE_SLOTS,)), dma((STAGE_SLOTS,)), dma((LAND_SLOTS,)), pltpu.SemaphoreType.REGULAR, dma((OWN_SLOTS,)), dma((parts,)), dma((2, RING)), dma((devices,)), dma((devices,))],
            compiler_params=pltpu.CompilerParams(collective_id=0, has_side_effects=True, vmem_limit_bytes=SCOPE),
            name='exchange',
        )(local_grads, master, moment_one, moment_two)

        direction, weight, _, _, new_one, new_two, stats = pl.pallas_call(
            functools.partial(moment_kernel, groups, cols),
            out_shape=(kept, kept, ring_shape, caught, state, state, pltpu.VMEM((2, GROUP, LANES), F32)),
            in_specs=[vmem] * 6 + [hbm] * 2,
            out_specs=[vmem, vmem, vmem, vmem, hbm, hbm, vmem],
            input_output_aliases={0: 0, 1: 1, 2: 2, 3: 3},
            scratch_shapes=[dma((RING,))] * 4,
            compiler_params=pltpu.CompilerParams(vmem_limit_bytes=SCOPE),
            name='moments',
        )(mean, weight, ring, catch, keep(clip), keep(weight_stat), moment_one, moment_two)

        land, rate, ride = pl.pallas_call(
            functools.partial(weight_kernel, sizes, groups, cols),
            out_shape=(landed, pltpu.VMEM((2, GROUP, LANES), F32), riding),
            in_specs=[vmem] * 3,
            out_specs=[vmem, vmem, hbm],
            input_output_aliases={2: 1},
            scratch_shapes=[pltpu.VMEM((devices, 2, GROUP, LANES), F32), pltpu.VMEM((SEND_SLOTS, GROUP, cols), BF16), pltpu.VMEM((RIDE_SLOTS, GROUP, cols), BF16),
                            dma((SEND_SLOTS,)), dma((groups - RIDE,)), dma((RIDE_SLOTS,)), dma((devices,)), dma((devices,))],
            compiler_params=pltpu.CompilerParams(collective_id=1, has_side_effects=True, vmem_limit_bytes=SCOPE),
            name='weights',
        )(keep(direction), keep(weight), keep(stats))

        given = lax.ppermute(ride, 'data', [(rank, (rank + 1) % sizes[1]) for rank in range(sizes[1])])

        params, new_master = pl.pallas_call(
            functools.partial(write_kernel, sizes, groups, cols),
            out_shape=(jax.ShapeDtypeStruct((blocks, sizes[1] * cols), BF16), state),
            in_specs=[vmem] * 4,
            out_specs=[hbm, hbm],
            scratch_shapes=[pltpu.VMEM((WRITE_SLOTS, GROUP, WRITE_CHUNK), F32), pltpu.VMEM((WRITE_SLOTS, GROUP, WRITE_CHUNK), BF16),
                            dma((WRITE_SLOTS,)), dma((groups,)), dma((WRITE_SLOTS,))],
            compiler_params=pltpu.CompilerParams(vmem_limit_bytes=SCOPE),
            name='write',
        )(keep(direction), keep(weight), keep(land), keep(rate))
        params = pl.pallas_call(
            functools.partial(place_kernel, sizes, groups, cols),
            out_shape=jax.ShapeDtypeStruct((blocks, sizes[1] * cols), BF16),
            in_specs=[vmem, hbm],
            out_specs=hbm,
            input_output_aliases={1: 0},
            scratch_shapes=[dma((RIDE,))],
            compiler_params=pltpu.CompilerParams(vmem_limit_bytes=SCOPE),
            name='place',
        )(keep(given), params)
        return params, new_master, new_one, new_two

    return jax.shard_map(device_step, mesh=mesh, in_specs=(P('data', None, 'model'), state_spec, state_spec, state_spec),
                         out_specs=(P(None, 'model'), state_spec, state_spec, state_spec), check_vma=False)
```

```python
import functools

import jax
import jax.numpy as jnp
from jax import lax
from jax.experimental import pallas as pl
from jax.experimental.pallas import tpu as pltpu
from jax.sharding import PartitionSpec as P

STEP = 4
LEARN_RATE = 0.08
BETA_ONE = 0.9
BETA_TWO = 0.999
EPSILON = 1e-6
WEIGHT_DECAY = 0.01
MAX_NORM = 1.0
CORR_ONE = 1.0 - BETA_ONE ** STEP
CORR_TWO = 1.0 - BETA_TWO ** STEP
TINY = 1.2e-38

MESH = pl.DeviceIdType.MESH
F32 = jnp.float32
BF16 = jnp.bfloat16
SCOPE = 4000 << 10
LANES = 128
GROUP = 8

PART = 16384
AHEAD = 4
LAND_SLOTS = 8
STAGE_SLOTS = 12
OWN_SLOTS = 7
RING = 18
LAG = 7
MOMENT_WIDTH = 4096
MEAN_WIDTH = 2048
CHUNK = 8192
SEND_SLOTS = 3
RIDE = 17
RIDE_SLOTS = 4
WRITE_SLOTS = 5
WRITE_CHUNK = 16384


def rows(group):
    return pl.ds(pl.multiple_of(group * GROUP, GROUP), GROUP)


def lanes_of():
    return lax.broadcasted_iota(jnp.int32, (GROUP, LANES), 1)


def put_lane(tile, lane_ids, lane, partial):
    row_sum = jnp.sum(partial, axis=1, keepdims=True)
    return tile + jnp.where(lane_ids == lane, row_sum, 0.0)


def tree_sum(values):
    while len(values) > 1:
        values = [a + b for a, b in zip(values[::2], values[1::2])] + ([values[-1]] if len(values) % 2 else [])
    return values[0]


def peers(model_size, data_size):
    model, data = lax.axis_index('model'), lax.axis_index('data')
    out = []
    for step in range(1, model_size * data_size):
        peer_model = lax.rem(model + step // data_size, model_size)
        peer_data = lax.rem(data + step % data_size, data_size)
        out.append(((peer_model, peer_data), peer_model * data_size + peer_data))
    return model * data_size + data, out


def enter(others):
    barrier = pltpu.get_barrier_semaphore()
    for device, _ in others:
        pl.semaphore_signal(barrier, inc=1, device_id=device, device_id_type=MESH)
    pl.semaphore_wait(barrier, len(others))


def share(me, others, source, slots, send_sem, recv_sem):
    copies = []
    for device, index in others:
        copy = pltpu.make_async_remote_copy(src_ref=source, dst_ref=slots.at[me], send_sem=send_sem.at[index], recv_sem=recv_sem.at[me], device_id=device, device_id_type=MESH)
        copy.start()
        copies.append(copy)
    for device, index in others:
        pltpu.make_async_remote_copy(src_ref=source, dst_ref=slots.at[index], send_sem=send_sem.at[index], recv_sem=recv_sem.at[index], device_id=device, device_id_type=MESH).wait_recv()
    for copy in copies:
        copy.wait_send()


def exchange_kernel(sizes, groups, cols, grads, master, one_in, two_in, mean_ref, weight_ref, ring, stage, clip_ref, stat_ref, land, own, part, slots,
                    stage_sem, send_sem, recv_sem, free_sem, own_sem, weight_sem, ring_sem, small_send, small_recv):
    model_size, data_size = sizes
    data = lax.axis_index('data')
    me, others = peers(model_size, data_size)
    peer = lax.rem(data + 1, data_size)
    peer_device = (lax.axis_index('model'), peer)
    per_group = cols // PART
    parts = groups * per_group

    def columns(index, base):
        return pl.ds(pl.multiple_of(base + lax.rem(index, per_group) * PART, PART), PART)

    def own_copy(index):
        slot = lax.rem(index, OWN_SLOTS)
        return pltpu.make_async_copy(grads.at[0, rows(index // per_group), columns(index, data * cols)], own.at[slot], own_sem.at[slot])

    def weight_copy(index):
        at = (rows(index // per_group), columns(index, 0))
        return pltpu.make_async_copy(master.at[at], weight_ref.at[at], weight_sem.at[index])

    def stage_copy(index):
        slot = lax.rem(index, STAGE_SLOTS)
        return pltpu.make_async_copy(grads.at[0, rows(index // per_group), columns(index, peer * cols)], stage.at[slot], stage_sem.at[slot])

    def send_copy(index):
        from_slot, to_slot = lax.rem(index, STAGE_SLOTS), lax.rem(index, LAND_SLOTS)
        return pltpu.make_async_remote_copy(src_ref=stage.at[from_slot], dst_ref=land.at[to_slot], send_sem=send_sem.at[from_slot], recv_sem=recv_sem.at[to_slot],
                                            device_id=peer_device, device_id_type=MESH)

    def ring_copies(chunk):
        at = (rows(chunk // (cols // CHUNK)), pl.ds(pl.multiple_of(lax.rem(chunk, cols // CHUNK) * CHUNK, CHUNK), CHUNK))
        return (pltpu.make_async_copy(one_in.at[at], ring.at[0, chunk], ring_sem.at[0, chunk]), pltpu.make_async_copy(two_in.at[at], ring.at[1, chunk], ring_sem.at[1, chunk]))

    def begin_stage(index, carry):
        stage_copy(index).start()
        return carry

    def begin_own(index, carry):
        own_copy(index).start()
        weight_copy(index).start()
        return carry

    def begin_send(index, carry):
        stage_copy(index).wait()
        send_copy(index).start()
        return carry

    lax.fori_loop(0, STAGE_SLOTS, begin_stage, 0)
    lax.fori_loop(0, OWN_SLOTS, begin_own, 0)
    enter(others)
    lax.fori_loop(0, AHEAD, begin_send, 0)
    lane_ids = lanes_of()
    width = MEAN_WIDTH
    zero = jnp.zeros((GROUP, LANES), F32)
    first_ring = parts - RING // 2

    def one_part(index, carry):
        total, stat = carry
        own_slot, land_slot = lax.rem(index, OWN_SLOTS), lax.rem(index, LAND_SLOTS)
        row_at = rows(index // per_group)
        col_at = lax.rem(index, per_group) * PART

        @pl.when(jnp.logical_and(index + AHEAD >= LAND_SLOTS, index + AHEAD < parts))
        def _():
            pl.semaphore_wait(free_sem, 1)

        @pl.when(index + AHEAD < parts)
        def _():
            begin_send(index + AHEAD, 0)

        own_copy(index).wait()
        weight_copy(index).wait()
        send_copy(index).wait_recv()

        def piece(step, sums):
            grad_sum, weight_sum = sums
            near = pl.ds(pl.multiple_of(step * width, width), width)
            far = pl.ds(pl.multiple_of(col_at + step * width, width), width)
            weight = weight_ref[row_at, far]
            mean = (own[own_slot, :, near].astype(F32) + land[land_slot, :, near].astype(F32)) * 0.5
            mean_ref[row_at, far] = mean
            cuts = range(0, width, LANES)
            grad_sum += tree_sum([mean[:, at:at + LANES] * mean[:, at:at + LANES] for at in cuts])
            weight_sum += tree_sum([weight[:, at:at + LANES] * weight[:, at:at + LANES] for at in cuts])
            return grad_sum, weight_sum

        grad_sum, weight_sum = lax.fori_loop(0, PART // width, piece, (zero, zero))

        @pl.when(index + LAND_SLOTS < parts)
        def _():
            pl.semaphore_signal(free_sem, inc=1, device_id=peer_device, device_id_type=MESH)

        @pl.when(index + OWN_SLOTS < parts)
        def _():
            begin_own(index + OWN_SLOTS, 0)

        send_copy(index).wait_send()

        @pl.when(index + STAGE_SLOTS < parts)
        def _():
            begin_stage(index + STAGE_SLOTS, 0)

        @pl.when(index >= first_ring)
        def _():
            for late in range(2):
                for copy in ring_copies((index - first_ring) * 2 + late):
                    copy.start()

        return total + grad_sum, put_lane(stat, lane_ids, index // per_group, weight_sum)

    total, stat = lax.fori_loop(0, parts, one_part, (zero, zero))
    stat_ref[...] = stat
    part[...] = total
    slots[me] = part[...]
    share(me, others, part, slots, small_send, small_recv)
    whole = tree_sum([slots[index] for index in range(model_size * data_size)])
    whole = jnp.sum(jnp.sum(whole, axis=1, keepdims=True), axis=0, keepdims=True)
    whole = jnp.broadcast_to(whole, (GROUP, LANES))
    clip_ref[...] = jnp.minimum(1.0, MAX_NORM / jnp.sqrt(whole))

    def finish(chunk, carry):
        for copy in ring_copies(chunk):
            copy.wait()
        return carry

    lax.fori_loop(0, RING, finish, 0)


def moment_kernel(groups, cols, mean_in, weight_in, ring_in, stage_in, clip, weight_stat, one_in, two_in, dir_ref, weight_ref, ring, stage, one_out, two_out, stat_ref,
                  one_get, two_get, one_put, two_put):
    per_group = cols // CHUNK
    chunks = groups * per_group
    width = MOMENT_WIDTH
    lane_ids = lanes_of()

    def place(chunk):
        return rows(chunk // per_group), pl.ds(pl.multiple_of(lax.rem(chunk, per_group) * CHUNK, CHUNK), CHUNK)

    def gets(chunk):
        slot = lax.rem(chunk, RING)
        at = place(chunk)
        return (pltpu.make_async_copy(one_in.at[at], ring.at[0, slot], one_get.at[slot]), pltpu.make_async_copy(two_in.at[at], ring.at[1, slot], two_get.at[slot]))

    def puts(chunk):
        slot = lax.rem(chunk, RING)
        at = place(chunk)
        return (pltpu.make_async_copy(ring.at[0, slot], one_out.at[at], one_put.at[slot]), pltpu.make_async_copy(ring.at[1, slot], two_out.at[at], two_put.at[slot]))

    def start(copies, priority=0):
        for copy in copies:
            copy.start(priority=priority)

    def wait(copies):
        for copy in copies:
            copy.wait()

    scale = jnp.concatenate([clip[...]] * (width // LANES), axis=1)
    one_scale = (1.0 - BETA_ONE) * scale
    two_scale = (1.0 - BETA_TWO) * scale * scale
    ratio = CORR_TWO ** 0.5 / CORR_ONE
    floor = EPSILON * CORR_TWO ** 0.5

    def one_chunk(chunk, stat):
        slot = lax.rem(chunk, RING)
        row_at = rows(chunk // per_group)
        col_at = lax.rem(chunk, per_group) * CHUNK

        @pl.when(chunk >= RING)
        def _():
            wait(gets(chunk))

        def piece(index, total):
            near = pl.ds(pl.multiple_of(index * width, width), width)
            far = pl.ds(pl.multiple_of(col_at + index * width, width), width)
            mean, weight = dir_ref[row_at, far], weight_ref[row_at, far]
            old_one, old_two = ring[0, slot, :, near], ring[1, slot, :, near]
            new_one = BETA_ONE * old_one + one_scale * mean
            new_two = BETA_TWO * old_two + two_scale * mean * mean
            root = new_two * lax.rsqrt(jnp.maximum(new_two, TINY))
            direction = (new_one * ratio) / (root + floor) + WEIGHT_DECAY * weight
            ring[0, slot, :, near] = new_one
            ring[1, slot, :, near] = new_two
            dir_ref[row_at, far] = direction
            return total + tree_sum([direction[:, at:at + LANES] * direction[:, at:at + LANES] for at in range(0, width, LANES)])

        total = lax.fori_loop(0, CHUNK // width, piece, jnp.zeros((GROUP, LANES), F32))
        start(puts(chunk), priority=1)
        ahead = chunk + RING - LAG

        @pl.when(jnp.logical_and(ahead >= RING, ahead < chunks))
        def _():
            wait(puts(ahead - RING))
            start(gets(ahead))

        return put_lane(stat, lane_ids, chunk // per_group, total)

    stat_ref[0] = lax.fori_loop(0, chunks, one_chunk, jnp.zeros((GROUP, LANES), F32))
    stat_ref[1] = weight_stat[...]

    def finish(chunk, carry):
        wait(puts(chunk))
        return carry

    lax.fori_loop(chunks - RING, chunks, finish, 0)


def segment_sums(values):
    lane_ids = lanes_of()
    row_ids = lax.broadcasted_iota(jnp.int32, (GROUP, LANES), 0)
    kind = lax.rem(lane_ids, 3)
    first = jnp.where(kind == 0, 3, 4)
    second = jnp.where(kind == 0, 4, jnp.where(kind == 1, 7, 8))
    segment = jnp.where(row_ids < first, 0, jnp.where(row_ids < second, 1, 2))
    out = jnp.zeros((GROUP, LANES), F32)
    for index in range(3):
        inside = segment == index
        out = jnp.where(inside, jnp.sum(jnp.where(inside, values, 0.0), axis=0, keepdims=True), out)
    return out


def weight_kernel(sizes, groups, cols, direction, weight, stats, land, rate, ride, slots, packed, spare, send_sem, recv_sem, ride_sem, small_send, small_recv):
    model_size, data_size = sizes
    data = lax.axis_index('data')
    me, others = peers(model_size, data_size)
    peer_device = (lax.axis_index('model'), lax.rem(data + 1, data_size))
    sent = groups - RIDE
    enter(others)
    slots[me] = stats[...]
    share(me, others, stats, slots, small_send, small_recv)
    lane_ids = lanes_of()
    dir_sq = segment_sums(tree_sum([slots[index, 0] for index in range(model_size * data_size)]))
    weight_sq = segment_sums(tree_sum([slots[index, 1] for index in range(model_size * data_size)]))
    rate[0] = LEARN_RATE * (jnp.sqrt(weight_sq) / jnp.sqrt(dir_sq))
    width = 1024

    def send_copy(group):
        slot = lax.rem(group, SEND_SLOTS)
        return pltpu.make_async_remote_copy(src_ref=packed.at[slot], dst_ref=land.at[group], send_sem=send_sem.at[slot], recv_sem=recv_sem.at[group],
                                            device_id=peer_device, device_id_type=MESH)

    def ride_copy(index):
        slot = lax.rem(index, RIDE_SLOTS)
        return pltpu.make_async_copy(spare.at[slot], ride.at[index], ride_sem.at[slot])

    def pack(group, target, slot):
        group_rate = jnp.sum(jnp.where(lane_ids == group, rate[0], 0.0), axis=1, keepdims=True)

        def piece(index, inner):
            at = pl.ds(pl.multiple_of(index * width, width), width)
            target[slot, :, at] = (weight[rows(group), at] - group_rate * direction[rows(group), at]).astype(BF16)
            return inner

        lax.fori_loop(0, cols // width, piece, 0, unroll=2)

    def one_group(group, carry):
        slot = lax.rem(group, SEND_SLOTS)

        @pl.when(group >= SEND_SLOTS)
        def _():
            send_copy(group - SEND_SLOTS).wait_send()

        pack(group, packed, slot)
        send_copy(group).start()

        def one_ride(index, inner):
            @pl.when(index >= RIDE_SLOTS)
            def _():
                ride_copy(index - RIDE_SLOTS).wait()

            pack(sent + index, spare, lax.rem(index, RIDE_SLOTS))
            ride_copy(index).start()
            return inner

        lax.fori_loop(group * RIDE // sent, (group + 1) * RIDE // sent, one_ride, 0)
        return carry

    lax.fori_loop(0, sent, one_group, 0)

    def finish(group, carry):
        send_copy(group).wait_recv()
        return carry

    lax.fori_loop(0, sent, finish, 0)
    for group in range(sent - SEND_SLOTS, sent):
        send_copy(group).wait_send()
    for index in range(RIDE - RIDE_SLOTS, RIDE):
        ride_copy(index).wait()


def write_kernel(sizes, groups, cols, direction, weight, land, rate, params, master, fresh, packed, master_sem, land_sem, own_sem):
    data_size = sizes[1]
    data = lax.axis_index('data')
    peer = lax.rem(data + 1, data_size)
    width = 1024
    lane_ids = lanes_of()
    per_group = cols // WRITE_CHUNK
    chunks = groups * per_group

    def columns(chunk, base):
        return pl.ds(pl.multiple_of(base + lax.rem(chunk, per_group) * WRITE_CHUNK, WRITE_CHUNK), WRITE_CHUNK)

    def puts(chunk):
        slot = lax.rem(chunk, WRITE_SLOTS)
        at = rows(chunk // per_group)
        return (pltpu.make_async_copy(fresh.at[slot], master.at[at, columns(chunk, 0)], master_sem.at[slot]),
                pltpu.make_async_copy(packed.at[slot], params.at[at, columns(chunk, data * cols)], own_sem.at[slot]))

    def land_copy(group):
        return pltpu.make_async_copy(land.at[group], params.at[rows(group), pl.ds(pl.multiple_of(peer * cols, LANES), cols)], land_sem.at[group])

    def one_chunk(chunk, carry):
        slot = lax.rem(chunk, WRITE_SLOTS)
        group = chunk // per_group

        @pl.when(jnp.logical_and(lax.rem(chunk, per_group) == 0, group < groups - RIDE))
        def _():
            land_copy(group).start()

        @pl.when(chunk >= WRITE_SLOTS)
        def _():
            for copy in puts(chunk - WRITE_SLOTS):
                copy.wait()

        group_rate = jnp.sum(jnp.where(lane_ids == group, rate[0], 0.0), axis=1, keepdims=True)

        def piece(index, inner):
            near = pl.ds(pl.multiple_of(index * width, width), width)
            far = pl.ds(pl.multiple_of(lax.rem(chunk, per_group) * WRITE_CHUNK + index * width, width), width)
            new = weight[rows(group), far] - group_rate * direction[rows(group), far]
            fresh[slot, :, near] = new
            packed[slot, :, near] = new.astype(BF16)
            return inner

        lax.fori_loop(0, WRITE_CHUNK // width, piece, 0, unroll=2)
        for priority, copy in enumerate(puts(chunk)):
            copy.start(priority=priority)
        return carry

    lax.fori_loop(0, chunks, one_chunk, 0)

    def finish(group, carry):
        land_copy(group).wait()
        return carry

    lax.fori_loop(0, groups - RIDE, finish, 0)
    for chunk in range(chunks - WRITE_SLOTS, chunks):
        for copy in puts(chunk):
            copy.wait()


def place_kernel(sizes, groups, cols, given, params_in, params, put_sem):
    data_size = sizes[1]
    peer = lax.rem(lax.axis_index('data') + 1, data_size)

    def put(index):
        return pltpu.make_async_copy(given.at[index], params.at[rows(groups - RIDE + index), pl.ds(pl.multiple_of(peer * cols, LANES), cols)], put_sem.at[index])

    def begin(index, carry):
        put(index).start()
        return carry

    def finish(index, carry):
        put(index).wait()
        return carry

    lax.fori_loop(0, RIDE, begin, 0)
    lax.fori_loop(0, RIDE, finish, 0)


def solution(mesh):
    sizes = (mesh.shape['model'], mesh.shape['data'])
    devices = sizes[0] * sizes[1]
    both_axes = ('model', 'data')
    state_spec = P(None, both_axes)
    hbm = pl.BlockSpec(memory_space=pl.ANY)
    vmem = pl.BlockSpec(memory_space=pltpu.VMEM)
    dma = pltpu.SemaphoreType.DMA

    def device_step(local_grads, master, moment_one, moment_two):
        blocks, cols = master.shape
        groups = blocks // GROUP
        kept = pltpu.VMEM((blocks, cols), F32)
        keep = functools.partial(pltpu.with_memory_space_constraint, memory_space=pltpu.VMEM)
        tile = pltpu.VMEM((GROUP, LANES), F32)
        state = jax.ShapeDtypeStruct((blocks, cols), F32)

        landed = pltpu.VMEM((groups - RIDE, GROUP, cols), BF16)
        riding = jax.ShapeDtypeStruct((RIDE, GROUP, cols), BF16)
        ring_shape = pltpu.VMEM((2, RING, GROUP, CHUNK), F32)
        landed = pltpu.VMEM((groups - RIDE, GROUP, cols), BF16)
        riding = jax.ShapeDtypeStruct((RIDE, GROUP, cols), BF16)
        parts = groups * (cols // PART)

        staged = pltpu.VMEM((STAGE_SLOTS, GROUP, PART), BF16)

        mean, weight, ring, stage, clip, weight_stat = pl.pallas_call(
            functools.partial(exchange_kernel, sizes, groups, cols),
            out_shape=(kept, kept, ring_shape, staged, tile, tile),
            in_specs=[hbm] * 4,
            out_specs=[vmem] * 6,
            scratch_shapes=[pltpu.VMEM((LAND_SLOTS, GROUP, PART), BF16), pltpu.VMEM((OWN_SLOTS, GROUP, PART), BF16), pltpu.VMEM((GROUP, LANES), F32), pltpu.VMEM((devices, GROUP, LANES), F32),
                            dma((STAGE_SLOTS,)), dma((STAGE_SLOTS,)), dma((LAND_SLOTS,)), pltpu.SemaphoreType.REGULAR, dma((OWN_SLOTS,)), dma((parts,)), dma((2, RING)), dma((devices,)), dma((devices,))],
            compiler_params=pltpu.CompilerParams(collective_id=0, has_side_effects=True, vmem_limit_bytes=SCOPE),
            name='exchange',
        )(local_grads, master, moment_one, moment_two)

        direction, weight, _, _, new_one, new_two, stats = pl.pallas_call(
            functools.partial(moment_kernel, groups, cols),
            out_shape=(kept, kept, ring_shape, staged, state, state, pltpu.VMEM((2, GROUP, LANES), F32)),
            in_specs=[vmem] * 6 + [hbm] * 2,
            out_specs=[vmem, vmem, vmem, vmem, hbm, hbm, vmem],
            input_output_aliases={0: 0, 1: 1, 2: 2, 3: 3},
            scratch_shapes=[dma((RING,))] * 4,
            compiler_params=pltpu.CompilerParams(vmem_limit_bytes=SCOPE),
            name='moments',
        )(mean, weight, ring, stage, keep(clip), keep(weight_stat), moment_one, moment_two)

        land, rate, ride = pl.pallas_call(
            functools.partial(weight_kernel, sizes, groups, cols),
            out_shape=(landed, pltpu.VMEM((2, GROUP, LANES), F32), riding),
            in_specs=[vmem] * 3,
            out_specs=[vmem, vmem, hbm],
            input_output_aliases={2: 1},
            scratch_shapes=[pltpu.VMEM((devices, 2, GROUP, LANES), F32), pltpu.VMEM((SEND_SLOTS, GROUP, cols), BF16), pltpu.VMEM((RIDE_SLOTS, GROUP, cols), BF16),
                            dma((SEND_SLOTS,)), dma((groups - RIDE,)), dma((RIDE_SLOTS,)), dma((devices,)), dma((devices,))],
            compiler_params=pltpu.CompilerParams(collective_id=1, has_side_effects=True, vmem_limit_bytes=SCOPE),
            name='weights',
        )(keep(direction), keep(weight), keep(stats))

        given = lax.ppermute(ride, 'data', [(rank, (rank + 1) % sizes[1]) for rank in range(sizes[1])])

        params, new_master = pl.pallas_call(
            functools.partial(write_kernel, sizes, groups, cols),
            out_shape=(jax.ShapeDtypeStruct((blocks, sizes[1] * cols), BF16), state),
            in_specs=[vmem] * 4,
            out_specs=[hbm, hbm],
            scratch_shapes=[pltpu.VMEM((WRITE_SLOTS, GROUP, WRITE_CHUNK), F32), pltpu.VMEM((WRITE_SLOTS, GROUP, WRITE_CHUNK), BF16),
                            dma((WRITE_SLOTS,)), dma((groups,)), dma((WRITE_SLOTS,))],
            compiler_params=pltpu.CompilerParams(vmem_limit_bytes=SCOPE),
            name='write',
        )(keep(direction), keep(weight), keep(land), keep(rate))
        params = pl.pallas_call(
            functools.partial(place_kernel, sizes, groups, cols),
            out_shape=jax.ShapeDtypeStruct((blocks, sizes[1] * cols), BF16),
            in_specs=[vmem, hbm],
            out_specs=hbm,
            input_output_aliases={1: 0},
            scratch_shapes=[dma((RIDE,))],
            compiler_params=pltpu.CompilerParams(vmem_limit_bytes=SCOPE),
            name='place',
        )(keep(given), params)
        return params, new_master, new_one, new_two

    return jax.shard_map(device_step, mesh=mesh, in_specs=(P('data', None, 'model'), state_spec, state_spec, state_spec),
                         out_specs=(P(None, 'model'), state_spec, state_spec, state_spec), check_vma=False)
```

```python
import functools

import jax
import jax.numpy as jnp
from jax import lax
from jax.experimental import pallas as pl
from jax.experimental.pallas import tpu as pltpu
from jax.sharding import PartitionSpec as P

STEP = 4
LEARN_RATE = 0.08
BETA_ONE = 0.9
BETA_TWO = 0.999
EPSILON = 1e-6
WEIGHT_DECAY = 0.01
MAX_NORM = 1.0
CORR_ONE = 1.0 - BETA_ONE ** STEP
CORR_TWO = 1.0 - BETA_TWO ** STEP
TINY = 1.2e-38

MESH = pl.DeviceIdType.MESH
F32 = jnp.float32
BF16 = jnp.bfloat16
SCOPE = 4000 << 10
LANES = 128
GROUP = 8

PART = 16384
AHEAD = 4
LAND_SLOTS = 8
STAGE_SLOTS = 12
OWN_SLOTS = 6
RING = 18
LAG = 7
MOMENT_WIDTH = 4096
MEAN_WIDTH = 4096
PACK_WIDTH = 4096
CHUNK = 8192
SEND_SLOTS = 3
RIDE = 17
RIDE_SLOTS = 3
WRITE_SLOTS = 5
WRITE_CHUNK = 16384


def rows(group):
    return pl.ds(pl.multiple_of(group * GROUP, GROUP), GROUP)


def lanes_of():
    return lax.broadcasted_iota(jnp.int32, (GROUP, LANES), 1)


def put_lane(tile, lane_ids, lane, partial):
    row_sum = jnp.sum(partial, axis=1, keepdims=True)
    return tile + jnp.where(lane_ids == lane, row_sum, 0.0)


def swap(values):
    parts = [values[:, at:at + LANES] for at in range(0, values.shape[1], LANES)]
    return jnp.concatenate([parts[index ^ 1] for index in range(len(parts))], axis=1)


def tree_sum(values):
    while len(values) > 1:
        values = [a + b for a, b in zip(values[::2], values[1::2])] + ([values[-1]] if len(values) % 2 else [])
    return values[0]


def peers(model_size, data_size):
    model, data = lax.axis_index('model'), lax.axis_index('data')
    out = []
    for step in range(1, model_size * data_size):
        peer_model = lax.rem(model + step // data_size, model_size)
        peer_data = lax.rem(data + step % data_size, data_size)
        out.append(((peer_model, peer_data), peer_model * data_size + peer_data))
    return model * data_size + data, out


def enter(others):
    barrier = pltpu.get_barrier_semaphore()
    for device, _ in others:
        pl.semaphore_signal(barrier, inc=1, device_id=device, device_id_type=MESH)
    pl.semaphore_wait(barrier, len(others))


def share(me, others, source, slots, send_sem, recv_sem):
    copies = []
    for device, index in others:
        copy = pltpu.make_async_remote_copy(src_ref=source, dst_ref=slots.at[me], send_sem=send_sem.at[index], recv_sem=recv_sem.at[me], device_id=device, device_id_type=MESH)
        copy.start()
        copies.append(copy)
    for device, index in others:
        pltpu.make_async_remote_copy(src_ref=source, dst_ref=slots.at[index], send_sem=send_sem.at[index], recv_sem=recv_sem.at[index], device_id=device, device_id_type=MESH).wait_recv()
    for copy in copies:
        copy.wait_send()


def exchange_kernel(sizes, groups, cols, grads, master, one_in, two_in, mean_ref, weight_ref, ring, stage, clip_ref, stat_ref, land, own, part, slots,
                    stage_sem, send_sem, recv_sem, free_sem, own_sem, weight_sem, ring_sem, small_send, small_recv):
    model_size, data_size = sizes
    data = lax.axis_index('data')
    me, others = peers(model_size, data_size)
    peer = lax.rem(data + 1, data_size)
    peer_device = (lax.axis_index('model'), peer)
    per_group = cols // PART
    parts = groups * per_group

    def columns(index, base):
        return pl.ds(pl.multiple_of(base + lax.rem(index, per_group) * PART, PART), PART)

    def own_copy(index):
        slot = lax.rem(index, OWN_SLOTS)
        return pltpu.make_async_copy(grads.at[0, rows(index // per_group), columns(index, data * cols)], own.at[slot], own_sem.at[slot])

    def weight_copy(index):
        at = (rows(index // per_group), columns(index, 0))
        return pltpu.make_async_copy(master.at[at], weight_ref.at[at], weight_sem.at[index])

    def stage_copy(index):
        slot = lax.rem(index, STAGE_SLOTS)
        return pltpu.make_async_copy(grads.at[0, rows(index // per_group), columns(index, peer * cols)], stage.at[slot], stage_sem.at[slot])

    def send_copy(index):
        from_slot, to_slot = lax.rem(index, STAGE_SLOTS), lax.rem(index, LAND_SLOTS)
        return pltpu.make_async_remote_copy(src_ref=stage.at[from_slot], dst_ref=land.at[to_slot], send_sem=send_sem.at[from_slot], recv_sem=recv_sem.at[to_slot],
                                            device_id=peer_device, device_id_type=MESH)

    def ring_copies(chunk):
        at = (rows(chunk // (cols // CHUNK)), pl.ds(pl.multiple_of(lax.rem(chunk, cols // CHUNK) * CHUNK, CHUNK), CHUNK))
        return (pltpu.make_async_copy(one_in.at[at], ring.at[0, chunk], ring_sem.at[0, chunk]), pltpu.make_async_copy(two_in.at[at], ring.at[1, chunk], ring_sem.at[1, chunk]))

    def begin_stage(index, carry):
        stage_copy(index).start()
        return carry

    def begin_own(index, carry):
        own_copy(index).start()
        weight_copy(index).start()
        return carry

    def begin_send(index, carry):
        stage_copy(index).wait()
        send_copy(index).start()
        return carry

    lax.fori_loop(0, STAGE_SLOTS, begin_stage, 0)
    lax.fori_loop(0, OWN_SLOTS, begin_own, 0)
    enter(others)
    lax.fori_loop(0, AHEAD, begin_send, 0)
    lane_ids = lanes_of()
    width = MEAN_WIDTH
    zero = jnp.zeros((GROUP, LANES), F32)
    first_ring = parts - RING // 2

    def one_part(index, carry):
        total, stat = carry
        own_slot, land_slot = lax.rem(index, OWN_SLOTS), lax.rem(index, LAND_SLOTS)
        row_at = rows(index // per_group)
        col_at = lax.rem(index, per_group) * PART

        @pl.when(jnp.logical_and(index + AHEAD >= LAND_SLOTS, index + AHEAD < parts))
        def _():
            pl.semaphore_wait(free_sem, 1)

        @pl.when(index + AHEAD < parts)
        def _():
            begin_send(index + AHEAD, 0)

        own_copy(index).wait()
        weight_copy(index).wait()
        send_copy(index).wait_recv()

        def piece(step, sums):
            grad_sum, weight_sum = sums
            near = pl.ds(pl.multiple_of(step * width, width), width)
            far = pl.ds(pl.multiple_of(col_at + step * width, width), width)
            weight = weight_ref[row_at, far]
            mean = (own[own_slot, :, near].astype(F32) + land[land_slot, :, near].astype(F32)) * 0.5
            mean_ref[row_at, far] = swap(mean)
            cuts = range(0, width, LANES)
            grad_sum += tree_sum([mean[:, at:at + LANES] * mean[:, at:at + LANES] for at in cuts])
            weight_sum += tree_sum([weight[:, at:at + LANES] * weight[:, at:at + LANES] for at in cuts])
            return grad_sum, weight_sum

        grad_sum, weight_sum = lax.fori_loop(0, PART // width, piece, (zero, zero))

        @pl.when(index + LAND_SLOTS < parts)
        def _():
            pl.semaphore_signal(free_sem, inc=1, device_id=peer_device, device_id_type=MESH)

        @pl.when(index + OWN_SLOTS < parts)
        def _():
            begin_own(index + OWN_SLOTS, 0)

        send_copy(index).wait_send()

        @pl.when(index + STAGE_SLOTS < parts)
        def _():
            begin_stage(index + STAGE_SLOTS, 0)

        @pl.when(index >= first_ring)
        def _():
            for late in range(2):
                for copy in ring_copies((index - first_ring) * 2 + late):
                    copy.start()

        return total + grad_sum, put_lane(stat, lane_ids, index // per_group, weight_sum)

    total, stat = lax.fori_loop(0, parts, one_part, (zero, zero))
    stat_ref[...] = stat
    part[...] = total
    slots[me] = part[...]
    share(me, others, part, slots, small_send, small_recv)
    whole = tree_sum([slots[index] for index in range(model_size * data_size)])
    whole = jnp.sum(jnp.sum(whole, axis=1, keepdims=True), axis=0, keepdims=True)
    whole = jnp.broadcast_to(whole, (GROUP, LANES))
    clip_ref[...] = jnp.minimum(1.0, MAX_NORM / jnp.sqrt(whole))

    def finish(chunk, carry):
        for copy in ring_copies(chunk):
            copy.wait()
        return carry

    lax.fori_loop(0, RING, finish, 0)


def moment_kernel(groups, cols, mean_in, weight_in, ring_in, stage_in, clip, weight_stat, one_in, two_in, dir_ref, weight_ref, ring, stage, one_out, two_out, stat_ref,
                  one_get, two_get, one_put, two_put):
    per_group = cols // CHUNK
    chunks = groups * per_group
    width = MOMENT_WIDTH
    lane_ids = lanes_of()

    def place(chunk):
        return rows(chunk // per_group), pl.ds(pl.multiple_of(lax.rem(chunk, per_group) * CHUNK, CHUNK), CHUNK)

    def gets(chunk):
        slot = lax.rem(chunk, RING)
        at = place(chunk)
        return (pltpu.make_async_copy(one_in.at[at], ring.at[0, slot], one_get.at[slot]), pltpu.make_async_copy(two_in.at[at], ring.at[1, slot], two_get.at[slot]))

    def puts(chunk):
        slot = lax.rem(chunk, RING)
        at = place(chunk)
        return (pltpu.make_async_copy(ring.at[0, slot], one_out.at[at], one_put.at[slot]), pltpu.make_async_copy(ring.at[1, slot], two_out.at[at], two_put.at[slot]))

    def start(copies, priority=0):
        for copy in copies:
            copy.start(priority=priority)

    def wait(copies):
        for copy in copies:
            copy.wait()

    scale = jnp.concatenate([clip[...]] * (width // LANES), axis=1)
    one_scale = (1.0 - BETA_ONE) * scale
    two_scale = (1.0 - BETA_TWO) * scale * scale
    ratio = CORR_TWO ** 0.5 / CORR_ONE
    floor = EPSILON * CORR_TWO ** 0.5

    def one_chunk(chunk, stat):
        slot = lax.rem(chunk, RING)
        row_at = rows(chunk // per_group)
        col_at = lax.rem(chunk, per_group) * CHUNK

        @pl.when(chunk >= RING)
        def _():
            wait(gets(chunk))

        def piece(index, total):
            near = pl.ds(pl.multiple_of(index * width, width), width)
            far = pl.ds(pl.multiple_of(col_at + index * width, width), width)
            mean, weight = swap(dir_ref[row_at, far]), weight_ref[row_at, far]
            old_one, old_two = ring[0, slot, :, near], ring[1, slot, :, near]
            new_one = BETA_ONE * old_one + one_scale * mean
            new_two = BETA_TWO * old_two + two_scale * mean * mean
            root = new_two * lax.rsqrt(jnp.maximum(new_two, TINY))
            direction = (new_one * ratio) / (root + floor) + WEIGHT_DECAY * weight
            ring[0, slot, :, near] = new_one
            ring[1, slot, :, near] = new_two
            dir_ref[row_at, far] = swap(direction)
            return total + tree_sum([direction[:, at:at + LANES] * direction[:, at:at + LANES] for at in range(0, width, LANES)])

        total = lax.fori_loop(0, CHUNK // width, piece, jnp.zeros((GROUP, LANES), F32))
        start(puts(chunk), priority=1)
        ahead = chunk + RING - LAG

        @pl.when(jnp.logical_and(ahead >= RING, ahead < chunks))
        def _():
            wait(puts(ahead - RING))
            start(gets(ahead))

        return put_lane(stat, lane_ids, chunk // per_group, total)

    stat_ref[0] = lax.fori_loop(0, chunks, one_chunk, jnp.zeros((GROUP, LANES), F32))
    stat_ref[1] = weight_stat[...]

    def finish(chunk, carry):
        wait(puts(chunk))
        return carry

    lax.fori_loop(chunks - RING, chunks, finish, 0)


def segment_sums(values):
    lane_ids = lanes_of()
    row_ids = lax.broadcasted_iota(jnp.int32, (GROUP, LANES), 0)
    kind = lax.rem(lane_ids, 3)
    first = jnp.where(kind == 0, 3, 4)
    second = jnp.where(kind == 0, 4, jnp.where(kind == 1, 7, 8))
    segment = jnp.where(row_ids < first, 0, jnp.where(row_ids < second, 1, 2))
    out = jnp.zeros((GROUP, LANES), F32)
    for index in range(3):
        inside = segment == index
        out = jnp.where(inside, jnp.sum(jnp.where(inside, values, 0.0), axis=0, keepdims=True), out)
    return out


def weight_kernel(sizes, groups, cols, direction, weight, stats, land, rate, ride, slots, packed, spare, send_sem, recv_sem, ride_sem, small_send, small_recv):
    model_size, data_size = sizes
    data = lax.axis_index('data')
    me, others = peers(model_size, data_size)
    peer_device = (lax.axis_index('model'), lax.rem(data + 1, data_size))
    sent = groups - RIDE
    enter(others)
    slots[me] = stats[...]
    share(me, others, stats, slots, small_send, small_recv)
    lane_ids = lanes_of()
    dir_sq = segment_sums(tree_sum([slots[index, 0] for index in range(model_size * data_size)]))
    weight_sq = segment_sums(tree_sum([slots[index, 1] for index in range(model_size * data_size)]))
    rate[0] = LEARN_RATE * (jnp.sqrt(weight_sq) / jnp.sqrt(dir_sq))
    width = PACK_WIDTH

    def send_copy(group):
        slot = lax.rem(group, SEND_SLOTS)
        return pltpu.make_async_remote_copy(src_ref=packed.at[slot], dst_ref=land.at[group], send_sem=send_sem.at[slot], recv_sem=recv_sem.at[group],
                                            device_id=peer_device, device_id_type=MESH)

    def ride_copy(index):
        slot = lax.rem(index, RIDE_SLOTS)
        return pltpu.make_async_copy(spare.at[slot], ride.at[index], ride_sem.at[slot])

    def pack(group, target, slot):
        group_rate = jnp.sum(jnp.where(lane_ids == group, rate[0], 0.0), axis=1, keepdims=True)

        def piece(index, inner):
            at = pl.ds(pl.multiple_of(index * width, width), width)
            target[slot, :, at] = (weight[rows(group), at] - group_rate * swap(direction[rows(group), at])).astype(BF16)
            return inner

        lax.fori_loop(0, cols // width, piece, 0)

    def one_group(group, carry):
        slot = lax.rem(group, SEND_SLOTS)

        @pl.when(group >= SEND_SLOTS)
        def _():
            send_copy(group - SEND_SLOTS).wait_send()

        pack(group, packed, slot)
        send_copy(group).start()

        def one_ride(index, inner):
            @pl.when(index >= RIDE_SLOTS)
            def _():
                ride_copy(index - RIDE_SLOTS).wait()

            pack(sent + index, spare, lax.rem(index, RIDE_SLOTS))
            ride_copy(index).start()
            return inner

        lax.fori_loop(group * RIDE // sent, (group + 1) * RIDE // sent, one_ride, 0)
        return carry

    lax.fori_loop(0, sent, one_group, 0)

    def finish(group, carry):
        send_copy(group).wait_recv()
        return carry

    lax.fori_loop(0, sent, finish, 0)
    for group in range(sent - SEND_SLOTS, sent):
        send_copy(group).wait_send()
    for index in range(RIDE - RIDE_SLOTS, RIDE):
        ride_copy(index).wait()


def write_kernel(sizes, groups, cols, direction, weight, land, rate, params, master, fresh, packed, master_sem, land_sem, own_sem):
    data_size = sizes[1]
    data = lax.axis_index('data')
    peer = lax.rem(data + 1, data_size)
    width = PACK_WIDTH
    lane_ids = lanes_of()
    per_group = cols // WRITE_CHUNK
    chunks = groups * per_group

    def columns(chunk, base):
        return pl.ds(pl.multiple_of(base + lax.rem(chunk, per_group) * WRITE_CHUNK, WRITE_CHUNK), WRITE_CHUNK)

    def puts(chunk):
        slot = lax.rem(chunk, WRITE_SLOTS)
        at = rows(chunk // per_group)
        return (pltpu.make_async_copy(fresh.at[slot], master.at[at, columns(chunk, 0)], master_sem.at[slot]),
                pltpu.make_async_copy(packed.at[slot], params.at[at, columns(chunk, data * cols)], own_sem.at[slot]))

    def land_copy(group):
        return pltpu.make_async_copy(land.at[group], params.at[rows(group), pl.ds(pl.multiple_of(peer * cols, LANES), cols)], land_sem.at[group])

    def one_chunk(chunk, carry):
        slot = lax.rem(chunk, WRITE_SLOTS)
        group = chunk // per_group

        @pl.when(jnp.logical_and(lax.rem(chunk, per_group) == 0, group < groups - RIDE))
        def _():
            land_copy(group).start()

        @pl.when(chunk >= WRITE_SLOTS)
        def _():
            for copy in puts(chunk - WRITE_SLOTS):
                copy.wait()

        group_rate = jnp.sum(jnp.where(lane_ids == group, rate[0], 0.0), axis=1, keepdims=True)

        def piece(index, inner):
            near = pl.ds(pl.multiple_of(index * width, width), width)
            far = pl.ds(pl.multiple_of(lax.rem(chunk, per_group) * WRITE_CHUNK + index * width, width), width)
            new = weight[rows(group), far] - group_rate * swap(direction[rows(group), far])
            fresh[slot, :, near] = new
            packed[slot, :, near] = new.astype(BF16)
            return inner

        lax.fori_loop(0, WRITE_CHUNK // width, piece, 0)
        for priority, copy in enumerate(puts(chunk)):
            copy.start(priority=priority)
        return carry

    lax.fori_loop(0, chunks, one_chunk, 0)

    def finish(group, carry):
        land_copy(group).wait()
        return carry

    lax.fori_loop(0, groups - RIDE, finish, 0)
    for chunk in range(chunks - WRITE_SLOTS, chunks):
        for copy in puts(chunk):
            copy.wait()


def place_kernel(sizes, groups, cols, given, params_in, params, put_sem):
    data_size = sizes[1]
    peer = lax.rem(lax.axis_index('data') + 1, data_size)

    def put(index):
        return pltpu.make_async_copy(given.at[index], params.at[rows(groups - RIDE + index), pl.ds(pl.multiple_of(peer * cols, LANES), cols)], put_sem.at[index])

    def begin(index, carry):
        put(index).start()
        return carry

    def finish(index, carry):
        put(index).wait()
        return carry

    lax.fori_loop(0, RIDE, begin, 0)
    lax.fori_loop(0, RIDE, finish, 0)


def solution(mesh):
    sizes = (mesh.shape['model'], mesh.shape['data'])
    devices = sizes[0] * sizes[1]
    both_axes = ('model', 'data')
    state_spec = P(None, both_axes)
    hbm = pl.BlockSpec(memory_space=pl.ANY)
    vmem = pl.BlockSpec(memory_space=pltpu.VMEM)
    dma = pltpu.SemaphoreType.DMA

    def device_step(local_grads, master, moment_one, moment_two):
        blocks, cols = master.shape
        groups = blocks // GROUP
        kept = pltpu.VMEM((blocks, cols), F32)
        keep = functools.partial(pltpu.with_memory_space_constraint, memory_space=pltpu.VMEM)
        tile = pltpu.VMEM((GROUP, LANES), F32)
        state = jax.ShapeDtypeStruct((blocks, cols), F32)

        landed = pltpu.VMEM((groups - RIDE, GROUP, cols), BF16)
        riding = jax.ShapeDtypeStruct((RIDE, GROUP, cols), BF16)
        ring_shape = pltpu.VMEM((2, RING, GROUP, CHUNK), F32)
        landed = pltpu.VMEM((groups - RIDE, GROUP, cols), BF16)
        riding = jax.ShapeDtypeStruct((RIDE, GROUP, cols), BF16)
        parts = groups * (cols // PART)

        staged = pltpu.VMEM((STAGE_SLOTS, GROUP, PART), BF16)

        mean, weight, ring, stage, clip, weight_stat = pl.pallas_call(
            functools.partial(exchange_kernel, sizes, groups, cols),
            out_shape=(kept, kept, ring_shape, staged, tile, tile),
            in_specs=[hbm] * 4,
            out_specs=[vmem] * 6,
            scratch_shapes=[pltpu.VMEM((LAND_SLOTS, GROUP, PART), BF16), pltpu.VMEM((OWN_SLOTS, GROUP, PART), BF16), pltpu.VMEM((GROUP, LANES), F32), pltpu.VMEM((devices, GROUP, LANES), F32),
                            dma((STAGE_SLOTS,)), dma((STAGE_SLOTS,)), dma((LAND_SLOTS,)), pltpu.SemaphoreType.REGULAR, dma((OWN_SLOTS,)), dma((parts,)), dma((2, RING)), dma((devices,)), dma((devices,))],
            compiler_params=pltpu.CompilerParams(collective_id=0, has_side_effects=True, vmem_limit_bytes=SCOPE),
            name='exchange',
        )(local_grads, master, moment_one, moment_two)

        direction, weight, _, _, new_one, new_two, stats = pl.pallas_call(
            functools.partial(moment_kernel, groups, cols),
            out_shape=(kept, kept, ring_shape, staged, state, state, pltpu.VMEM((2, GROUP, LANES), F32)),
            in_specs=[vmem] * 6 + [hbm] * 2,
            out_specs=[vmem, vmem, vmem, vmem, hbm, hbm, vmem],
            input_output_aliases={0: 0, 1: 1, 2: 2, 3: 3},
            scratch_shapes=[dma((RING,))] * 4,
            compiler_params=pltpu.CompilerParams(vmem_limit_bytes=SCOPE),
            name='moments',
        )(mean, weight, ring, stage, keep(clip), keep(weight_stat), moment_one, moment_two)

        land, rate, ride = pl.pallas_call(
            functools.partial(weight_kernel, sizes, groups, cols),
            out_shape=(landed, pltpu.VMEM((2, GROUP, LANES), F32), riding),
            in_specs=[vmem] * 3,
            out_specs=[vmem, vmem, hbm],
            input_output_aliases={2: 1},
            scratch_shapes=[pltpu.VMEM((devices, 2, GROUP, LANES), F32), pltpu.VMEM((SEND_SLOTS, GROUP, cols), BF16), pltpu.VMEM((RIDE_SLOTS, GROUP, cols), BF16),
                            dma((SEND_SLOTS,)), dma((groups - RIDE,)), dma((RIDE_SLOTS,)), dma((devices,)), dma((devices,))],
            compiler_params=pltpu.CompilerParams(collective_id=1, has_side_effects=True, vmem_limit_bytes=SCOPE),
            name='weights',
        )(keep(direction), keep(weight), keep(stats))

        given = lax.ppermute(ride, 'data', [(rank, (rank + 1) % sizes[1]) for rank in range(sizes[1])])

        params, new_master = pl.pallas_call(
            functools.partial(write_kernel, sizes, groups, cols),
            out_shape=(jax.ShapeDtypeStruct((blocks, sizes[1] * cols), BF16), state),
            in_specs=[vmem] * 4,
            out_specs=[hbm, hbm],
            scratch_shapes=[pltpu.VMEM((WRITE_SLOTS, GROUP, WRITE_CHUNK), F32), pltpu.VMEM((WRITE_SLOTS, GROUP, WRITE_CHUNK), BF16),
                            dma((WRITE_SLOTS,)), dma((groups,)), dma((WRITE_SLOTS,))],
            compiler_params=pltpu.CompilerParams(vmem_limit_bytes=SCOPE),
            name='write',
        )(keep(direction), keep(weight), keep(land), keep(rate))
        params = pl.pallas_call(
            functools.partial(place_kernel, sizes, groups, cols),
            out_shape=jax.ShapeDtypeStruct((blocks, sizes[1] * cols), BF16),
            in_specs=[vmem, hbm],
            out_specs=hbm,
            input_output_aliases={1: 0},
            scratch_shapes=[dma((RIDE,))],
            compiler_params=pltpu.CompilerParams(vmem_limit_bytes=SCOPE),
            name='place',
        )(keep(given), params)
        return params, new_master, new_one, new_two

    return jax.shard_map(device_step, mesh=mesh, in_specs=(P('data', None, 'model'), state_spec, state_spec, state_spec),
                         out_specs=(P(None, 'model'), state_spec, state_spec, state_spec), check_vma=False)
```

```python
import functools

import jax
import jax.numpy as jnp
from jax import lax
from jax.experimental import pallas as pl
from jax.experimental.pallas import tpu as pltpu
from jax.sharding import PartitionSpec as P

STEP = 4
LEARN_RATE = 0.08
BETA_ONE = 0.9
BETA_TWO = 0.999
EPSILON = 1e-6
WEIGHT_DECAY = 0.01
MAX_NORM = 1.0
CORR_ONE = 1.0 - BETA_ONE ** STEP
CORR_TWO = 1.0 - BETA_TWO ** STEP
TINY = 1.2e-38

MESH = pl.DeviceIdType.MESH
F32 = jnp.float32
BF16 = jnp.bfloat16
SCOPE = 4000 << 10
LANES = 128
GROUP = 8

PART = 16384
AHEAD = 4
LAND_SLOTS = 8
STAGE_SLOTS = 9
OWN_SLOTS = 6
RING = 20
LAG = 5
MOMENT_WIDTH = 4096
MEAN_WIDTH = 2048
PACK_WIDTH = 8192
CHUNK = 8192
SEND_SLOTS = 3
RIDE = 18
RIDE_SLOTS = 3
WRITE_SLOTS = 5
WRITE_CHUNK = 16384


def rows(group):
    return pl.ds(pl.multiple_of(group * GROUP, GROUP), GROUP)


def lanes_of():
    return lax.broadcasted_iota(jnp.int32, (GROUP, LANES), 1)


def put_lane(tile, lane_ids, lane, partial):
    row_sum = jnp.sum(partial, axis=1, keepdims=True)
    return tile + jnp.where(lane_ids == lane, row_sum, 0.0)


def swap(values):
    parts = [values[:, at:at + LANES] for at in range(0, values.shape[1], LANES)]
    return jnp.concatenate([parts[index ^ 1] for index in range(len(parts))], axis=1)


def tree_sum(values):
    while len(values) > 1:
        values = [a + b for a, b in zip(values[::2], values[1::2])] + ([values[-1]] if len(values) % 2 else [])
    return values[0]


def peers(model_size, data_size):
    model, data = lax.axis_index('model'), lax.axis_index('data')
    out = []
    for step in range(1, model_size * data_size):
        peer_model = lax.rem(model + step // data_size, model_size)
        peer_data = lax.rem(data + step % data_size, data_size)
        out.append(((peer_model, peer_data), peer_model * data_size + peer_data))
    return model * data_size + data, out


def enter(others):
    barrier = pltpu.get_barrier_semaphore()
    for device, _ in others:
        pl.semaphore_signal(barrier, inc=1, device_id=device, device_id_type=MESH)
    pl.semaphore_wait(barrier, len(others))


def share(me, others, source, slots, send_sem, recv_sem):
    copies = []
    for device, index in others:
        copy = pltpu.make_async_remote_copy(src_ref=source, dst_ref=slots.at[me], send_sem=send_sem.at[index], recv_sem=recv_sem.at[me], device_id=device, device_id_type=MESH)
        copy.start()
        copies.append(copy)
    for device, index in others:
        pltpu.make_async_remote_copy(src_ref=source, dst_ref=slots.at[index], send_sem=send_sem.at[index], recv_sem=recv_sem.at[index], device_id=device, device_id_type=MESH).wait_recv()
    for copy in copies:
        copy.wait_send()


def exchange_kernel(sizes, groups, cols, grads, master, one_in, two_in, mean_ref, weight_ref, ring, land, clip_ref, stat_ref, stage, own, part, slots,
                    stage_sem, send_sem, recv_sem, free_sem, own_sem, weight_sem, ring_sem, small_send, small_recv):
    model_size, data_size = sizes
    data = lax.axis_index('data')
    me, others = peers(model_size, data_size)
    peer = lax.rem(data + 1, data_size)
    peer_device = (lax.axis_index('model'), peer)
    per_group = cols // PART
    parts = groups * per_group

    def columns(index, base):
        return pl.ds(pl.multiple_of(base + lax.rem(index, per_group) * PART, PART), PART)

    def own_copy(index):
        slot = lax.rem(index, OWN_SLOTS)
        return pltpu.make_async_copy(grads.at[0, rows(index // per_group), columns(index, data * cols)], own.at[slot], own_sem.at[slot])

    def weight_copy(index):
        at = (rows(index // per_group), columns(index, 0))
        return pltpu.make_async_copy(master.at[at], weight_ref.at[at], weight_sem.at[index])

    def stage_copy(index):
        slot = lax.rem(index, STAGE_SLOTS)
        return pltpu.make_async_copy(grads.at[0, rows(index // per_group), columns(index, peer * cols)], stage.at[slot], stage_sem.at[slot])

    def send_copy(index):
        from_slot, to_slot = lax.rem(index, STAGE_SLOTS), lax.rem(index, LAND_SLOTS)
        return pltpu.make_async_remote_copy(src_ref=stage.at[from_slot], dst_ref=land.at[to_slot], send_sem=send_sem.at[from_slot], recv_sem=recv_sem.at[to_slot],
                                            device_id=peer_device, device_id_type=MESH)

    def ring_copies(chunk):
        at = (rows(chunk // (cols // CHUNK)), pl.ds(pl.multiple_of(lax.rem(chunk, cols // CHUNK) * CHUNK, CHUNK), CHUNK))
        return (pltpu.make_async_copy(one_in.at[at], ring.at[0, chunk], ring_sem.at[0, chunk]), pltpu.make_async_copy(two_in.at[at], ring.at[1, chunk], ring_sem.at[1, chunk]))

    def begin_stage(index, carry):
        stage_copy(index).start()
        return carry

    def begin_own(index, carry):
        own_copy(index).start()
        weight_copy(index).start()
        return carry

    def begin_send(index, carry):
        stage_copy(index).wait()
        send_copy(index).start()
        return carry

    lax.fori_loop(0, STAGE_SLOTS, begin_stage, 0)
    lax.fori_loop(0, OWN_SLOTS, begin_own, 0)
    enter(others)
    lax.fori_loop(0, AHEAD, begin_send, 0)
    lane_ids = lanes_of()
    width = MEAN_WIDTH
    zero = jnp.zeros((GROUP, LANES), F32)
    first_ring = parts - RING // 2

    def one_part(index, carry):
        total, stat = carry
        own_slot, land_slot = lax.rem(index, OWN_SLOTS), lax.rem(index, LAND_SLOTS)
        row_at = rows(index // per_group)
        col_at = lax.rem(index, per_group) * PART

        @pl.when(jnp.logical_and(index + AHEAD >= LAND_SLOTS, index + AHEAD < parts))
        def _():
            pl.semaphore_wait(free_sem, 1)

        @pl.when(index + AHEAD < parts)
        def _():
            begin_send(index + AHEAD, 0)

        own_copy(index).wait()
        weight_copy(index).wait()
        send_copy(index).wait_recv()

        def piece(step, sums):
            grad_sum, weight_sum = sums
            near = pl.ds(pl.multiple_of(step * width, width), width)
            far = pl.ds(pl.multiple_of(col_at + step * width, width), width)
            weight = weight_ref[row_at, far]
            mean = (own[own_slot, :, near].astype(F32) + land[land_slot, :, near].astype(F32)) * 0.5
            mean_ref[row_at, far] = swap(mean)
            cuts = range(0, width, LANES)
            grad_sum += tree_sum([mean[:, at:at + LANES] * mean[:, at:at + LANES] for at in cuts])
            weight_sum += tree_sum([weight[:, at:at + LANES] * weight[:, at:at + LANES] for at in cuts])
            return grad_sum, weight_sum

        grad_sum, weight_sum = lax.fori_loop(0, PART // width, piece, (zero, zero))

        @pl.when(index + LAND_SLOTS < parts)
        def _():
            pl.semaphore_signal(free_sem, inc=1, device_id=peer_device, device_id_type=MESH)

        @pl.when(index + OWN_SLOTS < parts)
        def _():
            begin_own(index + OWN_SLOTS, 0)

        send_copy(index).wait_send()

        @pl.when(index + STAGE_SLOTS < parts)
        def _():
            begin_stage(index + STAGE_SLOTS, 0)

        @pl.when(index >= first_ring)
        def _():
            for late in range(2):
                for copy in ring_copies((index - first_ring) * 2 + late):
                    copy.start()

        return total + grad_sum, put_lane(stat, lane_ids, index // per_group, weight_sum)

    total, stat = lax.fori_loop(0, parts, one_part, (zero, zero))
    stat_ref[...] = stat
    part[...] = total
    slots[me] = part[...]
    share(me, others, part, slots, small_send, small_recv)
    whole = tree_sum([slots[index] for index in range(model_size * data_size)])
    whole = jnp.sum(jnp.sum(whole, axis=1, keepdims=True), axis=0, keepdims=True)
    whole = jnp.broadcast_to(whole, (GROUP, LANES))
    clip_ref[...] = jnp.minimum(1.0, MAX_NORM / jnp.sqrt(whole))

    def finish(chunk, carry):
        for copy in ring_copies(chunk):
            copy.wait()
        return carry

    lax.fori_loop(0, RING, finish, 0)


def moment_kernel(groups, cols, mean_in, weight_in, ring_in, land_in, clip, weight_stat, one_in, two_in, dir_ref, weight_ref, ring, land, one_out, two_out, stat_ref,
                  one_get, two_get, one_put, two_put):
    per_group = cols // CHUNK
    chunks = groups * per_group
    width = MOMENT_WIDTH
    lane_ids = lanes_of()

    def place(chunk):
        return rows(chunk // per_group), pl.ds(pl.multiple_of(lax.rem(chunk, per_group) * CHUNK, CHUNK), CHUNK)

    def gets(chunk):
        slot = lax.rem(chunk, RING)
        at = place(chunk)
        return (pltpu.make_async_copy(one_in.at[at], ring.at[0, slot], one_get.at[slot]), pltpu.make_async_copy(two_in.at[at], ring.at[1, slot], two_get.at[slot]))

    def puts(chunk):
        slot = lax.rem(chunk, RING)
        at = place(chunk)
        return (pltpu.make_async_copy(ring.at[0, slot], one_out.at[at], one_put.at[slot]), pltpu.make_async_copy(ring.at[1, slot], two_out.at[at], two_put.at[slot]))

    def start(copies, priority=0):
        for copy in copies:
            copy.start(priority=priority)

    def wait(copies):
        for copy in copies:
            copy.wait()

    scale = jnp.concatenate([clip[...]] * (width // LANES), axis=1)
    one_scale = (1.0 - BETA_ONE) * scale
    two_scale = (1.0 - BETA_TWO) * scale * scale
    ratio = CORR_TWO ** 0.5 / CORR_ONE
    floor = EPSILON * CORR_TWO ** 0.5

    def one_chunk(chunk, stat):
        slot = lax.rem(chunk, RING)
        row_at = rows(chunk // per_group)
        col_at = lax.rem(chunk, per_group) * CHUNK

        @pl.when(chunk >= RING)
        def _():
            wait(gets(chunk))

        def piece(index, total):
            near = pl.ds(pl.multiple_of(index * width, width), width)
            far = pl.ds(pl.multiple_of(col_at + index * width, width), width)
            mean, weight = swap(dir_ref[row_at, far]), weight_ref[row_at, far]
            old_one, old_two = ring[0, slot, :, near], ring[1, slot, :, near]
            new_one = BETA_ONE * old_one + one_scale * mean
            new_two = BETA_TWO * old_two + two_scale * mean * mean
            root = new_two * lax.rsqrt(jnp.maximum(new_two, TINY))
            direction = (new_one * ratio) / (root + floor) + WEIGHT_DECAY * weight
            ring[0, slot, :, near] = new_one
            ring[1, slot, :, near] = new_two
            dir_ref[row_at, far] = swap(direction)
            return total + tree_sum([direction[:, at:at + LANES] * direction[:, at:at + LANES] for at in range(0, width, LANES)])

        total = lax.fori_loop(0, CHUNK // width, piece, jnp.zeros((GROUP, LANES), F32))
        start(puts(chunk), priority=1)
        ahead = chunk + RING - LAG

        @pl.when(jnp.logical_and(ahead >= RING, ahead < chunks))
        def _():
            wait(puts(ahead - RING))
            start(gets(ahead))

        return put_lane(stat, lane_ids, chunk // per_group, total)

    stat_ref[0] = lax.fori_loop(0, chunks, one_chunk, jnp.zeros((GROUP, LANES), F32))
    stat_ref[1] = weight_stat[...]

    def finish(chunk, carry):
        wait(puts(chunk))
        return carry

    lax.fori_loop(chunks - RING, chunks, finish, 0)


def segment_sums(values):
    lane_ids = lanes_of()
    row_ids = lax.broadcasted_iota(jnp.int32, (GROUP, LANES), 0)
    kind = lax.rem(lane_ids, 3)
    first = jnp.where(kind == 0, 3, 4)
    second = jnp.where(kind == 0, 4, jnp.where(kind == 1, 7, 8))
    segment = jnp.where(row_ids < first, 0, jnp.where(row_ids < second, 1, 2))
    out = jnp.zeros((GROUP, LANES), F32)
    for index in range(3):
        inside = segment == index
        out = jnp.where(inside, jnp.sum(jnp.where(inside, values, 0.0), axis=0, keepdims=True), out)
    return out


def weight_kernel(sizes, groups, cols, direction, weight, stats, land, rate, ride, slots, packed, spare, send_sem, recv_sem, ride_sem, small_send, small_recv):
    model_size, data_size = sizes
    data = lax.axis_index('data')
    me, others = peers(model_size, data_size)
    peer_device = (lax.axis_index('model'), lax.rem(data + 1, data_size))
    sent = groups - RIDE
    enter(others)
    slots[me] = stats[...]
    share(me, others, stats, slots, small_send, small_recv)
    lane_ids = lanes_of()
    dir_sq = segment_sums(tree_sum([slots[index, 0] for index in range(model_size * data_size)]))
    weight_sq = segment_sums(tree_sum([slots[index, 1] for index in range(model_size * data_size)]))
    rate[0] = LEARN_RATE * (jnp.sqrt(weight_sq) / jnp.sqrt(dir_sq))
    width = PACK_WIDTH

    def send_copy(group):
        slot = lax.rem(group, SEND_SLOTS)
        return pltpu.make_async_remote_copy(src_ref=packed.at[slot], dst_ref=land.at[group], send_sem=send_sem.at[slot], recv_sem=recv_sem.at[group],
                                            device_id=peer_device, device_id_type=MESH)

    def ride_copy(index):
        slot = lax.rem(index, RIDE_SLOTS)
        return pltpu.make_async_copy(spare.at[slot], ride.at[index], ride_sem.at[slot])

    def pack(group, target, slot):
        group_rate = jnp.sum(jnp.where(lane_ids == group, rate[0], 0.0), axis=1, keepdims=True)

        def piece(index, inner):
            at = pl.ds(pl.multiple_of(index * width, width), width)
            target[slot, :, at] = (weight[rows(group), at] - group_rate * swap(direction[rows(group), at])).astype(BF16)
            return inner

        lax.fori_loop(0, cols // width, piece, 0)

    def one_group(group, carry):
        slot = lax.rem(group, SEND_SLOTS)

        @pl.when(group >= SEND_SLOTS)
        def _():
            send_copy(group - SEND_SLOTS).wait_send()

        pack(group, packed, slot)
        send_copy(group).start()

        def one_ride(index, inner):
            @pl.when(index >= RIDE_SLOTS)
            def _():
                ride_copy(index - RIDE_SLOTS).wait()

            pack(sent + index, spare, lax.rem(index, RIDE_SLOTS))
            ride_copy(index).start()
            return inner

        lax.fori_loop(group * RIDE // sent, (group + 1) * RIDE // sent, one_ride, 0)
        return carry

    lax.fori_loop(0, sent, one_group, 0)

    def finish(group, carry):
        send_copy(group).wait_recv()
        return carry

    lax.fori_loop(0, sent, finish, 0)
    for group in range(sent - SEND_SLOTS, sent):
        send_copy(group).wait_send()
    for index in range(RIDE - RIDE_SLOTS, RIDE):
        ride_copy(index).wait()


def write_kernel(sizes, groups, cols, direction, weight, land, rate, params, master, fresh, packed, master_sem, land_sem, own_sem):
    data_size = sizes[1]
    data = lax.axis_index('data')
    peer = lax.rem(data + 1, data_size)
    width = 4096
    lane_ids = lanes_of()
    per_group = cols // WRITE_CHUNK
    chunks = groups * per_group

    def columns(chunk, base):
        return pl.ds(pl.multiple_of(base + lax.rem(chunk, per_group) * WRITE_CHUNK, WRITE_CHUNK), WRITE_CHUNK)

    def puts(chunk):
        slot = lax.rem(chunk, WRITE_SLOTS)
        at = rows(chunk // per_group)
        return (pltpu.make_async_copy(fresh.at[slot], master.at[at, columns(chunk, 0)], master_sem.at[slot]),
                pltpu.make_async_copy(packed.at[slot], params.at[at, columns(chunk, data * cols)], own_sem.at[slot]))

    def land_copy(group):
        return pltpu.make_async_copy(land.at[group], params.at[rows(group), pl.ds(pl.multiple_of(peer * cols, LANES), cols)], land_sem.at[group])

    def one_chunk(chunk, carry):
        slot = lax.rem(chunk, WRITE_SLOTS)
        group = chunk // per_group

        @pl.when(jnp.logical_and(lax.rem(chunk, per_group) == 0, group < groups - RIDE))
        def _():
            land_copy(group).start()

        @pl.when(chunk >= WRITE_SLOTS)
        def _():
            for copy in puts(chunk - WRITE_SLOTS):
                copy.wait()

        group_rate = jnp.sum(jnp.where(lane_ids == group, rate[0], 0.0), axis=1, keepdims=True)

        def piece(index, inner):
            near = pl.ds(pl.multiple_of(index * width, width), width)
            far = pl.ds(pl.multiple_of(lax.rem(chunk, per_group) * WRITE_CHUNK + index * width, width), width)
            new = weight[rows(group), far] - group_rate * swap(direction[rows(group), far])
            fresh[slot, :, near] = new
            packed[slot, :, near] = new.astype(BF16)
            return inner

        lax.fori_loop(0, WRITE_CHUNK // width, piece, 0)
        for priority, copy in enumerate(puts(chunk)):
            copy.start(priority=priority)
        return carry

    lax.fori_loop(0, chunks, one_chunk, 0)

    def finish(group, carry):
        land_copy(group).wait()
        return carry

    lax.fori_loop(0, groups - RIDE, finish, 0)
    for chunk in range(chunks - WRITE_SLOTS, chunks):
        for copy in puts(chunk):
            copy.wait()


def place_kernel(sizes, groups, cols, given, params_in, params, put_sem):
    data_size = sizes[1]
    peer = lax.rem(lax.axis_index('data') + 1, data_size)

    def put(index):
        return pltpu.make_async_copy(given.at[index], params.at[rows(groups - RIDE + index), pl.ds(pl.multiple_of(peer * cols, LANES), cols)], put_sem.at[index])

    def begin(index, carry):
        put(index).start()
        return carry

    def finish(index, carry):
        put(index).wait()
        return carry

    lax.fori_loop(0, RIDE, begin, 0)
    lax.fori_loop(0, RIDE, finish, 0)


def solution(mesh):
    sizes = (mesh.shape['model'], mesh.shape['data'])
    devices = sizes[0] * sizes[1]
    both_axes = ('model', 'data')
    state_spec = P(None, both_axes)
    hbm = pl.BlockSpec(memory_space=pl.ANY)
    vmem = pl.BlockSpec(memory_space=pltpu.VMEM)
    dma = pltpu.SemaphoreType.DMA

    def device_step(local_grads, master, moment_one, moment_two):
        blocks, cols = master.shape
        groups = blocks // GROUP
        kept = pltpu.VMEM((blocks, cols), F32)
        keep = functools.partial(pltpu.with_memory_space_constraint, memory_space=pltpu.VMEM)
        tile = pltpu.VMEM((GROUP, LANES), F32)
        state = jax.ShapeDtypeStruct((blocks, cols), F32)

        landed = pltpu.VMEM((groups - RIDE, GROUP, cols), BF16)
        riding = jax.ShapeDtypeStruct((RIDE, GROUP, cols), BF16)
        ring_shape = pltpu.VMEM((2, RING, GROUP, CHUNK), F32)
        landed = pltpu.VMEM((groups - RIDE, GROUP, cols), BF16)
        riding = jax.ShapeDtypeStruct((RIDE, GROUP, cols), BF16)
        parts = groups * (cols // PART)

        caught = pltpu.VMEM((LAND_SLOTS, GROUP, PART), BF16)

        mean, weight, ring, catch, clip, weight_stat = pl.pallas_call(
            functools.partial(exchange_kernel, sizes, groups, cols),
            out_shape=(kept, kept, ring_shape, caught, tile, tile),
            in_specs=[hbm] * 4,
            out_specs=[vmem] * 6,
            scratch_shapes=[pltpu.VMEM((STAGE_SLOTS, GROUP, PART), BF16), pltpu.VMEM((OWN_SLOTS, GROUP, PART), BF16), pltpu.VMEM((GROUP, LANES), F32), pltpu.VMEM((devices, GROUP, LANES), F32),
                            dma((STAGE_SLOTS,)), dma((STAGE_SLOTS,)), dma((LAND_SLOTS,)), pltpu.SemaphoreType.REGULAR, dma((OWN_SLOTS,)), dma((parts,)), dma((2, RING)), dma((devices,)), dma((devices,))],
            compiler_params=pltpu.CompilerParams(collective_id=0, has_side_effects=True, vmem_limit_bytes=SCOPE),
            name='exchange',
        )(local_grads, master, moment_one, moment_two)

        direction, weight, _, _, new_one, new_two, stats = pl.pallas_call(
            functools.partial(moment_kernel, groups, cols),
            out_shape=(kept, kept, ring_shape, caught, state, state, pltpu.VMEM((2, GROUP, LANES), F32)),
            in_specs=[vmem] * 6 + [hbm] * 2,
            out_specs=[vmem, vmem, vmem, vmem, hbm, hbm, vmem],
            input_output_aliases={0: 0, 1: 1, 2: 2, 3: 3},
            scratch_shapes=[dma((RING,))] * 4,
            compiler_params=pltpu.CompilerParams(vmem_limit_bytes=SCOPE),
            name='moments',
        )(mean, weight, ring, catch, keep(clip), keep(weight_stat), moment_one, moment_two)

        land, rate, ride = pl.pallas_call(
            functools.partial(weight_kernel, sizes, groups, cols),
            out_shape=(landed, pltpu.VMEM((2, GROUP, LANES), F32), riding),
            in_specs=[vmem] * 3,
            out_specs=[vmem, vmem, hbm],
            input_output_aliases={2: 1},
            scratch_shapes=[pltpu.VMEM((devices, 2, GROUP, LANES), F32), pltpu.VMEM((SEND_SLOTS, GROUP, cols), BF16), pltpu.VMEM((RIDE_SLOTS, GROUP, cols), BF16),
                            dma((SEND_SLOTS,)), dma((groups - RIDE,)), dma((RIDE_SLOTS,)), dma((devices,)), dma((devices,))],
            compiler_params=pltpu.CompilerParams(collective_id=1, has_side_effects=True, vmem_limit_bytes=SCOPE),
            name='weights',
        )(keep(direction), keep(weight), keep(stats))

        given = lax.ppermute(ride, 'data', [(rank, (rank + 1) % sizes[1]) for rank in range(sizes[1])])

        params, new_master = pl.pallas_call(
            functools.partial(write_kernel, sizes, groups, cols),
            out_shape=(jax.ShapeDtypeStruct((blocks, sizes[1] * cols), BF16), state),
            in_specs=[vmem] * 4,
            out_specs=[hbm, hbm],
            scratch_shapes=[pltpu.VMEM((WRITE_SLOTS, GROUP, WRITE_CHUNK), F32), pltpu.VMEM((WRITE_SLOTS, GROUP, WRITE_CHUNK), BF16),
                            dma((WRITE_SLOTS,)), dma((groups,)), dma((WRITE_SLOTS,))],
            compiler_params=pltpu.CompilerParams(vmem_limit_bytes=SCOPE),
            name='write',
        )(keep(direction), keep(weight), keep(land), keep(rate))
        params = pl.pallas_call(
            functools.partial(place_kernel, sizes, groups, cols),
            out_shape=jax.ShapeDtypeStruct((blocks, sizes[1] * cols), BF16),
            in_specs=[vmem, hbm],
            out_specs=hbm,
            input_output_aliases={1: 0},
            scratch_shapes=[dma((RIDE,))],
            compiler_params=pltpu.CompilerParams(vmem_limit_bytes=SCOPE),
            name='place',
        )(keep(given), params)
        return params, new_master, new_one, new_two

    return jax.shard_map(device_step, mesh=mesh, in_specs=(P('data', None, 'model'), state_spec, state_spec, state_spec),
                         out_specs=(P(None, 'model'), state_spec, state_spec, state_spec), check_vma=False)
```

```python
import functools

import jax
import jax.numpy as jnp
from jax import lax
from jax.experimental import pallas as pl
from jax.experimental.pallas import tpu as pltpu
from jax.sharding import PartitionSpec as P

STEP = 4
LEARN_RATE = 0.08
BETA_ONE = 0.9
BETA_TWO = 0.999
EPSILON = 1e-6
WEIGHT_DECAY = 0.01
MAX_NORM = 1.0
CORR_ONE = 1.0 - BETA_ONE ** STEP
CORR_TWO = 1.0 - BETA_TWO ** STEP
TINY = 1.2e-38

MESH = pl.DeviceIdType.MESH
F32 = jnp.float32
BF16 = jnp.bfloat16
SCOPE = 4000 << 10
LANES = 128
GROUP = 8

PART = 16384
AHEAD = 4
LAND_SLOTS = 8
STAGE_SLOTS = 9
OWN_SLOTS = 6
RING = 20
LAG = 3
MOMENT_WIDTH = 4096
MEAN_WIDTH = 2048
PACK_WIDTH = 8192
CHUNK = 8192
SEND_SLOTS = 2
RIDE = 17
RIDE_SLOTS = 4
WRITE_SLOTS = 5
WRITE_CHUNK = 16384


def rows(group):
    return pl.ds(pl.multiple_of(group * GROUP, GROUP), GROUP)


def lanes_of():
    return lax.broadcasted_iota(jnp.int32, (GROUP, LANES), 1)


def put_lane(tile, lane_ids, lane, partial):
    row_sum = jnp.sum(partial, axis=1, keepdims=True)
    return tile + jnp.where(lane_ids == lane, row_sum, 0.0)


def swap(values):
    parts = [values[:, at:at + LANES] for at in range(0, values.shape[1], LANES)]
    return jnp.concatenate([parts[index ^ 1] for index in range(len(parts))], axis=1)


def tree_sum(values):
    while len(values) > 1:
        values = [a + b for a, b in zip(values[::2], values[1::2])] + ([values[-1]] if len(values) % 2 else [])
    return values[0]


def peers(model_size, data_size):
    model, data = lax.axis_index('model'), lax.axis_index('data')
    out = []
    for step in range(1, model_size * data_size):
        peer_model = lax.rem(model + step // data_size, model_size)
        peer_data = lax.rem(data + step % data_size, data_size)
        out.append(((peer_model, peer_data), peer_model * data_size + peer_data))
    return model * data_size + data, out


def enter(others):
    barrier = pltpu.get_barrier_semaphore()
    for device, _ in others:
        pl.semaphore_signal(barrier, inc=1, device_id=device, device_id_type=MESH)
    pl.semaphore_wait(barrier, len(others))


def share(me, others, source, slots, send_sem, recv_sem):
    copies = []
    for device, index in others:
        copy = pltpu.make_async_remote_copy(src_ref=source, dst_ref=slots.at[me], send_sem=send_sem.at[index], recv_sem=recv_sem.at[me], device_id=device, device_id_type=MESH)
        copy.start()
        copies.append(copy)
    for device, index in others:
        pltpu.make_async_remote_copy(src_ref=source, dst_ref=slots.at[index], send_sem=send_sem.at[index], recv_sem=recv_sem.at[index], device_id=device, device_id_type=MESH).wait_recv()
    for copy in copies:
        copy.wait_send()


def exchange_kernel(sizes, groups, cols, grads, master, one_in, two_in, mean_ref, weight_ref, ring, land, clip_ref, stat_ref, stage, own, part, slots,
                    stage_sem, send_sem, recv_sem, free_sem, own_sem, weight_sem, ring_sem, small_send, small_recv):
    model_size, data_size = sizes
    data = lax.axis_index('data')
    me, others = peers(model_size, data_size)
    peer = lax.rem(data + 1, data_size)
    peer_device = (lax.axis_index('model'), peer)
    per_group = cols // PART
    parts = groups * per_group

    def columns(index, base):
        return pl.ds(pl.multiple_of(base + lax.rem(index, per_group) * PART, PART), PART)

    def own_copy(index):
        slot = lax.rem(index, OWN_SLOTS)
        return pltpu.make_async_copy(grads.at[0, rows(index // per_group), columns(index, data * cols)], own.at[slot], own_sem.at[slot])

    def weight_copy(index):
        at = (rows(index // per_group), columns(index, 0))
        return pltpu.make_async_copy(master.at[at], weight_ref.at[at], weight_sem.at[index])

    def stage_copy(index):
        slot = lax.rem(index, STAGE_SLOTS)
        return pltpu.make_async_copy(grads.at[0, rows(index // per_group), columns(index, peer * cols)], stage.at[slot], stage_sem.at[slot])

    def send_copy(index):
        from_slot, to_slot = lax.rem(index, STAGE_SLOTS), lax.rem(index, LAND_SLOTS)
        return pltpu.make_async_remote_copy(src_ref=stage.at[from_slot], dst_ref=land.at[to_slot], send_sem=send_sem.at[from_slot], recv_sem=recv_sem.at[to_slot],
                                            device_id=peer_device, device_id_type=MESH)

    def ring_copies(chunk):
        at = (rows(chunk // (cols // CHUNK)), pl.ds(pl.multiple_of(lax.rem(chunk, cols // CHUNK) * CHUNK, CHUNK), CHUNK))
        return (pltpu.make_async_copy(one_in.at[at], ring.at[0, chunk], ring_sem.at[0, chunk]), pltpu.make_async_copy(two_in.at[at], ring.at[1, chunk], ring_sem.at[1, chunk]))

    def begin_stage(index, carry):
        stage_copy(index).start()
        return carry

    def begin_own(index, carry):
        own_copy(index).start()
        weight_copy(index).start()
        return carry

    def begin_send(index, carry):
        stage_copy(index).wait()
        send_copy(index).start()
        return carry

    lax.fori_loop(0, STAGE_SLOTS, begin_stage, 0)
    lax.fori_loop(0, OWN_SLOTS, begin_own, 0)
    enter(others)
    lax.fori_loop(0, AHEAD, begin_send, 0)
    lane_ids = lanes_of()
    width = MEAN_WIDTH
    zero = jnp.zeros((GROUP, LANES), F32)
    first_ring = parts - RING // 2

    def one_part(index, carry):
        total, stat = carry
        own_slot, land_slot = lax.rem(index, OWN_SLOTS), lax.rem(index, LAND_SLOTS)
        row_at = rows(index // per_group)
        col_at = lax.rem(index, per_group) * PART

        @pl.when(jnp.logical_and(index + AHEAD >= LAND_SLOTS, index + AHEAD < parts))
        def _():
            pl.semaphore_wait(free_sem, 1)

        @pl.when(index + AHEAD < parts)
        def _():
            begin_send(index + AHEAD, 0)

        own_copy(index).wait()
        weight_copy(index).wait()
        send_copy(index).wait_recv()

        def piece(step, sums):
            grad_sum, weight_sum = sums
            near = pl.ds(pl.multiple_of(step * width, width), width)
            far = pl.ds(pl.multiple_of(col_at + step * width, width), width)
            weight = weight_ref[row_at, far]
            mean = (own[own_slot, :, near].astype(F32) + land[land_slot, :, near].astype(F32)) * 0.5
            mean_ref[row_at, far] = swap(mean)
            cuts = range(0, width, LANES)
            grad_sum += tree_sum([mean[:, at:at + LANES] * mean[:, at:at + LANES] for at in cuts])
            weight_sum += tree_sum([weight[:, at:at + LANES] * weight[:, at:at + LANES] for at in cuts])
            return grad_sum, weight_sum

        grad_sum, weight_sum = lax.fori_loop(0, PART // width, piece, (zero, zero))

        @pl.when(index + LAND_SLOTS < parts)
        def _():
            pl.semaphore_signal(free_sem, inc=1, device_id=peer_device, device_id_type=MESH)

        @pl.when(index + OWN_SLOTS < parts)
        def _():
            begin_own(index + OWN_SLOTS, 0)

        send_copy(index).wait_send()

        @pl.when(index + STAGE_SLOTS < parts)
        def _():
            begin_stage(index + STAGE_SLOTS, 0)

        @pl.when(index >= first_ring)
        def _():
            for late in range(2):
                for copy in ring_copies((index - first_ring) * 2 + late):
                    copy.start()

        return total + grad_sum, put_lane(stat, lane_ids, index // per_group, weight_sum)

    total, stat = lax.fori_loop(0, parts, one_part, (zero, zero))
    stat_ref[...] = stat
    part[...] = total
    slots[me] = part[...]
    share(me, others, part, slots, small_send, small_recv)
    whole = tree_sum([slots[index] for index in range(model_size * data_size)])
    whole = jnp.sum(jnp.sum(whole, axis=1, keepdims=True), axis=0, keepdims=True)
    whole = jnp.broadcast_to(whole, (GROUP, LANES))
    clip_ref[...] = jnp.minimum(1.0, MAX_NORM / jnp.sqrt(whole))

    def finish(chunk, carry):
        for copy in ring_copies(chunk):
            copy.wait()
        return carry

    lax.fori_loop(0, RING, finish, 0)


def moment_kernel(groups, cols, mean_in, weight_in, ring_in, land_in, clip, weight_stat, one_in, two_in, dir_ref, weight_ref, ring, land, one_out, two_out, stat_ref,
                  one_get, two_get, one_put, two_put):
    per_group = cols // CHUNK
    chunks = groups * per_group
    width = MOMENT_WIDTH
    lane_ids = lanes_of()

    def place(chunk):
        return rows(chunk // per_group), pl.ds(pl.multiple_of(lax.rem(chunk, per_group) * CHUNK, CHUNK), CHUNK)

    def gets(chunk):
        slot = lax.rem(chunk, RING)
        at = place(chunk)
        return (pltpu.make_async_copy(one_in.at[at], ring.at[0, slot], one_get.at[slot]), pltpu.make_async_copy(two_in.at[at], ring.at[1, slot], two_get.at[slot]))

    def puts(chunk):
        slot = lax.rem(chunk, RING)
        at = place(chunk)
        return (pltpu.make_async_copy(ring.at[0, slot], one_out.at[at], one_put.at[slot]), pltpu.make_async_copy(ring.at[1, slot], two_out.at[at], two_put.at[slot]))

    def start(copies, priority=0):
        for copy in copies:
            copy.start(priority=priority)

    def wait(copies):
        for copy in copies:
            copy.wait()

    scale = jnp.concatenate([clip[...]] * (width // LANES), axis=1)
    one_scale = (1.0 - BETA_ONE) * scale
    two_scale = (1.0 - BETA_TWO) * scale * scale
    ratio = CORR_TWO ** 0.5 / CORR_ONE
    floor = EPSILON * CORR_TWO ** 0.5

    def one_chunk(chunk, stat):
        slot = lax.rem(chunk, RING)
        row_at = rows(chunk // per_group)
        col_at = lax.rem(chunk, per_group) * CHUNK

        @pl.when(chunk >= RING)
        def _():
            wait(gets(chunk))

        def piece(index, total):
            near = pl.ds(pl.multiple_of(index * width, width), width)
            far = pl.ds(pl.multiple_of(col_at + index * width, width), width)
            mean, weight = swap(dir_ref[row_at, far]), weight_ref[row_at, far]
            old_one, old_two = ring[0, slot, :, near], ring[1, slot, :, near]
            new_one = BETA_ONE * old_one + one_scale * mean
            new_two = BETA_TWO * old_two + two_scale * mean * mean
            root = new_two * lax.rsqrt(jnp.maximum(new_two, TINY))
            direction = (new_one * ratio) / (root + floor) + WEIGHT_DECAY * weight
            ring[0, slot, :, near] = new_one
            ring[1, slot, :, near] = new_two
            dir_ref[row_at, far] = swap(direction)
            return total + tree_sum([direction[:, at:at + LANES] * direction[:, at:at + LANES] for at in range(0, width, LANES)])

        total = lax.fori_loop(0, CHUNK // width, piece, jnp.zeros((GROUP, LANES), F32))
        start(puts(chunk), priority=1)
        ahead = chunk + RING - LAG

        @pl.when(jnp.logical_and(ahead >= RING, ahead < chunks))
        def _():
            wait(puts(ahead - RING))
            start(gets(ahead))

        return put_lane(stat, lane_ids, chunk // per_group, total)

    stat_ref[0] = lax.fori_loop(0, chunks, one_chunk, jnp.zeros((GROUP, LANES), F32))
    stat_ref[1] = weight_stat[...]

    def finish(chunk, carry):
        wait(puts(chunk))
        return carry

    lax.fori_loop(chunks - RING, chunks, finish, 0)


def segment_sums(values):
    lane_ids = lanes_of()
    row_ids = lax.broadcasted_iota(jnp.int32, (GROUP, LANES), 0)
    kind = lax.rem(lane_ids, 3)
    first = jnp.where(kind == 0, 3, 4)
    second = jnp.where(kind == 0, 4, jnp.where(kind == 1, 7, 8))
    segment = jnp.where(row_ids < first, 0, jnp.where(row_ids < second, 1, 2))
    out = jnp.zeros((GROUP, LANES), F32)
    for index in range(3):
        inside = segment == index
        out = jnp.where(inside, jnp.sum(jnp.where(inside, values, 0.0), axis=0, keepdims=True), out)
    return out


def weight_kernel(sizes, groups, cols, direction, weight, stats, land, rate, ride, slots, packed, spare, send_sem, recv_sem, ride_sem, small_send, small_recv):
    model_size, data_size = sizes
    data = lax.axis_index('data')
    me, others = peers(model_size, data_size)
    peer_device = (lax.axis_index('model'), lax.rem(data + 1, data_size))
    sent = groups - RIDE
    enter(others)
    slots[me] = stats[...]
    share(me, others, stats, slots, small_send, small_recv)
    lane_ids = lanes_of()
    dir_sq = segment_sums(tree_sum([slots[index, 0] for index in range(model_size * data_size)]))
    weight_sq = segment_sums(tree_sum([slots[index, 1] for index in range(model_size * data_size)]))
    rate[0] = LEARN_RATE * (jnp.sqrt(weight_sq) / jnp.sqrt(dir_sq))
    width = PACK_WIDTH

    def send_copy(group):
        slot = lax.rem(group, SEND_SLOTS)
        return pltpu.make_async_remote_copy(src_ref=packed.at[slot], dst_ref=land.at[group], send_sem=send_sem.at[slot], recv_sem=recv_sem.at[group],
                                            device_id=peer_device, device_id_type=MESH)

    def ride_copy(index):
        slot = lax.rem(index, RIDE_SLOTS)
        return pltpu.make_async_copy(spare.at[slot], ride.at[index], ride_sem.at[slot])

    def pack(group, target, slot):
        group_rate = jnp.sum(jnp.where(lane_ids == group, rate[0], 0.0), axis=1, keepdims=True)

        def piece(index, inner):
            at = pl.ds(pl.multiple_of(index * width, width), width)
            target[slot, :, at] = (weight[rows(group), at] - group_rate * swap(direction[rows(group), at])).astype(BF16)
            return inner

        lax.fori_loop(0, cols // width, piece, 0)

    def one_group(group, carry):
        slot = lax.rem(group, SEND_SLOTS)

        @pl.when(group >= SEND_SLOTS)
        def _():
            send_copy(group - SEND_SLOTS).wait_send()

        pack(group, packed, slot)
        send_copy(group).start()

        def one_ride(index, inner):
            @pl.when(index >= RIDE_SLOTS)
            def _():
                ride_copy(index - RIDE_SLOTS).wait()

            pack(sent + index, spare, lax.rem(index, RIDE_SLOTS))
            ride_copy(index).start()
            return inner

        lax.fori_loop(group * RIDE // sent, (group + 1) * RIDE // sent, one_ride, 0)
        return carry

    lax.fori_loop(0, sent, one_group, 0)

    def finish(group, carry):
        send_copy(group).wait_recv()
        return carry

    lax.fori_loop(0, sent, finish, 0)
    for group in range(sent - SEND_SLOTS, sent):
        send_copy(group).wait_send()
    for index in range(RIDE - RIDE_SLOTS, RIDE):
        ride_copy(index).wait()


def write_kernel(sizes, groups, cols, direction, weight, land, rate, params, master, fresh, packed, master_sem, land_sem, own_sem):
    data_size = sizes[1]
    data = lax.axis_index('data')
    peer = lax.rem(data + 1, data_size)
    width = 4096
    lane_ids = lanes_of()
    per_group = cols // WRITE_CHUNK
    chunks = groups * per_group

    def columns(chunk, base):
        return pl.ds(pl.multiple_of(base + lax.rem(chunk, per_group) * WRITE_CHUNK, WRITE_CHUNK), WRITE_CHUNK)

    def puts(chunk):
        slot = lax.rem(chunk, WRITE_SLOTS)
        at = rows(chunk // per_group)
        return (pltpu.make_async_copy(fresh.at[slot], master.at[at, columns(chunk, 0)], master_sem.at[slot]),
                pltpu.make_async_copy(packed.at[slot], params.at[at, columns(chunk, data * cols)], own_sem.at[slot]))

    def land_copy(group):
        return pltpu.make_async_copy(land.at[group], params.at[rows(group), pl.ds(pl.multiple_of(peer * cols, LANES), cols)], land_sem.at[group])

    def one_chunk(chunk, carry):
        slot = lax.rem(chunk, WRITE_SLOTS)
        group = chunk // per_group

        @pl.when(jnp.logical_and(lax.rem(chunk, per_group) == 0, group < groups - RIDE))
        def _():
            land_copy(group).start()

        @pl.when(chunk >= WRITE_SLOTS)
        def _():
            for copy in puts(chunk - WRITE_SLOTS):
                copy.wait()

        group_rate = jnp.sum(jnp.where(lane_ids == group, rate[0], 0.0), axis=1, keepdims=True)

        def piece(index, inner):
            near = pl.ds(pl.multiple_of(index * width, width), width)
            far = pl.ds(pl.multiple_of(lax.rem(chunk, per_group) * WRITE_CHUNK + index * width, width), width)
            new = weight[rows(group), far] - group_rate * swap(direction[rows(group), far])
            fresh[slot, :, near] = new
            packed[slot, :, near] = new.astype(BF16)
            return inner

        lax.fori_loop(0, WRITE_CHUNK // width, piece, 0)
        for priority, copy in enumerate(puts(chunk)):
            copy.start(priority=priority)
        return carry

    lax.fori_loop(0, chunks, one_chunk, 0)

    def finish(group, carry):
        land_copy(group).wait()
        return carry

    lax.fori_loop(0, groups - RIDE, finish, 0)
    for chunk in range(chunks - WRITE_SLOTS, chunks):
        for copy in puts(chunk):
            copy.wait()


def place_kernel(sizes, groups, cols, given, params_in, params, put_sem):
    data_size = sizes[1]
    peer = lax.rem(lax.axis_index('data') + 1, data_size)

    def put(index):
        return pltpu.make_async_copy(given.at[index], params.at[rows(groups - RIDE + index), pl.ds(pl.multiple_of(peer * cols, LANES), cols)], put_sem.at[index])

    def begin(index, carry):
        put(index).start()
        return carry

    def finish(index, carry):
        put(index).wait()
        return carry

    lax.fori_loop(0, RIDE, begin, 0)
    lax.fori_loop(0, RIDE, finish, 0)


def solution(mesh):
    sizes = (mesh.shape['model'], mesh.shape['data'])
    devices = sizes[0] * sizes[1]
    both_axes = ('model', 'data')
    state_spec = P(None, both_axes)
    hbm = pl.BlockSpec(memory_space=pl.ANY)
    vmem = pl.BlockSpec(memory_space=pltpu.VMEM)
    dma = pltpu.SemaphoreType.DMA

    def device_step(local_grads, master, moment_one, moment_two):
        blocks, cols = master.shape
        groups = blocks // GROUP
        kept = pltpu.VMEM((blocks, cols), F32)
        keep = functools.partial(pltpu.with_memory_space_constraint, memory_space=pltpu.VMEM)
        tile = pltpu.VMEM((GROUP, LANES), F32)
        state = jax.ShapeDtypeStruct((blocks, cols), F32)

        landed = pltpu.VMEM((groups - RIDE, GROUP, cols), BF16)
        riding = jax.ShapeDtypeStruct((RIDE, GROUP, cols), BF16)
        ring_shape = pltpu.VMEM((2, RING, GROUP, CHUNK), F32)
        landed = pltpu.VMEM((groups - RIDE, GROUP, cols), BF16)
        riding = jax.ShapeDtypeStruct((RIDE, GROUP, cols), BF16)
        parts = groups * (cols // PART)

        caught = pltpu.VMEM((LAND_SLOTS, GROUP, PART), BF16)

        mean, weight, ring, catch, clip, weight_stat = pl.pallas_call(
            functools.partial(exchange_kernel, sizes, groups, cols),
            out_shape=(kept, kept, ring_shape, caught, tile, tile),
            in_specs=[hbm] * 4,
            out_specs=[vmem] * 6,
            scratch_shapes=[pltpu.VMEM((STAGE_SLOTS, GROUP, PART), BF16), pltpu.VMEM((OWN_SLOTS, GROUP, PART), BF16), pltpu.VMEM((GROUP, LANES), F32), pltpu.VMEM((devices, GROUP, LANES), F32),
                            dma((STAGE_SLOTS,)), dma((STAGE_SLOTS,)), dma((LAND_SLOTS,)), pltpu.SemaphoreType.REGULAR, dma((OWN_SLOTS,)), dma((parts,)), dma((2, RING)), dma((devices,)), dma((devices,))],
            compiler_params=pltpu.CompilerParams(collective_id=0, has_side_effects=True, vmem_limit_bytes=SCOPE),
            name='exchange',
        )(local_grads, master, moment_one, moment_two)

        direction, weight, _, _, new_one, new_two, stats = pl.pallas_call(
            functools.partial(moment_kernel, groups, cols),
            out_shape=(kept, kept, ring_shape, caught, state, state, pltpu.VMEM((2, GROUP, LANES), F32)),
            in_specs=[vmem] * 6 + [hbm] * 2,
            out_specs=[vmem, vmem, vmem, vmem, hbm, hbm, vmem],
            input_output_aliases={0: 0, 1: 1, 2: 2, 3: 3},
            scratch_shapes=[dma((RING,))] * 4,
            compiler_params=pltpu.CompilerParams(vmem_limit_bytes=SCOPE),
            name='moments',
        )(mean, weight, ring, catch, keep(clip), keep(weight_stat), moment_one, moment_two)

        land, rate, ride = pl.pallas_call(
            functools.partial(weight_kernel, sizes, groups, cols),
            out_shape=(landed, pltpu.VMEM((2, GROUP, LANES), F32), riding),
            in_specs=[vmem] * 3,
            out_specs=[vmem, vmem, hbm],
            input_output_aliases={2: 1},
            scratch_shapes=[pltpu.VMEM((devices, 2, GROUP, LANES), F32), pltpu.VMEM((SEND_SLOTS, GROUP, cols), BF16), pltpu.VMEM((RIDE_SLOTS, GROUP, cols), BF16),
                            dma((SEND_SLOTS,)), dma((groups - RIDE,)), dma((RIDE_SLOTS,)), dma((devices,)), dma((devices,))],
            compiler_params=pltpu.CompilerParams(collective_id=1, has_side_effects=True, vmem_limit_bytes=SCOPE),
            name='weights',
        )(keep(direction), keep(weight), keep(stats))

        given = lax.ppermute(ride, 'data', [(rank, (rank + 1) % sizes[1]) for rank in range(sizes[1])])

        params, new_master = pl.pallas_call(
            functools.partial(write_kernel, sizes, groups, cols),
            out_shape=(jax.ShapeDtypeStruct((blocks, sizes[1] * cols), BF16), state),
            in_specs=[vmem] * 4,
            out_specs=[hbm, hbm],
            scratch_shapes=[pltpu.VMEM((WRITE_SLOTS, GROUP, WRITE_CHUNK), F32), pltpu.VMEM((WRITE_SLOTS, GROUP, WRITE_CHUNK), BF16),
                            dma((WRITE_SLOTS,)), dma((groups,)), dma((WRITE_SLOTS,))],
            compiler_params=pltpu.CompilerParams(vmem_limit_bytes=SCOPE),
            name='write',
        )(keep(direction), keep(weight), keep(land), keep(rate))
        params = pl.pallas_call(
            functools.partial(place_kernel, sizes, groups, cols),
            out_shape=jax.ShapeDtypeStruct((blocks, sizes[1] * cols), BF16),
            in_specs=[vmem, hbm],
            out_specs=hbm,
            input_output_aliases={1: 0},
            scratch_shapes=[dma((RIDE,))],
            compiler_params=pltpu.CompilerParams(vmem_limit_bytes=SCOPE),
            name='place',
        )(keep(given), params)
        return params, new_master, new_one, new_two

    return jax.shard_map(device_step, mesh=mesh, in_specs=(P('data', None, 'model'), state_spec, state_spec, state_spec),
                         out_specs=(P(None, 'model'), state_spec, state_spec, state_spec), check_vma=False)
```

```python
import functools

import jax
import jax.numpy as jnp
from jax import lax
from jax.experimental import pallas as pl
from jax.experimental.pallas import tpu as pltpu
from jax.sharding import PartitionSpec as P

STEP = 4
LEARN_RATE = 0.08
BETA_ONE = 0.9
BETA_TWO = 0.999
EPSILON = 1e-6
WEIGHT_DECAY = 0.01
MAX_NORM = 1.0
CORR_ONE = 1.0 - BETA_ONE ** STEP
CORR_TWO = 1.0 - BETA_TWO ** STEP
TINY = 1.2e-38

MESH = pl.DeviceIdType.MESH
F32 = jnp.float32
BF16 = jnp.bfloat16
SCOPE = 4000 << 10
LANES = 128
GROUP = 8

PART = 16384
AHEAD = 4
LAND_SLOTS = 8
STAGE_SLOTS = 9
OWN_SLOTS = 6
RING = 20
LAG = 4
MOMENT_WIDTH = 8192
MEAN_WIDTH = 2048
PACK_WIDTH = 8192
CHUNK = 8192
SEND_SLOTS = 3
RIDE = 17
RIDE_SLOTS = 4
WRITE_SLOTS = 5
WRITE_CHUNK = 16384


def rows(group):
    return pl.ds(pl.multiple_of(group * GROUP, GROUP), GROUP)


def lanes_of():
    return lax.broadcasted_iota(jnp.int32, (GROUP, LANES), 1)


def put_lane(tile, lane_ids, lane, partial):
    row_sum = jnp.sum(partial, axis=1, keepdims=True)
    return tile + jnp.where(lane_ids == lane, row_sum, 0.0)


def swap(values):
    parts = [values[:, at:at + LANES] for at in range(0, values.shape[1], LANES)]
    return jnp.concatenate([parts[index ^ 1] for index in range(len(parts))], axis=1)


def tree_sum(values):
    while len(values) > 1:
        values = [a + b for a, b in zip(values[::2], values[1::2])] + ([values[-1]] if len(values) % 2 else [])
    return values[0]


def peers(model_size, data_size):
    model, data = lax.axis_index('model'), lax.axis_index('data')
    out = []
    for step in range(1, model_size * data_size):
        peer_model = lax.rem(model + step // data_size, model_size)
        peer_data = lax.rem(data + step % data_size, data_size)
        out.append(((peer_model, peer_data), peer_model * data_size + peer_data))
    return model * data_size + data, out


def enter(others):
    barrier = pltpu.get_barrier_semaphore()
    for device, _ in others:
        pl.semaphore_signal(barrier, inc=1, device_id=device, device_id_type=MESH)
    pl.semaphore_wait(barrier, len(others))


def share(me, others, source, slots, send_sem, recv_sem):
    copies = []
    for device, index in others:
        copy = pltpu.make_async_remote_copy(src_ref=source, dst_ref=slots.at[me], send_sem=send_sem.at[index], recv_sem=recv_sem.at[me], device_id=device, device_id_type=MESH)
        copy.start()
        copies.append(copy)
    for device, index in others:
        pltpu.make_async_remote_copy(src_ref=source, dst_ref=slots.at[index], send_sem=send_sem.at[index], recv_sem=recv_sem.at[index], device_id=device, device_id_type=MESH).wait_recv()
    for copy in copies:
        copy.wait_send()


def exchange_kernel(sizes, groups, cols, grads, master, one_in, two_in, mean_ref, weight_ref, ring, land, clip_ref, stat_ref, stage, own, part, slots,
                    stage_sem, send_sem, recv_sem, free_sem, own_sem, weight_sem, ring_sem, small_send, small_recv):
    model_size, data_size = sizes
    data = lax.axis_index('data')
    me, others = peers(model_size, data_size)
    peer = lax.rem(data + 1, data_size)
    peer_device = (lax.axis_index('model'), peer)
    per_group = cols // PART
    parts = groups * per_group

    def columns(index, base):
        return pl.ds(pl.multiple_of(base + lax.rem(index, per_group) * PART, PART), PART)

    def own_copy(index):
        slot = lax.rem(index, OWN_SLOTS)
        return pltpu.make_async_copy(grads.at[0, rows(index // per_group), columns(index, data * cols)], own.at[slot], own_sem.at[slot])

    def weight_copy(index):
        at = (rows(index // per_group), columns(index, 0))
        return pltpu.make_async_copy(master.at[at], weight_ref.at[at], weight_sem.at[index])

    def stage_copy(index):
        slot = lax.rem(index, STAGE_SLOTS)
        return pltpu.make_async_copy(grads.at[0, rows(index // per_group), columns(index, peer * cols)], stage.at[slot], stage_sem.at[slot])

    def send_copy(index):
        from_slot, to_slot = lax.rem(index, STAGE_SLOTS), lax.rem(index, LAND_SLOTS)
        return pltpu.make_async_remote_copy(src_ref=stage.at[from_slot], dst_ref=land.at[to_slot], send_sem=send_sem.at[from_slot], recv_sem=recv_sem.at[to_slot],
                                            device_id=peer_device, device_id_type=MESH)

    def ring_copies(chunk):
        at = (rows(chunk // (cols // CHUNK)), pl.ds(pl.multiple_of(lax.rem(chunk, cols // CHUNK) * CHUNK, CHUNK), CHUNK))
        return (pltpu.make_async_copy(one_in.at[at], ring.at[0, chunk], ring_sem.at[0, chunk]), pltpu.make_async_copy(two_in.at[at], ring.at[1, chunk], ring_sem.at[1, chunk]))

    def begin_stage(index, carry):
        stage_copy(index).start()
        return carry

    def begin_own(index, carry):
        own_copy(index).start()
        weight_copy(index).start()
        return carry

    def begin_send(index, carry):
        stage_copy(index).wait()
        send_copy(index).start()
        return carry

    lax.fori_loop(0, STAGE_SLOTS, begin_stage, 0)
    lax.fori_loop(0, OWN_SLOTS, begin_own, 0)
    enter(others)
    lax.fori_loop(0, AHEAD, begin_send, 0)
    lane_ids = lanes_of()
    width = MEAN_WIDTH
    zero = jnp.zeros((GROUP, LANES), F32)
    first_ring = parts - RING // 2

    def one_part(index, carry):
        total, stat = carry
        own_slot, land_slot = lax.rem(index, OWN_SLOTS), lax.rem(index, LAND_SLOTS)
        row_at = rows(index // per_group)
        col_at = lax.rem(index, per_group) * PART

        @pl.when(jnp.logical_and(index + AHEAD >= LAND_SLOTS, index + AHEAD < parts))
        def _():
            pl.semaphore_wait(free_sem, 1)

        @pl.when(index + AHEAD < parts)
        def _():
            begin_send(index + AHEAD, 0)

        own_copy(index).wait()
        weight_copy(index).wait()
        send_copy(index).wait_recv()

        def piece(step, sums):
            grad_sum, weight_sum = sums
            near = pl.ds(pl.multiple_of(step * width, width), width)
            far = pl.ds(pl.multiple_of(col_at + step * width, width), width)
            weight = weight_ref[row_at, far]
            mean = (own[own_slot, :, near].astype(F32) + land[land_slot, :, near].astype(F32)) * 0.5
            mean_ref[row_at, far] = swap(mean)
            cuts = range(0, width, LANES)
            grad_sum += tree_sum([mean[:, at:at + LANES] * mean[:, at:at + LANES] for at in cuts])
            weight_sum += tree_sum([weight[:, at:at + LANES] * weight[:, at:at + LANES] for at in cuts])
            return grad_sum, weight_sum

        grad_sum, weight_sum = lax.fori_loop(0, PART // width, piece, (zero, zero))

        @pl.when(index + LAND_SLOTS < parts)
        def _():
            pl.semaphore_signal(free_sem, inc=1, device_id=peer_device, device_id_type=MESH)

        @pl.when(index + OWN_SLOTS < parts)
        def _():
            begin_own(index + OWN_SLOTS, 0)

        send_copy(index).wait_send()

        @pl.when(index + STAGE_SLOTS < parts)
        def _():
            begin_stage(index + STAGE_SLOTS, 0)

        @pl.when(index >= first_ring)
        def _():
            for late in range(2):
                for copy in ring_copies((index - first_ring) * 2 + late):
                    copy.start()

        return total + grad_sum, put_lane(stat, lane_ids, index // per_group, weight_sum)

    total, stat = lax.fori_loop(0, parts, one_part, (zero, zero))
    stat_ref[...] = stat
    part[...] = total
    slots[me] = part[...]
    share(me, others, part, slots, small_send, small_recv)
    whole = tree_sum([slots[index] for index in range(model_size * data_size)])
    whole = jnp.sum(jnp.sum(whole, axis=1, keepdims=True), axis=0, keepdims=True)
    whole = jnp.broadcast_to(whole, (GROUP, LANES))
    clip_ref[...] = jnp.minimum(1.0, MAX_NORM / jnp.sqrt(whole))

    def finish(chunk, carry):
        for copy in ring_copies(chunk):
            copy.wait()
        return carry

    lax.fori_loop(0, RING, finish, 0)


def moment_kernel(groups, cols, mean_in, weight_in, ring_in, land_in, clip, weight_stat, one_in, two_in, dir_ref, weight_ref, ring, land, one_out, two_out, stat_ref,
                  one_get, two_get, one_put, two_put):
    per_group = cols // CHUNK
    chunks = groups * per_group
    width = MOMENT_WIDTH
    lane_ids = lanes_of()

    def place(chunk):
        return rows(chunk // per_group), pl.ds(pl.multiple_of(lax.rem(chunk, per_group) * CHUNK, CHUNK), CHUNK)

    def gets(chunk):
        slot = lax.rem(chunk, RING)
        at = place(chunk)
        return (pltpu.make_async_copy(one_in.at[at], ring.at[0, slot], one_get.at[slot]), pltpu.make_async_copy(two_in.at[at], ring.at[1, slot], two_get.at[slot]))

    def puts(chunk):
        slot = lax.rem(chunk, RING)
        at = place(chunk)
        return (pltpu.make_async_copy(ring.at[0, slot], one_out.at[at], one_put.at[slot]), pltpu.make_async_copy(ring.at[1, slot], two_out.at[at], two_put.at[slot]))

    def start(copies, priority=0):
        for copy in copies:
            copy.start(priority=priority)

    def wait(copies):
        for copy in copies:
            copy.wait()

    scale = jnp.concatenate([clip[...]] * (width // LANES), axis=1)
    one_scale = (1.0 - BETA_ONE) * scale
    two_scale = (1.0 - BETA_TWO) * scale * scale
    ratio = CORR_TWO ** 0.5 / CORR_ONE
    floor = EPSILON * CORR_TWO ** 0.5

    def one_chunk(chunk, stat):
        slot = lax.rem(chunk, RING)
        row_at = rows(chunk // per_group)
        col_at = lax.rem(chunk, per_group) * CHUNK

        @pl.when(chunk >= RING)
        def _():
            wait(gets(chunk))

        def piece(index, total):
            near = pl.ds(pl.multiple_of(index * width, width), width)
            far = pl.ds(pl.multiple_of(col_at + index * width, width), width)
            mean, weight = swap(dir_ref[row_at, far]), weight_ref[row_at, far]
            old_one, old_two = ring[0, slot, :, near], ring[1, slot, :, near]
            new_one = BETA_ONE * old_one + one_scale * mean
            new_two = BETA_TWO * old_two + two_scale * mean * mean
            root = new_two * lax.rsqrt(jnp.maximum(new_two, TINY))
            direction = (new_one * ratio) / (root + floor) + WEIGHT_DECAY * weight
            ring[0, slot, :, near] = new_one
            ring[1, slot, :, near] = new_two
            dir_ref[row_at, far] = swap(direction)
            return total + tree_sum([direction[:, at:at + LANES] * direction[:, at:at + LANES] for at in range(0, width, LANES)])

        total = lax.fori_loop(0, CHUNK // width, piece, jnp.zeros((GROUP, LANES), F32))
        start(puts(chunk), priority=1)
        ahead = chunk + RING - LAG

        @pl.when(jnp.logical_and(ahead >= RING, ahead < chunks))
        def _():
            wait(puts(ahead - RING))
            start(gets(ahead))

        return put_lane(stat, lane_ids, chunk // per_group, total)

    stat_ref[0] = lax.fori_loop(0, chunks, one_chunk, jnp.zeros((GROUP, LANES), F32))
    stat_ref[1] = weight_stat[...]

    def finish(chunk, carry):
        wait(puts(chunk))
        return carry

    lax.fori_loop(chunks - RING, chunks, finish, 0)


def segment_sums(values):
    lane_ids = lanes_of()
    row_ids = lax.broadcasted_iota(jnp.int32, (GROUP, LANES), 0)
    kind = lax.rem(lane_ids, 3)
    first = jnp.where(kind == 0, 3, 4)
    second = jnp.where(kind == 0, 4, jnp.where(kind == 1, 7, 8))
    segment = jnp.where(row_ids < first, 0, jnp.where(row_ids < second, 1, 2))
    out = jnp.zeros((GROUP, LANES), F32)
    for index in range(3):
        inside = segment == index
        out = jnp.where(inside, jnp.sum(jnp.where(inside, values, 0.0), axis=0, keepdims=True), out)
    return out


def weight_kernel(sizes, groups, cols, direction, weight, stats, land, rate, ride, slots, packed, spare, send_sem, recv_sem, ride_sem, small_send, small_recv):
    model_size, data_size = sizes
    data = lax.axis_index('data')
    me, others = peers(model_size, data_size)
    peer_device = (lax.axis_index('model'), lax.rem(data + 1, data_size))
    sent = groups - RIDE
    enter(others)
    slots[me] = stats[...]
    share(me, others, stats, slots, small_send, small_recv)
    lane_ids = lanes_of()
    dir_sq = segment_sums(tree_sum([slots[index, 0] for index in range(model_size * data_size)]))
    weight_sq = segment_sums(tree_sum([slots[index, 1] for index in range(model_size * data_size)]))
    rate[0] = LEARN_RATE * (jnp.sqrt(weight_sq) / jnp.sqrt(dir_sq))
    width = PACK_WIDTH

    def send_copy(group):
        slot = lax.rem(group, SEND_SLOTS)
        return pltpu.make_async_remote_copy(src_ref=packed.at[slot], dst_ref=land.at[group], send_sem=send_sem.at[slot], recv_sem=recv_sem.at[group],
                                            device_id=peer_device, device_id_type=MESH)

    def ride_copy(index):
        slot = lax.rem(index, RIDE_SLOTS)
        return pltpu.make_async_copy(spare.at[slot], ride.at[index], ride_sem.at[slot])

    def pack(group, target, slot):
        group_rate = jnp.sum(jnp.where(lane_ids == group, rate[0], 0.0), axis=1, keepdims=True)

        def piece(index, inner):
            at = pl.ds(pl.multiple_of(index * width, width), width)
            target[slot, :, at] = (weight[rows(group), at] - group_rate * swap(direction[rows(group), at])).astype(BF16)
            return inner

        lax.fori_loop(0, cols // width, piece, 0)

    def one_group(group, carry):
        slot = lax.rem(group, SEND_SLOTS)

        @pl.when(group >= SEND_SLOTS)
        def _():
            send_copy(group - SEND_SLOTS).wait_send()

        pack(group, packed, slot)
        send_copy(group).start()

        def one_ride(index, inner):
            @pl.when(index >= RIDE_SLOTS)
            def _():
                ride_copy(index - RIDE_SLOTS).wait()

            pack(sent + index, spare, lax.rem(index, RIDE_SLOTS))
            ride_copy(index).start()
            return inner

        lax.fori_loop(group * RIDE // sent, (group + 1) * RIDE // sent, one_ride, 0)
        return carry

    lax.fori_loop(0, sent, one_group, 0)

    def finish(group, carry):
        send_copy(group).wait_recv()
        return carry

    lax.fori_loop(0, sent, finish, 0)
    for group in range(sent - SEND_SLOTS, sent):
        send_copy(group).wait_send()
    for index in range(RIDE - RIDE_SLOTS, RIDE):
        ride_copy(index).wait()


def write_kernel(sizes, groups, cols, direction, weight, land, rate, params, master, fresh, packed, master_sem, land_sem, own_sem):
    data_size = sizes[1]
    data = lax.axis_index('data')
    peer = lax.rem(data + 1, data_size)
    width = 4096
    lane_ids = lanes_of()
    per_group = cols // WRITE_CHUNK
    chunks = groups * per_group

    def columns(chunk, base):
        return pl.ds(pl.multiple_of(base + lax.rem(chunk, per_group) * WRITE_CHUNK, WRITE_CHUNK), WRITE_CHUNK)

    def puts(chunk):
        slot = lax.rem(chunk, WRITE_SLOTS)
        at = rows(chunk // per_group)
        return (pltpu.make_async_copy(fresh.at[slot], master.at[at, columns(chunk, 0)], master_sem.at[slot]),
                pltpu.make_async_copy(packed.at[slot], params.at[at, columns(chunk, data * cols)], own_sem.at[slot]))

    def land_copy(group):
        return pltpu.make_async_copy(land.at[group], params.at[rows(group), pl.ds(pl.multiple_of(peer * cols, LANES), cols)], land_sem.at[group])

    def one_chunk(chunk, carry):
        slot = lax.rem(chunk, WRITE_SLOTS)
        group = chunk // per_group

        @pl.when(jnp.logical_and(lax.rem(chunk, per_group) == 0, group < groups - RIDE))
        def _():
            land_copy(group).start()

        @pl.when(chunk >= WRITE_SLOTS)
        def _():
            for copy in puts(chunk - WRITE_SLOTS):
                copy.wait()

        group_rate = jnp.sum(jnp.where(lane_ids == group, rate[0], 0.0), axis=1, keepdims=True)

        def piece(index, inner):
            near = pl.ds(pl.multiple_of(index * width, width), width)
            far = pl.ds(pl.multiple_of(lax.rem(chunk, per_group) * WRITE_CHUNK + index * width, width), width)
            new = weight[rows(group), far] - group_rate * swap(direction[rows(group), far])
            fresh[slot, :, near] = new
            packed[slot, :, near] = new.astype(BF16)
            return inner

        lax.fori_loop(0, WRITE_CHUNK // width, piece, 0)
        for priority, copy in enumerate(puts(chunk)):
            copy.start(priority=priority)
        return carry

    lax.fori_loop(0, chunks, one_chunk, 0)

    def finish(group, carry):
        land_copy(group).wait()
        return carry

    lax.fori_loop(0, groups - RIDE, finish, 0)
    for chunk in range(chunks - WRITE_SLOTS, chunks):
        for copy in puts(chunk):
            copy.wait()


def place_kernel(sizes, groups, cols, given, params_in, params, put_sem):
    data_size = sizes[1]
    peer = lax.rem(lax.axis_index('data') + 1, data_size)

    def put(index):
        return pltpu.make_async_copy(given.at[index], params.at[rows(groups - RIDE + index), pl.ds(pl.multiple_of(peer * cols, LANES), cols)], put_sem.at[index])

    def begin(index, carry):
        put(index).start()
        return carry

    def finish(index, carry):
        put(index).wait()
        return carry

    lax.fori_loop(0, RIDE, begin, 0)
    lax.fori_loop(0, RIDE, finish, 0)


def solution(mesh):
    sizes = (mesh.shape['model'], mesh.shape['data'])
    devices = sizes[0] * sizes[1]
    both_axes = ('model', 'data')
    state_spec = P(None, both_axes)
    hbm = pl.BlockSpec(memory_space=pl.ANY)
    vmem = pl.BlockSpec(memory_space=pltpu.VMEM)
    dma = pltpu.SemaphoreType.DMA

    def device_step(local_grads, master, moment_one, moment_two):
        blocks, cols = master.shape
        groups = blocks // GROUP
        kept = pltpu.VMEM((blocks, cols), F32)
        keep = functools.partial(pltpu.with_memory_space_constraint, memory_space=pltpu.VMEM)
        tile = pltpu.VMEM((GROUP, LANES), F32)
        state = jax.ShapeDtypeStruct((blocks, cols), F32)

        landed = pltpu.VMEM((groups - RIDE, GROUP, cols), BF16)
        riding = jax.ShapeDtypeStruct((RIDE, GROUP, cols), BF16)
        ring_shape = pltpu.VMEM((2, RING, GROUP, CHUNK), F32)
        landed = pltpu.VMEM((groups - RIDE, GROUP, cols), BF16)
        riding = jax.ShapeDtypeStruct((RIDE, GROUP, cols), BF16)
        parts = groups * (cols // PART)

        caught = pltpu.VMEM((LAND_SLOTS, GROUP, PART), BF16)

        mean, weight, ring, catch, clip, weight_stat = pl.pallas_call(
            functools.partial(exchange_kernel, sizes, groups, cols),
            out_shape=(kept, kept, ring_shape, caught, tile, tile),
            in_specs=[hbm] * 4,
            out_specs=[vmem] * 6,
            scratch_shapes=[pltpu.VMEM((STAGE_SLOTS, GROUP, PART), BF16), pltpu.VMEM((OWN_SLOTS, GROUP, PART), BF16), pltpu.VMEM((GROUP, LANES), F32), pltpu.VMEM((devices, GROUP, LANES), F32),
                            dma((STAGE_SLOTS,)), dma((STAGE_SLOTS,)), dma((LAND_SLOTS,)), pltpu.SemaphoreType.REGULAR, dma((OWN_SLOTS,)), dma((parts,)), dma((2, RING)), dma((devices,)), dma((devices,))],
            compiler_params=pltpu.CompilerParams(collective_id=0, has_side_effects=True, vmem_limit_bytes=SCOPE),
            name='exchange',
        )(local_grads, master, moment_one, moment_two)

        direction, weight, _, _, new_one, new_two, stats = pl.pallas_call(
            functools.partial(moment_kernel, groups, cols),
            out_shape=(kept, kept, ring_shape, caught, state, state, pltpu.VMEM((2, GROUP, LANES), F32)),
            in_specs=[vmem] * 6 + [hbm] * 2,
            out_specs=[vmem, vmem, vmem, vmem, hbm, hbm, vmem],
            input_output_aliases={0: 0, 1: 1, 2: 2, 3: 3},
            scratch_shapes=[dma((RING,))] * 4,
            compiler_params=pltpu.CompilerParams(vmem_limit_bytes=SCOPE),
            name='moments',
        )(mean, weight, ring, catch, keep(clip), keep(weight_stat), moment_one, moment_two)

        land, rate, ride = pl.pallas_call(
            functools.partial(weight_kernel, sizes, groups, cols),
            out_shape=(landed, pltpu.VMEM((2, GROUP, LANES), F32), riding),
            in_specs=[vmem] * 3,
            out_specs=[vmem, vmem, hbm],
            input_output_aliases={2: 1},
            scratch_shapes=[pltpu.VMEM((devices, 2, GROUP, LANES), F32), pltpu.VMEM((SEND_SLOTS, GROUP, cols), BF16), pltpu.VMEM((RIDE_SLOTS, GROUP, cols), BF16),
                            dma((SEND_SLOTS,)), dma((groups - RIDE,)), dma((RIDE_SLOTS,)), dma((devices,)), dma((devices,))],
            compiler_params=pltpu.CompilerParams(collective_id=1, has_side_effects=True, vmem_limit_bytes=SCOPE),
            name='weights',
        )(keep(direction), keep(weight), keep(stats))

        given = lax.ppermute(ride, 'data', [(rank, (rank + 1) % sizes[1]) for rank in range(sizes[1])])

        params, new_master = pl.pallas_call(
            functools.partial(write_kernel, sizes, groups, cols),
            out_shape=(jax.ShapeDtypeStruct((blocks, sizes[1] * cols), BF16), state),
            in_specs=[vmem] * 4,
            out_specs=[hbm, hbm],
            scratch_shapes=[pltpu.VMEM((WRITE_SLOTS, GROUP, WRITE_CHUNK), F32), pltpu.VMEM((WRITE_SLOTS, GROUP, WRITE_CHUNK), BF16),
                            dma((WRITE_SLOTS,)), dma((groups,)), dma((WRITE_SLOTS,))],
            compiler_params=pltpu.CompilerParams(vmem_limit_bytes=SCOPE),
            name='write',
        )(keep(direction), keep(weight), keep(land), keep(rate))
        params = pl.pallas_call(
            functools.partial(place_kernel, sizes, groups, cols),
            out_shape=jax.ShapeDtypeStruct((blocks, sizes[1] * cols), BF16),
            in_specs=[vmem, hbm],
            out_specs=hbm,
            input_output_aliases={1: 0},
            scratch_shapes=[dma((RIDE,))],
            compiler_params=pltpu.CompilerParams(vmem_limit_bytes=SCOPE),
            name='place',
        )(keep(given), params)
        return params, new_master, new_one, new_two

    return jax.shard_map(device_step, mesh=mesh, in_specs=(P('data', None, 'model'), state_spec, state_spec, state_spec),
                         out_specs=(P(None, 'model'), state_spec, state_spec, state_spec), check_vma=False)
```

```python
import functools

import jax
import jax.numpy as jnp
from jax import lax
from jax.experimental import pallas as pl
from jax.experimental.pallas import tpu as pltpu
from jax.sharding import PartitionSpec as P

STEP = 4
LEARN_RATE = 0.08
BETA_ONE = 0.9
BETA_TWO = 0.999
EPSILON = 1e-6
WEIGHT_DECAY = 0.01
MAX_NORM = 1.0
CORR_ONE = 1.0 - BETA_ONE ** STEP
CORR_TWO = 1.0 - BETA_TWO ** STEP
TINY = 1.2e-38

MESH = pl.DeviceIdType.MESH
F32 = jnp.float32
BF16 = jnp.bfloat16
SCOPE = 4000 << 10
LANES = 128
GROUP = 8

PART = 16384
AHEAD = 6
LAND_SLOTS = 8
STAGE_SLOTS = 9
OWN_SLOTS = 6
RING = 20
LAG = 4
MOMENT_WIDTH = 8192
MEAN_WIDTH = 2048
PACK_WIDTH = 8192
CHUNK = 8192
SEND_SLOTS = 3
RIDE = 17
RIDE_SLOTS = 4
WRITE_SLOTS = 5
WRITE_CHUNK = 16384


def rows(group):
    return pl.ds(pl.multiple_of(group * GROUP, GROUP), GROUP)


def lanes_of():
    return lax.broadcasted_iota(jnp.int32, (GROUP, LANES), 1)


def put_lane(tile, lane_ids, lane, partial):
    row_sum = jnp.sum(partial, axis=1, keepdims=True)
    return tile + jnp.where(lane_ids == lane, row_sum, 0.0)


def swap(values):
    parts = [values[:, at:at + LANES] for at in range(0, values.shape[1], LANES)]
    return jnp.concatenate([parts[index ^ 1] for index in range(len(parts))], axis=1)


def tree_sum(values):
    while len(values) > 1:
        values = [a + b for a, b in zip(values[::2], values[1::2])] + ([values[-1]] if len(values) % 2 else [])
    return values[0]


def peers(model_size, data_size):
    model, data = lax.axis_index('model'), lax.axis_index('data')
    out = []
    for step in range(1, model_size * data_size):
        peer_model = lax.rem(model + step // data_size, model_size)
        peer_data = lax.rem(data + step % data_size, data_size)
        out.append(((peer_model, peer_data), peer_model * data_size + peer_data))
    return model * data_size + data, out


def enter(others):
    barrier = pltpu.get_barrier_semaphore()
    for device, _ in others:
        pl.semaphore_signal(barrier, inc=1, device_id=device, device_id_type=MESH)
    pl.semaphore_wait(barrier, len(others))


def share(me, others, source, slots, send_sem, recv_sem):
    copies = []
    for device, index in others:
        copy = pltpu.make_async_remote_copy(src_ref=source, dst_ref=slots.at[me], send_sem=send_sem.at[index], recv_sem=recv_sem.at[me], device_id=device, device_id_type=MESH)
        copy.start()
        copies.append(copy)
    for device, index in others:
        pltpu.make_async_remote_copy(src_ref=source, dst_ref=slots.at[index], send_sem=send_sem.at[index], recv_sem=recv_sem.at[index], device_id=device, device_id_type=MESH).wait_recv()
    for copy in copies:
        copy.wait_send()


def exchange_kernel(sizes, groups, cols, grads, master, one_in, two_in, mean_ref, weight_ref, ring, land, clip_ref, stat_ref, stage, own, part, slots,
                    stage_sem, send_sem, recv_sem, free_sem, own_sem, weight_sem, ring_sem, small_send, small_recv):
    model_size, data_size = sizes
    data = lax.axis_index('data')
    me, others = peers(model_size, data_size)
    peer = lax.rem(data + 1, data_size)
    peer_device = (lax.axis_index('model'), peer)
    per_group = cols // PART
    parts = groups * per_group

    def columns(index, base):
        return pl.ds(pl.multiple_of(base + lax.rem(index, per_group) * PART, PART), PART)

    def own_copy(index):
        slot = lax.rem(index, OWN_SLOTS)
        return pltpu.make_async_copy(grads.at[0, rows(index // per_group), columns(index, data * cols)], own.at[slot], own_sem.at[slot])

    def weight_copy(index):
        at = (rows(index // per_group), columns(index, 0))
        return pltpu.make_async_copy(master.at[at], weight_ref.at[at], weight_sem.at[index])

    def stage_copy(index):
        slot = lax.rem(index, STAGE_SLOTS)
        return pltpu.make_async_copy(grads.at[0, rows(index // per_group), columns(index, peer * cols)], stage.at[slot], stage_sem.at[slot])

    def send_copy(index):
        from_slot, to_slot = lax.rem(index, STAGE_SLOTS), lax.rem(index, LAND_SLOTS)
        return pltpu.make_async_remote_copy(src_ref=stage.at[from_slot], dst_ref=land.at[to_slot], send_sem=send_sem.at[from_slot], recv_sem=recv_sem.at[to_slot],
                                            device_id=peer_device, device_id_type=MESH)

    def ring_copies(chunk):
        at = (rows(chunk // (cols // CHUNK)), pl.ds(pl.multiple_of(lax.rem(chunk, cols // CHUNK) * CHUNK, CHUNK), CHUNK))
        return (pltpu.make_async_copy(one_in.at[at], ring.at[0, chunk], ring_sem.at[0, chunk]), pltpu.make_async_copy(two_in.at[at], ring.at[1, chunk], ring_sem.at[1, chunk]))

    def begin_stage(index, carry):
        stage_copy(index).start()
        return carry

    def begin_own(index, carry):
        own_copy(index).start()
        weight_copy(index).start()
        return carry

    def begin_send(index, carry):
        stage_copy(index).wait()
        send_copy(index).start()
        return carry

    lax.fori_loop(0, STAGE_SLOTS, begin_stage, 0)
    lax.fori_loop(0, OWN_SLOTS, begin_own, 0)
    enter(others)
    lax.fori_loop(0, AHEAD, begin_send, 0)
    lane_ids = lanes_of()
    width = MEAN_WIDTH
    zero = jnp.zeros((GROUP, LANES), F32)
    first_ring = parts - RING // 2

    def one_part(index, carry):
        total, stat = carry
        own_slot, land_slot = lax.rem(index, OWN_SLOTS), lax.rem(index, LAND_SLOTS)
        row_at = rows(index // per_group)
        col_at = lax.rem(index, per_group) * PART

        @pl.when(jnp.logical_and(index + AHEAD >= LAND_SLOTS, index + AHEAD < parts))
        def _():
            pl.semaphore_wait(free_sem, 1)

        @pl.when(index + AHEAD < parts)
        def _():
            begin_send(index + AHEAD, 0)

        own_copy(index).wait()
        weight_copy(index).wait()
        send_copy(index).wait_recv()

        def piece(step, sums):
            grad_sum, weight_sum = sums
            near = pl.ds(pl.multiple_of(step * width, width), width)
            far = pl.ds(pl.multiple_of(col_at + step * width, width), width)
            weight = weight_ref[row_at, far]
            mean = (own[own_slot, :, near].astype(F32) + land[land_slot, :, near].astype(F32)) * 0.5
            mean_ref[row_at, far] = swap(mean)
            cuts = range(0, width, LANES)
            grad_sum += tree_sum([mean[:, at:at + LANES] * mean[:, at:at + LANES] for at in cuts])
            weight_sum += tree_sum([weight[:, at:at + LANES] * weight[:, at:at + LANES] for at in cuts])
            return grad_sum, weight_sum

        grad_sum, weight_sum = lax.fori_loop(0, PART // width, piece, (zero, zero))

        @pl.when(index + LAND_SLOTS < parts)
        def _():
            pl.semaphore_signal(free_sem, inc=1, device_id=peer_device, device_id_type=MESH)

        @pl.when(index + OWN_SLOTS < parts)
        def _():
            begin_own(index + OWN_SLOTS, 0)

        send_copy(index).wait_send()

        @pl.when(index + STAGE_SLOTS < parts)
        def _():
            begin_stage(index + STAGE_SLOTS, 0)

        @pl.when(index >= first_ring)
        def _():
            for late in range(2):
                for copy in ring_copies((index - first_ring) * 2 + late):
                    copy.start()

        return total + grad_sum, put_lane(stat, lane_ids, index // per_group, weight_sum)

    total, stat = lax.fori_loop(0, parts, one_part, (zero, zero))
    stat_ref[...] = stat
    part[...] = total
    slots[me] = part[...]
    share(me, others, part, slots, small_send, small_recv)
    whole = tree_sum([slots[index] for index in range(model_size * data_size)])
    whole = jnp.sum(jnp.sum(whole, axis=1, keepdims=True), axis=0, keepdims=True)
    whole = jnp.broadcast_to(whole, (GROUP, LANES))
    clip_ref[...] = jnp.minimum(1.0, MAX_NORM / jnp.sqrt(whole))

    def finish(chunk, carry):
        for copy in ring_copies(chunk):
            copy.wait()
        return carry

    lax.fori_loop(0, RING, finish, 0)


def moment_kernel(groups, cols, mean_in, weight_in, ring_in, land_in, clip, weight_stat, one_in, two_in, dir_ref, weight_ref, ring, land, one_out, two_out, stat_ref,
                  one_get, two_get, one_put, two_put):
    per_group = cols // CHUNK
    chunks = groups * per_group
    width = MOMENT_WIDTH
    lane_ids = lanes_of()

    def place(chunk):
        return rows(chunk // per_group), pl.ds(pl.multiple_of(lax.rem(chunk, per_group) * CHUNK, CHUNK), CHUNK)

    def gets(chunk):
        slot = lax.rem(chunk, RING)
        at = place(chunk)
        return (pltpu.make_async_copy(one_in.at[at], ring.at[0, slot], one_get.at[slot]), pltpu.make_async_copy(two_in.at[at], ring.at[1, slot], two_get.at[slot]))

    def puts(chunk):
        slot = lax.rem(chunk, RING)
        at = place(chunk)
        return (pltpu.make_async_copy(ring.at[0, slot], one_out.at[at], one_put.at[slot]), pltpu.make_async_copy(ring.at[1, slot], two_out.at[at], two_put.at[slot]))

    def start(copies, priority=0):
        for copy in copies:
            copy.start(priority=priority)

    def wait(copies):
        for copy in copies:
            copy.wait()

    scale = jnp.concatenate([clip[...]] * (width // LANES), axis=1)
    one_scale = (1.0 - BETA_ONE) * scale
    two_scale = (1.0 - BETA_TWO) * scale * scale
    ratio = CORR_TWO ** 0.5 / CORR_ONE
    floor = EPSILON * CORR_TWO ** 0.5

    def one_chunk(chunk, stat):
        slot = lax.rem(chunk, RING)
        row_at = rows(chunk // per_group)
        col_at = lax.rem(chunk, per_group) * CHUNK

        @pl.when(chunk >= RING)
        def _():
            wait(gets(chunk))

        def piece(index, total):
            near = pl.ds(pl.multiple_of(index * width, width), width)
            far = pl.ds(pl.multiple_of(col_at + index * width, width), width)
            mean, weight = swap(dir_ref[row_at, far]), weight_ref[row_at, far]
            old_one, old_two = ring[0, slot, :, near], ring[1, slot, :, near]
            new_one = BETA_ONE * old_one + one_scale * mean
            new_two = BETA_TWO * old_two + two_scale * mean * mean
            root = new_two * lax.rsqrt(jnp.maximum(new_two, TINY))
            direction = (new_one * ratio) / (root + floor) + WEIGHT_DECAY * weight
            ring[0, slot, :, near] = new_one
            ring[1, slot, :, near] = new_two
            dir_ref[row_at, far] = swap(direction)
            return total + tree_sum([direction[:, at:at + LANES] * direction[:, at:at + LANES] for at in range(0, width, LANES)])

        total = lax.fori_loop(0, CHUNK // width, piece, jnp.zeros((GROUP, LANES), F32))
        start(puts(chunk), priority=1)
        ahead = chunk + RING - LAG

        @pl.when(jnp.logical_and(ahead >= RING, ahead < chunks))
        def _():
            wait(puts(ahead - RING))
            for priority, copy in enumerate(gets(ahead)):
                copy.start(priority=priority)

        return put_lane(stat, lane_ids, chunk // per_group, total)

    stat_ref[0] = lax.fori_loop(0, chunks, one_chunk, jnp.zeros((GROUP, LANES), F32))
    stat_ref[1] = weight_stat[...]

    def finish(chunk, carry):
        wait(puts(chunk))
        return carry

    lax.fori_loop(chunks - RING, chunks, finish, 0)


def segment_sums(values):
    lane_ids = lanes_of()
    row_ids = lax.broadcasted_iota(jnp.int32, (GROUP, LANES), 0)
    kind = lax.rem(lane_ids, 3)
    first = jnp.where(kind == 0, 3, 4)
    second = jnp.where(kind == 0, 4, jnp.where(kind == 1, 7, 8))
    segment = jnp.where(row_ids < first, 0, jnp.where(row_ids < second, 1, 2))
    out = jnp.zeros((GROUP, LANES), F32)
    for index in range(3):
        inside = segment == index
        out = jnp.where(inside, jnp.sum(jnp.where(inside, values, 0.0), axis=0, keepdims=True), out)
    return out


def weight_kernel(sizes, groups, cols, direction, weight, stats, land, rate, ride, slots, packed, spare, send_sem, recv_sem, ride_sem, small_send, small_recv):
    model_size, data_size = sizes
    data = lax.axis_index('data')
    me, others = peers(model_size, data_size)
    peer_device = (lax.axis_index('model'), lax.rem(data + 1, data_size))
    sent = groups - RIDE
    enter(others)
    slots[me] = stats[...]
    share(me, others, stats, slots, small_send, small_recv)
    lane_ids = lanes_of()
    dir_sq = segment_sums(tree_sum([slots[index, 0] for index in range(model_size * data_size)]))
    weight_sq = segment_sums(tree_sum([slots[index, 1] for index in range(model_size * data_size)]))
    rate[0] = LEARN_RATE * (jnp.sqrt(weight_sq) / jnp.sqrt(dir_sq))
    width = PACK_WIDTH

    def send_copy(group):
        slot = lax.rem(group, SEND_SLOTS)
        return pltpu.make_async_remote_copy(src_ref=packed.at[slot], dst_ref=land.at[group], send_sem=send_sem.at[slot], recv_sem=recv_sem.at[group],
                                            device_id=peer_device, device_id_type=MESH)

    def ride_copy(index):
        slot = lax.rem(index, RIDE_SLOTS)
        return pltpu.make_async_copy(spare.at[slot], ride.at[index], ride_sem.at[slot])

    def pack(group, target, slot):
        group_rate = jnp.sum(jnp.where(lane_ids == group, rate[0], 0.0), axis=1, keepdims=True)

        def piece(index, inner):
            at = pl.ds(pl.multiple_of(index * width, width), width)
            target[slot, :, at] = (weight[rows(group), at] - group_rate * swap(direction[rows(group), at])).astype(BF16)
            return inner

        lax.fori_loop(0, cols // width, piece, 0)

    def one_group(group, carry):
        slot = lax.rem(group, SEND_SLOTS)

        @pl.when(group >= SEND_SLOTS)
        def _():
            send_copy(group - SEND_SLOTS).wait_send()

        pack(group, packed, slot)
        send_copy(group).start()

        def one_ride(index, inner):
            @pl.when(index >= RIDE_SLOTS)
            def _():
                ride_copy(index - RIDE_SLOTS).wait()

            pack(sent + index, spare, lax.rem(index, RIDE_SLOTS))
            ride_copy(index).start()
            return inner

        lax.fori_loop(group * RIDE // sent, (group + 1) * RIDE // sent, one_ride, 0)
        return carry

    lax.fori_loop(0, sent, one_group, 0)

    def finish(group, carry):
        send_copy(group).wait_recv()
        return carry

    lax.fori_loop(0, sent, finish, 0)
    for group in range(sent - SEND_SLOTS, sent):
        send_copy(group).wait_send()
    for index in range(RIDE - RIDE_SLOTS, RIDE):
        ride_copy(index).wait()


def write_kernel(sizes, groups, cols, direction, weight, land, rate, params, master, fresh, packed, master_sem, land_sem, own_sem):
    data_size = sizes[1]
    data = lax.axis_index('data')
    peer = lax.rem(data + 1, data_size)
    width = 4096
    lane_ids = lanes_of()
    per_group = cols // WRITE_CHUNK
    chunks = groups * per_group

    def columns(chunk, base):
        return pl.ds(pl.multiple_of(base + lax.rem(chunk, per_group) * WRITE_CHUNK, WRITE_CHUNK), WRITE_CHUNK)

    def puts(chunk):
        slot = lax.rem(chunk, WRITE_SLOTS)
        at = rows(chunk // per_group)
        return (pltpu.make_async_copy(fresh.at[slot], master.at[at, columns(chunk, 0)], master_sem.at[slot]),
                pltpu.make_async_copy(packed.at[slot], params.at[at, columns(chunk, data * cols)], own_sem.at[slot]))

    def land_copy(group):
        return pltpu.make_async_copy(land.at[group], params.at[rows(group), pl.ds(pl.multiple_of(peer * cols, LANES), cols)], land_sem.at[group])

    def one_chunk(chunk, carry):
        slot = lax.rem(chunk, WRITE_SLOTS)
        group = chunk // per_group

        @pl.when(jnp.logical_and(lax.rem(chunk, per_group) == 0, group < groups - RIDE))
        def _():
            land_copy(group).start()

        @pl.when(chunk >= WRITE_SLOTS)
        def _():
            for copy in puts(chunk - WRITE_SLOTS):
                copy.wait()

        group_rate = jnp.sum(jnp.where(lane_ids == group, rate[0], 0.0), axis=1, keepdims=True)

        def piece(index, inner):
            near = pl.ds(pl.multiple_of(index * width, width), width)
            far = pl.ds(pl.multiple_of(lax.rem(chunk, per_group) * WRITE_CHUNK + index * width, width), width)
            new = weight[rows(group), far] - group_rate * swap(direction[rows(group), far])
            fresh[slot, :, near] = new
            packed[slot, :, near] = new.astype(BF16)
            return inner

        lax.fori_loop(0, WRITE_CHUNK // width, piece, 0)
        for priority, copy in enumerate(puts(chunk)):
            copy.start(priority=priority)
        return carry

    lax.fori_loop(0, chunks, one_chunk, 0)

    def finish(group, carry):
        land_copy(group).wait()
        return carry

    lax.fori_loop(0, groups - RIDE, finish, 0)
    for chunk in range(chunks - WRITE_SLOTS, chunks):
        for copy in puts(chunk):
            copy.wait()


def place_kernel(sizes, groups, cols, given, params_in, params, put_sem):
    data_size = sizes[1]
    peer = lax.rem(lax.axis_index('data') + 1, data_size)

    def put(index):
        return pltpu.make_async_copy(given.at[index], params.at[rows(groups - RIDE + index), pl.ds(pl.multiple_of(peer * cols, LANES), cols)], put_sem.at[index])

    def begin(index, carry):
        put(index).start()
        return carry

    def finish(index, carry):
        put(index).wait()
        return carry

    lax.fori_loop(0, RIDE, begin, 0)
    lax.fori_loop(0, RIDE, finish, 0)


def solution(mesh):
    sizes = (mesh.shape['model'], mesh.shape['data'])
    devices = sizes[0] * sizes[1]
    both_axes = ('model', 'data')
    state_spec = P(None, both_axes)
    hbm = pl.BlockSpec(memory_space=pl.ANY)
    vmem = pl.BlockSpec(memory_space=pltpu.VMEM)
    dma = pltpu.SemaphoreType.DMA

    def device_step(local_grads, master, moment_one, moment_two):
        blocks, cols = master.shape
        groups = blocks // GROUP
        kept = pltpu.VMEM((blocks, cols), F32)
        keep = functools.partial(pltpu.with_memory_space_constraint, memory_space=pltpu.VMEM)
        tile = pltpu.VMEM((GROUP, LANES), F32)
        state = jax.ShapeDtypeStruct((blocks, cols), F32)

        landed = pltpu.VMEM((groups - RIDE, GROUP, cols), BF16)
        riding = jax.ShapeDtypeStruct((RIDE, GROUP, cols), BF16)
        ring_shape = pltpu.VMEM((2, RING, GROUP, CHUNK), F32)
        landed = pltpu.VMEM((groups - RIDE, GROUP, cols), BF16)
        riding = jax.ShapeDtypeStruct((RIDE, GROUP, cols), BF16)
        parts = groups * (cols // PART)

        caught = pltpu.VMEM((LAND_SLOTS, GROUP, PART), BF16)

        mean, weight, ring, catch, clip, weight_stat = pl.pallas_call(
            functools.partial(exchange_kernel, sizes, groups, cols),
            out_shape=(kept, kept, ring_shape, caught, tile, tile),
            in_specs=[hbm] * 4,
            out_specs=[vmem] * 6,
            scratch_shapes=[pltpu.VMEM((STAGE_SLOTS, GROUP, PART), BF16), pltpu.VMEM((OWN_SLOTS, GROUP, PART), BF16), pltpu.VMEM((GROUP, LANES), F32), pltpu.VMEM((devices, GROUP, LANES), F32),
                            dma((STAGE_SLOTS,)), dma((STAGE_SLOTS,)), dma((LAND_SLOTS,)), pltpu.SemaphoreType.REGULAR, dma((OWN_SLOTS,)), dma((parts,)), dma((2, RING)), dma((devices,)), dma((devices,))],
            compiler_params=pltpu.CompilerParams(collective_id=0, has_side_effects=True, vmem_limit_bytes=SCOPE),
            name='exchange',
        )(local_grads, master, moment_one, moment_two)

        direction, weight, _, _, new_one, new_two, stats = pl.pallas_call(
            functools.partial(moment_kernel, groups, cols),
            out_shape=(kept, kept, ring_shape, caught, state, state, pltpu.VMEM((2, GROUP, LANES), F32)),
            in_specs=[vmem] * 6 + [hbm] * 2,
            out_specs=[vmem, vmem, vmem, vmem, hbm, hbm, vmem],
            input_output_aliases={0: 0, 1: 1, 2: 2, 3: 3},
            scratch_shapes=[dma((RING,))] * 4,
            compiler_params=pltpu.CompilerParams(vmem_limit_bytes=SCOPE),
            name='moments',
        )(mean, weight, ring, catch, keep(clip), keep(weight_stat), moment_one, moment_two)

        land, rate, ride = pl.pallas_call(
            functools.partial(weight_kernel, sizes, groups, cols),
            out_shape=(landed, pltpu.VMEM((2, GROUP, LANES), F32), riding),
            in_specs=[vmem] * 3,
            out_specs=[vmem, vmem, hbm],
            input_output_aliases={2: 1},
            scratch_shapes=[pltpu.VMEM((devices, 2, GROUP, LANES), F32), pltpu.VMEM((SEND_SLOTS, GROUP, cols), BF16), pltpu.VMEM((RIDE_SLOTS, GROUP, cols), BF16),
                            dma((SEND_SLOTS,)), dma((groups - RIDE,)), dma((RIDE_SLOTS,)), dma((devices,)), dma((devices,))],
            compiler_params=pltpu.CompilerParams(collective_id=1, has_side_effects=True, vmem_limit_bytes=SCOPE),
            name='weights',
        )(keep(direction), keep(weight), keep(stats))

        given = lax.ppermute(ride, 'data', [(rank, (rank + 1) % sizes[1]) for rank in range(sizes[1])])

        params, new_master = pl.pallas_call(
            functools.partial(write_kernel, sizes, groups, cols),
            out_shape=(jax.ShapeDtypeStruct((blocks, sizes[1] * cols), BF16), state),
            in_specs=[vmem] * 4,
            out_specs=[hbm, hbm],
            scratch_shapes=[pltpu.VMEM((WRITE_SLOTS, GROUP, WRITE_CHUNK), F32), pltpu.VMEM((WRITE_SLOTS, GROUP, WRITE_CHUNK), BF16),
                            dma((WRITE_SLOTS,)), dma((groups,)), dma((WRITE_SLOTS,))],
            compiler_params=pltpu.CompilerParams(vmem_limit_bytes=SCOPE),
            name='write',
        )(keep(direction), keep(weight), keep(land), keep(rate))
        params = pl.pallas_call(
            functools.partial(place_kernel, sizes, groups, cols),
            out_shape=jax.ShapeDtypeStruct((blocks, sizes[1] * cols), BF16),
            in_specs=[vmem, hbm],
            out_specs=hbm,
            input_output_aliases={1: 0},
            scratch_shapes=[dma((RIDE,))],
            compiler_params=pltpu.CompilerParams(vmem_limit_bytes=SCOPE),
            name='place',
        )(keep(given), params)
        return params, new_master, new_one, new_two

    return jax.shard_map(device_step, mesh=mesh, in_specs=(P('data', None, 'model'), state_spec, state_spec, state_spec),
                         out_specs=(P(None, 'model'), state_spec, state_spec, state_spec), check_vma=False)
```

```python
import functools

import jax
import jax.numpy as jnp
from jax import lax
from jax.experimental import pallas as pl
from jax.experimental.pallas import tpu as pltpu
from jax.sharding import PartitionSpec as P

STEP = 4
LEARN_RATE = 0.08
BETA_ONE = 0.9
BETA_TWO = 0.999
EPSILON = 1e-6
WEIGHT_DECAY = 0.01
MAX_NORM = 1.0
CORR_ONE = 1.0 - BETA_ONE ** STEP
CORR_TWO = 1.0 - BETA_TWO ** STEP
TINY = 1.2e-38

MESH = pl.DeviceIdType.MESH
F32 = jnp.float32
BF16 = jnp.bfloat16
SCOPE = 4000 << 10
LANES = 128
GROUP = 8

PART = 16384
AHEAD = 5
LAND_SLOTS = 8
STAGE_SLOTS = 10
OWN_SLOTS = 5
RING = 20
LAG = 4
MOMENT_WIDTH = 8192
MEAN_WIDTH = 2048
PACK_WIDTH = 8192
CHUNK = 8192
SEND_SLOTS = 3
RIDE = 17
RIDE_SLOTS = 4
WRITE_SLOTS = 5
WRITE_CHUNK = 16384


def rows(group):
    return pl.ds(pl.multiple_of(group * GROUP, GROUP), GROUP)


def lanes_of():
    return lax.broadcasted_iota(jnp.int32, (GROUP, LANES), 1)


def put_lane(tile, lane_ids, lane, partial):
    row_sum = jnp.sum(partial, axis=1, keepdims=True)
    return tile + jnp.where(lane_ids == lane, row_sum, 0.0)


def swap(values):
    parts = [values[:, at:at + LANES] for at in range(0, values.shape[1], LANES)]
    return jnp.concatenate([parts[index ^ 1] for index in range(len(parts))], axis=1)


def tree_sum(values):
    while len(values) > 1:
        values = [a + b for a, b in zip(values[::2], values[1::2])] + ([values[-1]] if len(values) % 2 else [])
    return values[0]


def peers(model_size, data_size):
    model, data = lax.axis_index('model'), lax.axis_index('data')
    out = []
    for step in range(1, model_size * data_size):
        peer_model = lax.rem(model + step // data_size, model_size)
        peer_data = lax.rem(data + step % data_size, data_size)
        out.append(((peer_model, peer_data), peer_model * data_size + peer_data))
    return model * data_size + data, out


def enter(others):
    barrier = pltpu.get_barrier_semaphore()
    for device, _ in others:
        pl.semaphore_signal(barrier, inc=1, device_id=device, device_id_type=MESH)
    pl.semaphore_wait(barrier, len(others))


def share(me, others, source, slots, send_sem, recv_sem):
    copies = []
    for device, index in others:
        copy = pltpu.make_async_remote_copy(src_ref=source, dst_ref=slots.at[me], send_sem=send_sem.at[index], recv_sem=recv_sem.at[me], device_id=device, device_id_type=MESH)
        copy.start()
        copies.append(copy)
    for device, index in others:
        pltpu.make_async_remote_copy(src_ref=source, dst_ref=slots.at[index], send_sem=send_sem.at[index], recv_sem=recv_sem.at[index], device_id=device, device_id_type=MESH).wait_recv()
    for copy in copies:
        copy.wait_send()


def exchange_kernel(sizes, groups, cols, grads, master, one_in, two_in, mean_ref, weight_ref, ring, land, clip_ref, stat_ref, stage, own, part, slots,
                    stage_sem, send_sem, recv_sem, free_sem, own_sem, weight_sem, ring_sem, small_send, small_recv):
    model_size, data_size = sizes
    data = lax.axis_index('data')
    me, others = peers(model_size, data_size)
    peer = lax.rem(data + 1, data_size)
    peer_device = (lax.axis_index('model'), peer)
    per_group = cols // PART
    parts = groups * per_group

    def columns(index, base):
        return pl.ds(pl.multiple_of(base + lax.rem(index, per_group) * PART, PART), PART)

    def own_copy(index):
        slot = lax.rem(index, OWN_SLOTS)
        return pltpu.make_async_copy(grads.at[0, rows(index // per_group), columns(index, data * cols)], own.at[slot], own_sem.at[slot])

    def weight_copy(index):
        at = (rows(index // per_group), columns(index, 0))
        return pltpu.make_async_copy(master.at[at], weight_ref.at[at], weight_sem.at[index])

    def stage_copy(index):
        slot = lax.rem(index, STAGE_SLOTS)
        return pltpu.make_async_copy(grads.at[0, rows(index // per_group), columns(index, peer * cols)], stage.at[slot], stage_sem.at[slot])

    def send_copy(index):
        from_slot, to_slot = lax.rem(index, STAGE_SLOTS), lax.rem(index, LAND_SLOTS)
        return pltpu.make_async_remote_copy(src_ref=stage.at[from_slot], dst_ref=land.at[to_slot], send_sem=send_sem.at[from_slot], recv_sem=recv_sem.at[to_slot],
                                            device_id=peer_device, device_id_type=MESH)

    def ring_copies(chunk):
        at = (rows(chunk // (cols // CHUNK)), pl.ds(pl.multiple_of(lax.rem(chunk, cols // CHUNK) * CHUNK, CHUNK), CHUNK))
        return (pltpu.make_async_copy(one_in.at[at], ring.at[0, chunk], ring_sem.at[0, chunk]), pltpu.make_async_copy(two_in.at[at], ring.at[1, chunk], ring_sem.at[1, chunk]))

    def begin_stage(index, carry):
        stage_copy(index).start()
        return carry

    def begin_own(index, carry):
        own_copy(index).start()
        weight_copy(index).start()
        return carry

    def begin_send(index, carry):
        stage_copy(index).wait()
        send_copy(index).start()
        return carry

    lax.fori_loop(0, STAGE_SLOTS, begin_stage, 0)
    lax.fori_loop(0, OWN_SLOTS, begin_own, 0)
    enter(others)
    lax.fori_loop(0, AHEAD, begin_send, 0)
    lane_ids = lanes_of()
    width = MEAN_WIDTH
    zero = jnp.zeros((GROUP, LANES), F32)
    first_ring = parts - RING // 2

    def one_part(index, carry):
        total, stat = carry
        own_slot, land_slot = lax.rem(index, OWN_SLOTS), lax.rem(index, LAND_SLOTS)
        row_at = rows(index // per_group)
        col_at = lax.rem(index, per_group) * PART

        @pl.when(jnp.logical_and(index + AHEAD >= LAND_SLOTS, index + AHEAD < parts))
        def _():
            pl.semaphore_wait(free_sem, 1)

        @pl.when(index + AHEAD < parts)
        def _():
            begin_send(index + AHEAD, 0)

        own_copy(index).wait()
        weight_copy(index).wait()
        send_copy(index).wait_recv()

        def piece(step, sums):
            grad_sum, weight_sum = sums
            near = pl.ds(pl.multiple_of(step * width, width), width)
            far = pl.ds(pl.multiple_of(col_at + step * width, width), width)
            weight = weight_ref[row_at, far]
            mean = (own[own_slot, :, near].astype(F32) + land[land_slot, :, near].astype(F32)) * 0.5
            mean_ref[row_at, far] = swap(mean)
            cuts = range(0, width, LANES)
            grad_sum += tree_sum([mean[:, at:at + LANES] * mean[:, at:at + LANES] for at in cuts])
            weight_sum += tree_sum([weight[:, at:at + LANES] * weight[:, at:at + LANES] for at in cuts])
            return grad_sum, weight_sum

        grad_sum, weight_sum = lax.fori_loop(0, PART // width, piece, (zero, zero))

        @pl.when(index + LAND_SLOTS < parts)
        def _():
            pl.semaphore_signal(free_sem, inc=1, device_id=peer_device, device_id_type=MESH)

        @pl.when(index + OWN_SLOTS < parts)
        def _():
            begin_own(index + OWN_SLOTS, 0)

        send_copy(index).wait_send()

        @pl.when(index + STAGE_SLOTS < parts)
        def _():
            begin_stage(index + STAGE_SLOTS, 0)

        @pl.when(index >= first_ring)
        def _():
            for late in range(2):
                for copy in ring_copies((index - first_ring) * 2 + late):
                    copy.start()

        return total + grad_sum, put_lane(stat, lane_ids, index // per_group, weight_sum)

    total, stat = lax.fori_loop(0, parts, one_part, (zero, zero))
    stat_ref[...] = stat
    part[...] = total
    slots[me] = part[...]
    share(me, others, part, slots, small_send, small_recv)
    whole = tree_sum([slots[index] for index in range(model_size * data_size)])
    whole = jnp.sum(jnp.sum(whole, axis=1, keepdims=True), axis=0, keepdims=True)
    whole = jnp.broadcast_to(whole, (GROUP, LANES))
    clip_ref[...] = jnp.minimum(1.0, MAX_NORM / jnp.sqrt(whole))

    def finish(chunk, carry):
        for copy in ring_copies(chunk):
            copy.wait()
        return carry

    lax.fori_loop(0, RING, finish, 0)


def moment_kernel(groups, cols, mean_in, weight_in, ring_in, land_in, clip, weight_stat, one_in, two_in, dir_ref, weight_ref, ring, land, one_out, two_out, stat_ref,
                  one_get, two_get, one_put, two_put):
    per_group = cols // CHUNK
    chunks = groups * per_group
    width = MOMENT_WIDTH
    lane_ids = lanes_of()

    def place(chunk):
        return rows(chunk // per_group), pl.ds(pl.multiple_of(lax.rem(chunk, per_group) * CHUNK, CHUNK), CHUNK)

    def gets(chunk):
        slot = lax.rem(chunk, RING)
        at = place(chunk)
        return (pltpu.make_async_copy(one_in.at[at], ring.at[0, slot], one_get.at[slot]), pltpu.make_async_copy(two_in.at[at], ring.at[1, slot], two_get.at[slot]))

    def puts(chunk):
        slot = lax.rem(chunk, RING)
        at = place(chunk)
        return (pltpu.make_async_copy(ring.at[0, slot], one_out.at[at], one_put.at[slot]), pltpu.make_async_copy(ring.at[1, slot], two_out.at[at], two_put.at[slot]))

    def start(copies, priority=0):
        for copy in copies:
            copy.start(priority=priority)

    def wait(copies):
        for copy in copies:
            copy.wait()

    scale = jnp.concatenate([clip[...]] * (width // LANES), axis=1)
    one_scale = (1.0 - BETA_ONE) * scale
    two_scale = (1.0 - BETA_TWO) * scale * scale
    ratio = CORR_TWO ** 0.5 / CORR_ONE
    floor = EPSILON * CORR_TWO ** 0.5

    def one_chunk(chunk, stat):
        slot = lax.rem(chunk, RING)
        row_at = rows(chunk // per_group)
        col_at = lax.rem(chunk, per_group) * CHUNK

        @pl.when(chunk >= RING)
        def _():
            wait(gets(chunk))

        def piece(index, total):
            near = pl.ds(pl.multiple_of(index * width, width), width)
            far = pl.ds(pl.multiple_of(col_at + index * width, width), width)
            mean, weight = swap(dir_ref[row_at, far]), weight_ref[row_at, far]
            old_one, old_two = ring[0, slot, :, near], ring[1, slot, :, near]
            new_one = BETA_ONE * old_one + one_scale * mean
            new_two = BETA_TWO * old_two + two_scale * mean * mean
            root = new_two * lax.rsqrt(jnp.maximum(new_two, TINY))
            direction = (new_one * ratio) / (root + floor) + WEIGHT_DECAY * weight
            ring[0, slot, :, near] = new_one
            ring[1, slot, :, near] = new_two
            dir_ref[row_at, far] = swap(direction)
            return total + tree_sum([direction[:, at:at + LANES] * direction[:, at:at + LANES] for at in range(0, width, LANES)])

        total = lax.fori_loop(0, CHUNK // width, piece, jnp.zeros((GROUP, LANES), F32))
        start(puts(chunk), priority=1)
        ahead = chunk + RING - LAG

        @pl.when(jnp.logical_and(ahead >= RING, ahead < chunks))
        def _():
            wait(puts(ahead - RING))
            start(gets(ahead))

        return put_lane(stat, lane_ids, chunk // per_group, total)

    stat_ref[0] = lax.fori_loop(0, chunks, one_chunk, jnp.zeros((GROUP, LANES), F32))
    stat_ref[1] = weight_stat[...]

    def finish(chunk, carry):
        wait(puts(chunk))
        return carry

    lax.fori_loop(chunks - RING, chunks, finish, 0)


def segment_sums(values):
    lane_ids = lanes_of()
    row_ids = lax.broadcasted_iota(jnp.int32, (GROUP, LANES), 0)
    kind = lax.rem(lane_ids, 3)
    first = jnp.where(kind == 0, 3, 4)
    second = jnp.where(kind == 0, 4, jnp.where(kind == 1, 7, 8))
    segment = jnp.where(row_ids < first, 0, jnp.where(row_ids < second, 1, 2))
    out = jnp.zeros((GROUP, LANES), F32)
    for index in range(3):
        inside = segment == index
        out = jnp.where(inside, jnp.sum(jnp.where(inside, values, 0.0), axis=0, keepdims=True), out)
    return out


def weight_kernel(sizes, groups, cols, direction, weight, stats, land, rate, ride, slots, packed, spare, send_sem, recv_sem, ride_sem, small_send, small_recv):
    model_size, data_size = sizes
    data = lax.axis_index('data')
    me, others = peers(model_size, data_size)
    peer_device = (lax.axis_index('model'), lax.rem(data + 1, data_size))
    sent = groups - RIDE
    enter(others)
    slots[me] = stats[...]
    share(me, others, stats, slots, small_send, small_recv)
    lane_ids = lanes_of()
    dir_sq = segment_sums(tree_sum([slots[index, 0] for index in range(model_size * data_size)]))
    weight_sq = segment_sums(tree_sum([slots[index, 1] for index in range(model_size * data_size)]))
    rate[0] = LEARN_RATE * (jnp.sqrt(weight_sq) / jnp.sqrt(dir_sq))
    width = PACK_WIDTH

    def send_copy(group):
        slot = lax.rem(group, SEND_SLOTS)
        return pltpu.make_async_remote_copy(src_ref=packed.at[slot], dst_ref=land.at[group], send_sem=send_sem.at[slot], recv_sem=recv_sem.at[group],
                                            device_id=peer_device, device_id_type=MESH)

    def ride_copy(index):
        slot = lax.rem(index, RIDE_SLOTS)
        return pltpu.make_async_copy(spare.at[slot], ride.at[index], ride_sem.at[slot])

    def pack(group, target, slot):
        group_rate = jnp.sum(jnp.where(lane_ids == group, rate[0], 0.0), axis=1, keepdims=True)

        def piece(index, inner):
            at = pl.ds(pl.multiple_of(index * width, width), width)
            target[slot, :, at] = (weight[rows(group), at] - group_rate * swap(direction[rows(group), at])).astype(BF16)
            return inner

        lax.fori_loop(0, cols // width, piece, 0)

    def one_group(group, carry):
        slot = lax.rem(group, SEND_SLOTS)

        @pl.when(group >= SEND_SLOTS)
        def _():
            send_copy(group - SEND_SLOTS).wait_send()

        pack(group, packed, slot)
        send_copy(group).start()

        def one_ride(index, inner):
            @pl.when(index >= RIDE_SLOTS)
            def _():
                ride_copy(index - RIDE_SLOTS).wait()

            pack(sent + index, spare, lax.rem(index, RIDE_SLOTS))
            ride_copy(index).start()
            return inner

        lax.fori_loop(group * RIDE // sent, (group + 1) * RIDE // sent, one_ride, 0)
        return carry

    lax.fori_loop(0, sent, one_group, 0)

    def finish(group, carry):
        send_copy(group).wait_recv()
        return carry

    lax.fori_loop(0, sent, finish, 0)
    for group in range(sent - SEND_SLOTS, sent):
        send_copy(group).wait_send()
    for index in range(RIDE - RIDE_SLOTS, RIDE):
        ride_copy(index).wait()


def write_kernel(sizes, groups, cols, direction, weight, land, rate, params, master, fresh, packed, master_sem, land_sem, own_sem):
    data_size = sizes[1]
    data = lax.axis_index('data')
    peer = lax.rem(data + 1, data_size)
    width = 4096
    lane_ids = lanes_of()
    per_group = cols // WRITE_CHUNK
    chunks = groups * per_group

    def columns(chunk, base):
        return pl.ds(pl.multiple_of(base + lax.rem(chunk, per_group) * WRITE_CHUNK, WRITE_CHUNK), WRITE_CHUNK)

    def puts(chunk):
        slot = lax.rem(chunk, WRITE_SLOTS)
        at = rows(chunk // per_group)
        return (pltpu.make_async_copy(fresh.at[slot], master.at[at, columns(chunk, 0)], master_sem.at[slot]),
                pltpu.make_async_copy(packed.at[slot], params.at[at, columns(chunk, data * cols)], own_sem.at[slot]))

    def land_copy(group):
        return pltpu.make_async_copy(land.at[group], params.at[rows(group), pl.ds(pl.multiple_of(peer * cols, LANES), cols)], land_sem.at[group])

    def one_chunk(chunk, carry):
        slot = lax.rem(chunk, WRITE_SLOTS)
        group = chunk // per_group

        @pl.when(jnp.logical_and(lax.rem(chunk, per_group) == 0, group < groups - RIDE))
        def _():
            land_copy(group).start()

        @pl.when(chunk >= WRITE_SLOTS)
        def _():
            for copy in puts(chunk - WRITE_SLOTS):
                copy.wait()

        group_rate = jnp.sum(jnp.where(lane_ids == group, rate[0], 0.0), axis=1, keepdims=True)

        def piece(index, inner):
            near = pl.ds(pl.multiple_of(index * width, width), width)
            far = pl.ds(pl.multiple_of(lax.rem(chunk, per_group) * WRITE_CHUNK + index * width, width), width)
            new = weight[rows(group), far] - group_rate * swap(direction[rows(group), far])
            fresh[slot, :, near] = new
            packed[slot, :, near] = new.astype(BF16)
            return inner

        lax.fori_loop(0, WRITE_CHUNK // width, piece, 0)
        for priority, copy in enumerate(puts(chunk)):
            copy.start(priority=priority)
        return carry

    lax.fori_loop(0, chunks, one_chunk, 0)

    def finish(group, carry):
        land_copy(group).wait()
        return carry

    lax.fori_loop(0, groups - RIDE, finish, 0)
    for chunk in range(chunks - WRITE_SLOTS, chunks):
        for copy in puts(chunk):
            copy.wait()


def place_kernel(sizes, groups, cols, given, params_in, params, put_sem):
    data_size = sizes[1]
    peer = lax.rem(lax.axis_index('data') + 1, data_size)

    def put(index):
        return pltpu.make_async_copy(given.at[index], params.at[rows(groups - RIDE + index), pl.ds(pl.multiple_of(peer * cols, LANES), cols)], put_sem.at[index])

    def begin(index, carry):
        put(index).start()
        return carry

    def finish(index, carry):
        put(index).wait()
        return carry

    lax.fori_loop(0, RIDE, begin, 0)
    lax.fori_loop(0, RIDE, finish, 0)


def solution(mesh):
    sizes = (mesh.shape['model'], mesh.shape['data'])
    devices = sizes[0] * sizes[1]
    both_axes = ('model', 'data')
    state_spec = P(None, both_axes)
    hbm = pl.BlockSpec(memory_space=pl.ANY)
    vmem = pl.BlockSpec(memory_space=pltpu.VMEM)
    dma = pltpu.SemaphoreType.DMA

    def device_step(local_grads, master, moment_one, moment_two):
        blocks, cols = master.shape
        groups = blocks // GROUP
        kept = pltpu.VMEM((blocks, cols), F32)
        keep = functools.partial(pltpu.with_memory_space_constraint, memory_space=pltpu.VMEM)
        tile = pltpu.VMEM((GROUP, LANES), F32)
        state = jax.ShapeDtypeStruct((blocks, cols), F32)

        landed = pltpu.VMEM((groups - RIDE, GROUP, cols), BF16)
        riding = jax.ShapeDtypeStruct((RIDE, GROUP, cols), BF16)
        ring_shape = pltpu.VMEM((2, RING, GROUP, CHUNK), F32)
        landed = pltpu.VMEM((groups - RIDE, GROUP, cols), BF16)
        riding = jax.ShapeDtypeStruct((RIDE, GROUP, cols), BF16)
        parts = groups * (cols // PART)

        caught = pltpu.VMEM((LAND_SLOTS, GROUP, PART), BF16)

        mean, weight, ring, catch, clip, weight_stat = pl.pallas_call(
            functools.partial(exchange_kernel, sizes, groups, cols),
            out_shape=(kept, kept, ring_shape, caught, tile, tile),
            in_specs=[hbm] * 4,
            out_specs=[vmem] * 6,
            scratch_shapes=[pltpu.VMEM((STAGE_SLOTS, GROUP, PART), BF16), pltpu.VMEM((OWN_SLOTS, GROUP, PART), BF16), pltpu.VMEM((GROUP, LANES), F32), pltpu.VMEM((devices, GROUP, LANES), F32),
                            dma((STAGE_SLOTS,)), dma((STAGE_SLOTS,)), dma((LAND_SLOTS,)), pltpu.SemaphoreType.REGULAR, dma((OWN_SLOTS,)), dma((parts,)), dma((2, RING)), dma((devices,)), dma((devices,))],
            compiler_params=pltpu.CompilerParams(collective_id=0, has_side_effects=True, vmem_limit_bytes=SCOPE),
            name='exchange',
        )(local_grads, master, moment_one, moment_two)

        direction, weight, _, _, new_one, new_two, stats = pl.pallas_call(
            functools.partial(moment_kernel, groups, cols),
            out_shape=(kept, kept, ring_shape, caught, state, state, pltpu.VMEM((2, GROUP, LANES), F32)),
            in_specs=[vmem] * 6 + [hbm] * 2,
            out_specs=[vmem, vmem, vmem, vmem, hbm, hbm, vmem],
            input_output_aliases={0: 0, 1: 1, 2: 2, 3: 3},
            scratch_shapes=[dma((RING,))] * 4,
            compiler_params=pltpu.CompilerParams(vmem_limit_bytes=SCOPE),
            name='moments',
        )(mean, weight, ring, catch, keep(clip), keep(weight_stat), moment_one, moment_two)

        land, rate, ride = pl.pallas_call(
            functools.partial(weight_kernel, sizes, groups, cols),
            out_shape=(landed, pltpu.VMEM((2, GROUP, LANES), F32), riding),
            in_specs=[vmem] * 3,
            out_specs=[vmem, vmem, hbm],
            input_output_aliases={2: 1},
            scratch_shapes=[pltpu.VMEM((devices, 2, GROUP, LANES), F32), pltpu.VMEM((SEND_SLOTS, GROUP, cols), BF16), pltpu.VMEM((RIDE_SLOTS, GROUP, cols), BF16),
                            dma((SEND_SLOTS,)), dma((groups - RIDE,)), dma((RIDE_SLOTS,)), dma((devices,)), dma((devices,))],
            compiler_params=pltpu.CompilerParams(collective_id=1, has_side_effects=True, vmem_limit_bytes=SCOPE),
            name='weights',
        )(keep(direction), keep(weight), keep(stats))

        given = lax.ppermute(ride, 'data', [(rank, (rank + 1) % sizes[1]) for rank in range(sizes[1])])

        params, new_master = pl.pallas_call(
            functools.partial(write_kernel, sizes, groups, cols),
            out_shape=(jax.ShapeDtypeStruct((blocks, sizes[1] * cols), BF16), state),
            in_specs=[vmem] * 4,
            out_specs=[hbm, hbm],
            scratch_shapes=[pltpu.VMEM((WRITE_SLOTS, GROUP, WRITE_CHUNK), F32), pltpu.VMEM((WRITE_SLOTS, GROUP, WRITE_CHUNK), BF16),
                            dma((WRITE_SLOTS,)), dma((groups,)), dma((WRITE_SLOTS,))],
            compiler_params=pltpu.CompilerParams(vmem_limit_bytes=SCOPE),
            name='write',
        )(keep(direction), keep(weight), keep(land), keep(rate))
        params = pl.pallas_call(
            functools.partial(place_kernel, sizes, groups, cols),
            out_shape=jax.ShapeDtypeStruct((blocks, sizes[1] * cols), BF16),
            in_specs=[vmem, hbm],
            out_specs=hbm,
            input_output_aliases={1: 0},
            scratch_shapes=[dma((RIDE,))],
            compiler_params=pltpu.CompilerParams(vmem_limit_bytes=SCOPE),
            name='place',
        )(keep(given), params)
        return params, new_master, new_one, new_two

    return jax.shard_map(device_step, mesh=mesh, in_specs=(P('data', None, 'model'), state_spec, state_spec, state_spec),
                         out_specs=(P(None, 'model'), state_spec, state_spec, state_spec), check_vma=False)
```
